8 devices in a mesh: py: 2 (over z, y), px: 4 (over x, core).
Axes of the slice: x: 2, y: 2, z: 1, core: 2. Of those that a mesh axis runs over, the one named last changes fastest.
Arguments:
- shift: float32 [256, 512, 24], P('px', 'py')
- rhs_field: float32 [256, 512, 24], P('px', 'py')
- x_init: float32 [256, 512, 24], P('px', 'py')
- cond_x: float32 [256, 512, 24], P('px', 'py')
- cond_y: float32 [256, 512, 24], P('px', 'py')
- cond_z: float32 [256, 512, 24], P('px', 'py')
Outputs:
- output 1: float32 [256, 512, 24], P('px', 'py')
- output 2: float32 [21], replicated
All inputs are finite; a program needn't handle non-finite values.
Results may differ from the reference program's by a relative error of at most 0.001.
Values sent between devices are 32-bit elements.
A program may use at most 1 GiB of HBM per device.

```python
import jax
import jax.numpy as jnp
from jax import lax

GRID_X = 256
GRID_Y = 512
GRID_Z = 24
ITERS = 20
TOTAL_CELLS = GRID_X * GRID_Y * GRID_Z


def next_along(values, along_dim):
    dim_len = values.shape[along_dim]
    kept_part = lax.slice_in_dim(values, 1, dim_len, axis=along_dim)
    zero_plane = jnp.zeros_like(lax.slice_in_dim(values, 0, 1, axis=along_dim))
    return jnp.concatenate([kept_part, zero_plane], axis=along_dim)


def prev_along(values, along_dim):
    dim_len = values.shape[along_dim]
    kept_part = lax.slice_in_dim(values, 0, dim_len - 1, axis=along_dim)
    zero_plane = jnp.zeros_like(lax.slice_in_dim(values, 0, 1, axis=along_dim))
    return jnp.concatenate([zero_plane, kept_part], axis=along_dim)


def low_basis(length):
    centers = (jnp.arange(length).astype(jnp.float32) + 0.5) / length
    return jnp.stack([jnp.ones_like(centers), jnp.cos(jnp.pi * centers)])


def setup_inputs(seed: int = 0) -> dict:
    keys = jax.random.split(jax.random.key(seed), 7)
    grid_shape = (GRID_X, GRID_Y, GRID_Z)
    shift = jax.random.uniform(keys[0], grid_shape, jnp.float32, 0.3, 1.5)
    rhs_field = jax.random.normal(keys[1], grid_shape, jnp.float32)
    mode_coef = 2.0 * jax.random.normal(keys[6], (2, 2, 2), jnp.float32)
    smooth_part = jnp.einsum("abc,ai,bj,ck->ijk", mode_coef, low_basis(GRID_X),
                             low_basis(GRID_Y), low_basis(GRID_Z))
    x_init = 0.5 * jax.random.normal(keys[2], grid_shape, jnp.float32) + smooth_part
    cond_x = jnp.exp(jax.random.uniform(keys[3], grid_shape, jnp.float32, -2.0, 0.7))
    cond_y = jnp.exp(jax.random.uniform(keys[4], grid_shape, jnp.float32, -2.0, 0.7))
    cond_z = jnp.exp(jax.random.uniform(keys[5], grid_shape, jnp.float32, -2.0, 0.7))
    return {"shift": shift, "rhs_field": rhs_field, "x_init": x_init,
            "cond_x": cond_x, "cond_y": cond_y, "cond_z": cond_z}


def reference(shift, rhs_field, x_init, cond_x, cond_y, cond_z):
    plane_x = jnp.arange(GRID_X).reshape(GRID_X, 1, 1)
    plane_y = jnp.arange(GRID_Y).reshape(1, GRID_Y, 1)
    plane_z = jnp.arange(GRID_Z).reshape(1, 1, GRID_Z)
    plus_x = jnp.where(plane_x < GRID_X - 1, cond_x, 0.0)
    plus_y = jnp.where(plane_y < GRID_Y - 1, cond_y, 0.0)
    plus_z = jnp.where(plane_z < GRID_Z - 1, cond_z, 0.0)
    minus_x = prev_along(plus_x, 0)
    minus_y = prev_along(plus_y, 1)
    minus_z = prev_along(plus_z, 2)
    diag_coef = shift + plus_x + minus_x + plus_y + minus_y + plus_z + minus_z

    def apply_op(vec):
        return (diag_coef * vec
                - plus_x * next_along(vec, 0) - minus_x * prev_along(vec, 0)
                - plus_y * next_along(vec, 1) - minus_y * prev_along(vec, 1)
                - plus_z * next_along(vec, 2) - minus_z * prev_along(vec, 2))

    def cg_step(state_now, unused):
        x_cur, r_cur, p_cur, rho_cur = state_now
        q_vec = apply_op(p_cur)
        step_alpha = rho_cur / jnp.sum(p_cur * q_vec)
        x_new = x_cur + step_alpha * p_cur
        r_new = r_cur - step_alpha * q_vec
        rho_new = jnp.sum(r_new * r_new)
        p_new = r_new + (rho_new / rho_cur) * p_cur
        return (x_new, r_new, p_new, rho_new), rho_new

    r_start = rhs_field - apply_op(x_init)
    rho_start = jnp.sum(r_start * r_start)
    final_state, rho_steps = lax.scan(cg_step, (x_init, r_start, r_start, rho_start), None, length=ITERS)
    history = jnp.sqrt(jnp.concatenate([rho_start[None], rho_steps]) / TOTAL_CELLS)
    return final_state[0], history
```

```python
import functools

import jax
import jax.numpy as jnp
from jax import lax
from jax.experimental import pallas as pl
from jax.experimental.pallas import tpu as pltpu
from jax.sharding import PartitionSpec as P

ITERS = 20
SUM_AXES = ("px", "py")
MESH = pl.DeviceIdType.MESH
NX, NZ = 64, 24
BODY = NX * NZ
FULL = BODY + 2 * NZ
HI = BODY + NZ
OTHERS = tuple((dy, dx) for dy in range(2) for dx in range(4) if (dy, dx) != (0, 0))
SEND_AT = {1: 4, 2: 9, 3: 15, 4: 19}
TAKE_AT = {6: 1, 11: 2, 17: 3}
STEPS_AT = {6: (0, 2), 7: (2, 4), 8: (4, 5), 11: (5, 7), 12: (7, 9), 13: (9, 10),
            17: (10, 12), 18: (12, 14), 19: (14, 16)}
RENEW_AT = {8: 9, 13: 14}
S_A, S_B, S_C, S_GP, S_G, S_CL, S_DL, S_Y, S_RHO, S_LEAD, S_HIST, S_BA, S_LA, S_LB, S_LA2, S_LB2, S_ERR, S_D, S_E, S_RHO0 = range(20)


def lanes():
    return lax.broadcasted_iota(jnp.int32, (8, 128), 1)


def rows8():
    return lax.broadcasted_iota(jnp.int32, (8, 128), 0)


def lane_sum(v):
    return jnp.broadcast_to(jnp.sum(v, axis=1, keepdims=True), (8, 128))


def full_sum(v):
    return jnp.broadcast_to(jnp.sum(jnp.sum(v, axis=0, keepdims=True), axis=1, keepdims=True), (8, 128))


def three(v):
    return jnp.concatenate([v, v, v], axis=0)


def kernel(s_h, b_h, x0_h, kx_h, ky_h, kz_h, out_h, hist_ref,
           Z, X0, D, KX, KY, KZ, PKS, H, KYP, KYH, HK, RS, RR, PT, ST, CO, YB,
           lsem, osem, is_s, is_r, hs, hr, rs, rr):
    px, py = lax.axis_index("px"), lax.axis_index("py")
    me = py * 4 + px
    lane, row = lanes(), rows8()
    lane24 = lax.broadcasted_iota(jnp.int32, (24, 128), 1)
    row24 = lax.broadcasted_iota(jnp.int32, (24, 128), 0)
    first, last = lane24 == 0, lane24 == 127
    has_lo, has_hi = px > 0, px < 3

    loads = []
    for n, (src, dst, base) in enumerate((
            (ky_h, KY, 0), (x0_h, X0, NZ), (kx_h, KX, NZ), (kz_h, KZ, 8), (s_h, D, 0), (b_h, None, NZ))):
        for t in range(2):
            to = Z.at[0, t, pl.ds(base, BODY), :] if dst is None else dst.at[t, pl.ds(base, BODY), :]
            cp = pltpu.make_async_copy(src.at[:, pl.ds(128 * t, 128)], to, lsem.at[2 * n + t])
            cp.start()
            loads.append(cp)

    zero_plane = jnp.zeros((NZ, 128), jnp.float32)
    for t in range(2):
        KX[t, pl.ds(0, NZ), :] = zero_plane
        X0[t, pl.ds(0, NZ), :] = zero_plane
        X0[t, pl.ds(HI, NZ), :] = zero_plane
        KZ[t, pl.ds(0, 8), :] = jnp.zeros((8, 128), jnp.float32)
    KYH[...] = jnp.zeros((2, 8, 128), jnp.float32)

    @pl.loop(0, ITERS + 1)
    def _(k):
        for t in range(2):
            Z[k, t, pl.ds(0, NZ), :] = zero_plane
            Z[k, t, pl.ds(HI, NZ), :] = zero_plane

    barrier = pltpu.get_barrier_semaphore()
    for dy, dx in OTHERS:
        pl.semaphore_signal(barrier, inc=1, device_id=(lax.rem(py + dy, 2), lax.rem(px + dx, 4)),
                            device_id_type=MESH)
    pl.semaphore_wait(barrier, len(OTHERS))

    def to_x(step):
        return (py, px + step)

    to_y = (1 - py, px)

    def remote(src, dst, ssem, rsem, dev):
        return pltpu.make_async_remote_copy(src_ref=src, dst_ref=dst, send_sem=ssem, recv_sem=rsem,
                                            device_id=dev, device_id_type=MESH)

    def init_up(t):
        cols = pl.ds(128 * t, 128)
        return (remote(kx_h.at[pl.ds(BODY - NZ, NZ), cols], KX.at[t, pl.ds(0, NZ), :], is_s.at[t], is_r.at[t], to_x(1)),
                remote(x0_h.at[pl.ds(BODY - NZ, NZ), cols], X0.at[t, pl.ds(0, NZ), :], is_s.at[2 + t], is_r.at[2 + t], to_x(1)))

    def init_down(t):
        cols = pl.ds(128 * t, 128)
        return (remote(x0_h.at[pl.ds(0, NZ), cols], X0.at[t, pl.ds(HI, NZ), :], is_s.at[4 + t], is_r.at[4 + t], to_x(-1)),)

    @pl.when(has_hi)
    def _():
        for t in range(2):
            for cp in init_up(t):
                cp.start()

    @pl.when(has_lo)
    def _():
        for t in range(2):
            for cp in init_down(t):
                cp.start()

    off = 1 - py

    def pack_into(acc, j, lo, hi):
        v = jnp.where(py == 0, hi, lo)
        for q in range(3):
            at = 3 * j + q
            moved = pltpu.roll(v[8 * q:8 * q + 8], lax.rem(at + 2 * off, 128), 1)
            acc = jnp.where(lane == at + off, moved, acc)
        return acc

    def pack(read, dst):
        for h in range(2):
            def step(j, acc):
                lo, hi = read(32 * h + j)
                return pack_into(acc, j, lo, hi)
            dst[h] = lax.fori_loop(0, 32, step, jnp.zeros((8, 128), jnp.float32), unroll=4)

    def unpack(tile, j):
        parts = [pltpu.roll(tile, 127 - (3 * j + q), 1) for q in range(3)]
        return jnp.concatenate(parts, axis=0)

    def rowsof(i):
        return pl.multiple_of(NZ * i, 8)

    loads[0].wait()
    loads[1].wait()
    pack(lambda i: (KY[0, pl.ds(rowsof(i), NZ), :], KY[1, pl.ds(rowsof(i), NZ), :]), KYP)
    ky_copy = remote(KYP, KYH, is_s.at[6], is_r.at[6], to_y)

    @pl.when(py == 0)
    def _():
        ky_copy.start()

    loads[2].wait()
    loads[3].wait()
    pack(lambda i: (X0[0, pl.ds(rowsof(i + 1), NZ), :], X0[1, pl.ds(rowsof(i + 1), NZ), :]), PKS.at[0])
    x0_copy = remote(PKS.at[0], H.at[0], is_s.at[7], is_r.at[7], to_y)
    x0_copy.start()

    for cp in loads[4:10]:
        cp.wait()

    keep_x = jnp.where(has_hi, 1.0, 0.0)
    for t in range(2):
        KX[t, pl.ds(BODY, NZ), :] = KX[t, pl.ds(BODY, NZ), :] * keep_x
    dead_y = last & (py == 1)
    dead_z = row24 == NZ - 1

    def mask_step(i, acc):
        s1, s2, kx1, ky1, kz1, k2 = acc
        r = rowsof(i)
        for t in range(2):
            s = D[t, pl.ds(r, NZ), :]
            kx = KX[t, pl.ds(r + NZ, NZ), :]
            ky = KY[t, pl.ds(r, NZ), :]
            kz = jnp.where(dead_z, 0.0, KZ[t, pl.ds(r + 8, NZ), :])
            if t == 1:
                ky = jnp.where(dead_y, 0.0, ky)
                KY[t, pl.ds(r, NZ), :] = ky
            KZ[t, pl.ds(r + 8, NZ), :] = kz
            s1, s2 = s1 + s, s2 + s * s
            kx1, ky1, kz1 = kx1 + kx, ky1 + ky, kz1 + kz
            k2 = k2 + (kx * kx + ky * ky + kz * kz)
        return s1, s2, kx1, ky1, kz1, k2

    sums = lax.fori_loop(0, NX, mask_step, (jnp.zeros((NZ, 128), jnp.float32),) * 6)
    stats = jnp.zeros((8, 128), jnp.float32)
    for n, v in enumerate(sums):
        stats = jnp.where((row == 2) & (lane == n), full_sum(v), stats)

    def sum_copies(e):
        return [remote(RS.at[e], RR.at[e, me], rs.at[e, n], rr.at[e],
                       (lax.rem(py + dy, 2), lax.rem(px + dx, 4))) for n, (dy, dx) in enumerate(OTHERS)]

    def sum_send(e, tile):
        RS[e] = tile
        RR[e, me] = tile
        for cp in sum_copies(e):
            cp.start()

    def sum_take(e):
        pltpu.make_async_copy(RR.at[e, pl.ds(0, 7)], RR.at[e, pl.ds(0, 7)], rr.at[e]).wait()
        total = RR[e, 0]
        for n in range(1, 8):
            total = total + RR[e, n]
        return total

    sum_send(0, stats)

    def up_copy(k):
        return remote(Z.at[k, :, pl.ds(BODY, NZ), :], Z.at[k, :, pl.ds(0, NZ), :], hs.at[k, 0], hr.at[k, 0], to_x(1))

    def down_copy(k):
        return remote(Z.at[k, :, pl.ds(NZ, NZ), :], Z.at[k, :, pl.ds(HI, NZ), :], hs.at[k, 1], hr.at[k, 1], to_x(-1))

    def y_copy(k):
        return remote(PKS.at[k + 1], H.at[k + 1], hs.at[k, 2], hr.at[k, 2], to_y)

    def send_x(k):
        @pl.when(has_hi)
        def _():
            up_copy(k).start()

        @pl.when(has_lo)
        def _():
            down_copy(k).start()

    def take_halo(k):
        @pl.when(has_lo)
        def _():
            up_copy(k).wait_recv()

        @pl.when(has_hi)
        def _():
            down_copy(k).wait_recv()

        y_copy(k).wait_recv()

    def neighbours(vec, i, h, j, tile_raw, tile_k):
        r = rowsof(i)
        u = [vec(t, r + NZ) for t in range(2)]
        ky = [KY[t, pl.ds(r, NZ), :] for t in range(2)]
        up = [pltpu.roll(u[t], 127, 1) for t in range(2)]
        down = [pltpu.roll(ky[t] * u[t], 1, 1) for t in range(2)]
        y_up = [jnp.where(last, up[1], up[0]), jnp.where(last, unpack(tile_raw, j), up[1])]
        y_down = [jnp.where(first, unpack(tile_k, j), down[0]), jnp.where(first, down[0], down[1])]
        out = []
        for t in range(2):
            part = ky[t] * y_up[t] + y_down[t]
            part = part + KX[t, pl.ds(r + NZ, NZ), :] * vec(t, r + 2 * NZ)
            part = part + KX[t, pl.ds(r, NZ), :] * vec(t, r)
            part = part + KZ[t, pl.ds(r + 8, NZ), :] * vec(t, r + NZ + 1)
            part = part + KZ[t, pl.ds(r + 7, NZ), :] * vec(t, r + NZ - 1)
            out.append(part)
        return u, out

    @pl.when(has_lo)
    def _():
        for t in range(2):
            for cp in init_up(t):
                cp.wait_recv()

    @pl.when(has_hi)
    def _():
        for t in range(2):
            for cp in init_down(t):
                cp.wait_recv()

    @pl.when(py == 1)
    def _():
        ky_copy.wait_recv()

    x0_copy.wait_recv()
    for h in range(2):
        HK[h] = H[0, h] * KYH[h]
    loads[10].wait()
    loads[11].wait()

    def start_plane(i, h, carry):
        acc, rho = carry
        j = i - 32 * h
        r = rowsof(i)
        u, nb = neighbours(lambda t, q: X0[t, pl.ds(q, NZ), :], i, h, j, H[0, h], HK[h])
        down = [pltpu.roll(KY[t, pl.ds(r, NZ), :], 1, 1) for t in range(2)]
        ky_lo = [jnp.where(first, unpack(KYH[h], j), down[0]), jnp.where(first, down[0], down[1])]
        new = []
        for t in range(2):
            diag = D[t, pl.ds(r, NZ), :] + KY[t, pl.ds(r, NZ), :] + ky_lo[t]
            diag = diag + KX[t, pl.ds(r + NZ, NZ), :] + KX[t, pl.ds(r, NZ), :]
            diag = diag + KZ[t, pl.ds(r + 8, NZ), :] + KZ[t, pl.ds(r + 7, NZ), :]
            D[t, pl.ds(r, NZ), :] = diag
            res = Z[0, t, pl.ds(r + NZ, NZ), :] - (diag * u[t] - nb[t])
            Z[0, t, pl.ds(r + NZ, NZ), :] = res
            rho = rho + res * res
            new.append(res)
        return pack_into(acc, j, new[0], new[1]), rho

    def sweep(plane, k, sums0, more=None):
        zero = jnp.zeros((8, 128), jnp.float32)
        acc0, sums1 = plane(0, 0, (zero, sums0))
        acc1, sums1 = plane(NX - 1, 1, (zero, sums1))
        if more is None:
            send_x(k)
        else:
            @pl.when(more)
            def _():
                send_x(k)
        acc0, sums1 = lax.fori_loop(1, 32, lambda i, c: plane(i, 0, c), (acc0, sums1))
        acc1, sums1 = lax.fori_loop(32, NX - 1, lambda i, c: plane(i, 1, c), (acc1, sums1))
        PKS[k + 1, 0] = acc0
        PKS[k + 1, 1] = acc1
        if more is None:
            y_copy(k).start()
        else:
            @pl.when(more)
            def _():
                y_copy(k).start()
        return sums1

    zero24 = jnp.zeros((NZ, 128), jnp.float32)
    rho0 = sweep(lambda i, h, c: start_plane(i, h, c), 0, zero24)
    PT[...] = jnp.where((row == 0) & (lane == 0), full_sum(rho0), 0.0)

    for n in range(20):
        ST[n] = jnp.zeros((8, 128), jnp.float32)
    totals = sum_take(0)
    cells = float(NX * 256 * NZ * 8)
    mean = [full_sum(jnp.where((row == 2) & (lane == n), totals, 0.0)) * (1.0 / cells) for n in range(6)]
    var_s = jnp.maximum(mean[1] - mean[0] * mean[0], 0.0)
    var_k = jnp.maximum(mean[5] - mean[2] * mean[2] - mean[3] * mean[3] - mean[4] * mean[4], 0.0)
    b_first = jnp.sqrt(3.0 * mean[5] + 1.5 * (var_s + 2.0 * var_k))
    a_first = jnp.maximum(mean[0] - 0.5 * jnp.sqrt(var_s), 0.3) + 2.0 * b_first

    def set_coefs(k0, a_new, b_new):
        old_b = ST[S_B]
        b_arr = jnp.where(lane >= k0, b_new, old_b)
        ST[S_A] = jnp.where(lane >= k0, a_new, ST[S_A])
        ST[S_B] = b_arr
        ST[S_C] = jnp.where(lane == 0, 0.0, pltpu.roll(b_arr, 1, 1))
        inv = 1.0 / b_new
        for k in range(k0, ITERS):
            CO[k, 0] = a_new
            if k > k0:
                CO[k, 1] = b_new
            elif k == 0:
                CO[k, 1] = jnp.zeros((8, 128), jnp.float32)
            else:
                CO[k, 1] = CO[k - 1, 3]
            CO[k, 2] = inv
            CO[k, 3] = b_new

    set_coefs(0, a_first, b_first)

    def gram_start(total):
        rho = full_sum(jnp.where((row == 0) & (lane == 0), total, 0.0))
        one = jnp.where(lane == 0, 1.0, 0.0)
        ST[S_G] = one * rho
        ST[S_CL] = one
        ST[S_DL] = one
        ST[S_LEAD] = jnp.ones((8, 128), jnp.float32)
        ST[S_RHO] = rho
        ST[S_RHO0] = rho
        ST[S_HIST] = one * rho

    def gram_load(total):
        ST[S_D] = jnp.broadcast_to(total[0:1], (8, 128))
        ST[S_E] = jnp.broadcast_to(total[1:2], (8, 128))

    def gram_step(k):
        a, b, c = ST[S_A], ST[S_B], ST[S_C]
        g, gp, cl, dl = ST[S_G], ST[S_GP], ST[S_CL], ST[S_DL]
        e_row, d_row = ST[S_E], ST[S_D]
        rho, lead = ST[S_RHO], ST[S_LEAD]
        b_k, c_k, a_k = CO[k, 3], CO[k, 1], CO[k, 0]
        at_k, at_k1 = lane == k, lane == k + 1
        rec = ((a - a_k) * g + b * pltpu.roll(g, 127, 1)
               + c * pltpu.roll(g, 1, 1) - c_k * gp) * CO[k, 2]
        g_new = jnp.where(lane < k, rec, jnp.where(at_k, e_row, jnp.where(at_k1, d_row, 0.0)))
        g_full = jnp.where(at_k1, pltpu.roll(e_row, 1, 1), g)
        image = a * dl + pltpu.roll(b * dl, 1, 1) + pltpu.roll(c * dl, 127, 1)
        delta = lead * lane_sum(image * g_full)
        alpha = rho / delta
        y = ST[S_Y] + alpha * dl
        cl = cl - alpha * image
        lead = -alpha * b_k * lead
        prod = cl * g_new
        rho_new = lead * lane_sum(prod)
        size = jnp.abs(lead) * lane_sum(jnp.abs(prod))
        beta = rho_new / rho
        dl = cl + beta * dl
        ST[S_G], ST[S_GP], ST[S_CL], ST[S_DL] = g_new, g, cl, dl
        ST[S_Y], ST[S_RHO], ST[S_LEAD] = y, rho_new, lead
        ST[S_HIST] = jnp.where(at_k1, rho_new, ST[S_HIST])
        inv_alpha = 1.0 / alpha
        ST[S_LA2], ST[S_LB2] = ST[S_LA], ST[S_LB]
        ST[S_LA] = inv_alpha + ST[S_BA]
        ST[S_LB] = jnp.sqrt(jnp.abs(beta)) * inv_alpha
        ST[S_BA] = beta * inv_alpha
        err = size / jnp.abs(rho_new) * jnp.sqrt(jnp.abs(rho_new) / ST[S_RHO0])
        err = jnp.where(rho_new > 0.0, err, 1e30)
        ST[S_ERR] = jnp.maximum(ST[S_ERR], jnp.where(err < 1e30, err, 1e30))

    def renew(k0):
        a_new = 0.5 * (ST[S_LA] + ST[S_LA2])
        b_new = 0.5 * (ST[S_LB] + ST[S_LB2])
        a_ok = (a_new > 0.3) & (a_new < 26.8)
        a_new = jnp.where(a_ok, a_new, a_first)
        b_new = jnp.where(a_ok & (b_new > 0.25 * b_first) & (b_new < 2.0 * b_first), b_new, b_first)
        set_coefs(k0, a_new, b_new)

    def apply_step(k):
        take_halo(k)
        for h in range(2):
            HK[h] = H[k + 1, h] * KYH[h]
        a_k, c_k, i_k = three(CO[k, 0]), three(CO[k, 1]), three(CO[k, 2])
        before = jnp.maximum(k - 1, 0)

        def plane(i, h, carry):
            acc, (dots, cross) = carry
            j = i - 32 * h
            r = rowsof(i)
            u, nb = neighbours(lambda t, q: Z[k, t, pl.ds(q, NZ), :], i, h, j, H[k + 1, h], HK[h])
            new = []
            for t in range(2):
                val = (D[t, pl.ds(r, NZ), :] - a_k) * u[t] - nb[t] - c_k * Z[before, t, pl.ds(r + NZ, NZ), :]
                val = val * i_k
                Z[k + 1, t, pl.ds(r + NZ, NZ), :] = val
                dots = dots + val * val
                cross = cross + val * u[t]
                new.append(val)
            return pack_into(acc, j, new[0], new[1]), (dots, cross)

        dots, cross = sweep(plane, k + 1, (zero24, zero24), k < ITERS - 1)
        tile = jnp.where((row == 0) & (lane == k + 1), full_sum(dots), PT[...])
        tile = jnp.where((row == 1) & (lane == k), full_sum(cross), tile)
        PT[...] = tile
        for e, at in SEND_AT.items():
            @pl.when(k == at)
            def _():
                sum_send(e, tile)
        for at, e in TAKE_AT.items():
            @pl.when(k == at)
            def _():
                total = sum_take(e)
                gram_load(total)
                if e == 1:
                    gram_start(total)
        for at, (lo, hi) in STEPS_AT.items():
            @pl.when(k == at)
            def _():
                @pl.loop(lo, hi)
                def _(s):
                    gram_step(s)
        for at, k0 in RENEW_AT.items():
            @pl.when(k == at)
            def _():
                renew(k0)

    @pl.loop(0, ITERS)
    def _(k):
        apply_step(k)

    gram_load(sum_take(4))

    @pl.loop(16, ITERS)
    def _(s):
        gram_step(s)

    y = ST[S_Y]
    for k in range(ITERS):
        YB[k] = lane_sum(jnp.where(lane == k, y, 0.0))
    hist = jnp.sqrt(ST[S_HIST] * (1.0 / cells))
    hist_ref[...] = jnp.where(row == 0, hist, ST[S_ERR])

    def combine(i, c):
        r = rowsof(i + 1)
        acc = [X0[t, pl.ds(r, NZ), :] for t in range(2)]
        for k in range(ITERS):
            w = three(YB[k])
            for t in range(2):
                acc[t] = acc[t] + w * Z[k, t, pl.ds(r, NZ), :]
        for t in range(2):
            X0[t, pl.ds(r, NZ), :] = acc[t]
        return c

    outs = []
    for part in range(4):
        lax.fori_loop(16 * part, 16 * part + 16, combine, 0)
        for t in range(2):
            cp = pltpu.make_async_copy(X0.at[t, pl.ds(NZ + 16 * NZ * part, 16 * NZ), :],
                                       out_h.at[pl.ds(16 * NZ * part, 16 * NZ), pl.ds(128 * t, 128)],
                                       osem.at[2 * part + t])
            cp.start()
            outs.append(cp)

    @pl.when(has_hi)
    def _():
        for t in range(2):
            for cp in init_up(t):
                cp.wait_send()

    @pl.when(has_lo)
    def _():
        for t in range(2):
            for cp in init_down(t):
                cp.wait_send()

    @pl.when(py == 0)
    def _():
        ky_copy.wait_send()

    x0_copy.wait_send()

    @pl.loop(0, ITERS)
    def _(k):
        @pl.when(has_hi)
        def _():
            up_copy(k).wait_send()

        @pl.when(has_lo)
        def _():
            down_copy(k).wait_send()

        y_copy(k).wait_send()

    for e in range(5):
        for cp in sum_copies(e):
            cp.wait_send()
    for cp in outs:
        cp.wait()


def fused_solve(shift, rhs_field, x_init, cond_x, cond_y, cond_z):
    def flat(v):
        return jnp.transpose(v, (0, 2, 1)).reshape(BODY, 256)

    f32 = jnp.float32
    any_spec = pl.BlockSpec(memory_space=pl.ANY)
    x_rows, small = pl.pallas_call(
        kernel,
        out_shape=(jax.ShapeDtypeStruct((BODY, 256), f32), jax.ShapeDtypeStruct((8, 128), f32)),
        in_specs=[any_spec] * 6,
        out_specs=(any_spec, pl.BlockSpec(memory_space=pltpu.VMEM)),
        scratch_shapes=[
            pltpu.VMEM((ITERS + 1, 2, FULL, 128), f32),
            pltpu.VMEM((2, FULL, 128), f32),
            pltpu.VMEM((2, BODY, 128), f32),
            pltpu.VMEM((2, BODY + NZ, 128), f32),
            pltpu.VMEM((2, BODY, 128), f32),
            pltpu.VMEM((2, BODY + 8, 128), f32),
            pltpu.VMEM((ITERS + 2, 2, 8, 128), f32),
            pltpu.VMEM((ITERS + 2, 2, 8, 128), f32),
            pltpu.VMEM((2, 8, 128), f32),
            pltpu.VMEM((2, 8, 128), f32),
            pltpu.VMEM((2, 8, 128), f32),
            pltpu.VMEM((5, 8, 128), f32),
            pltpu.VMEM((5, 8, 8, 128), f32),
            pltpu.VMEM((8, 128), f32),
            pltpu.VMEM((20, 8, 128), f32),
            pltpu.VMEM((ITERS, 4, 8, 128), f32),
            pltpu.VMEM((ITERS, 8, 128), f32),
            pltpu.SemaphoreType.DMA((12,)),
            pltpu.SemaphoreType.DMA((8,)),
            pltpu.SemaphoreType.DMA((8,)),
            pltpu.SemaphoreType.DMA((8,)),
            pltpu.SemaphoreType.DMA((ITERS, 3)),
            pltpu.SemaphoreType.DMA((ITERS, 3)),
            pltpu.SemaphoreType.DMA((5, 7)),
            pltpu.SemaphoreType.DMA((5,)),
        ],
        compiler_params=pltpu.CompilerParams(collective_id=0, has_side_effects=True,
                                             vmem_limit_bytes=60 * 1024 * 1024),
    )(*(flat(v) for v in (shift, rhs_field, x_init, cond_x, cond_y, cond_z)))
    x_out = jnp.transpose(x_rows.reshape(NX, NZ, 256), (0, 2, 1))
    return x_out, small[0, :ITERS + 1], small[1, 0]


def solution(mesh):
    field_spec = P("px", "py", None)

    def local_solve(*fields):
        x_out, history, _ = fused_solve(*fields)
        return x_out, history

    return jax.shard_map(local_solve, mesh=mesh, in_specs=(field_spec,) * 6,
                         out_specs=(field_spec, P()), check_vma=False)
```

```python
import functools

import jax
import jax.numpy as jnp
from jax import lax
from jax.experimental import pallas as pl
from jax.experimental.pallas import tpu as pltpu
from jax.sharding import PartitionSpec as P

ITERS = 20
SUM_AXES = ("px", "py")
MESH = pl.DeviceIdType.MESH
NX, NZ = 64, 24
BODY = NX * NZ
FULL = BODY + 2 * NZ
HI = BODY + NZ
OTHERS = tuple((dy, dx) for dy in range(2) for dx in range(4) if (dy, dx) != (0, 0))
SEND_AT = {1: 4, 2: 9, 3: 15, 4: 19}
TAKE_AT = {6: 1, 11: 2, 17: 3}
STEPS_AT = {6: (0, 2), 7: (2, 4), 8: (4, 5), 11: (5, 7), 12: (7, 9), 13: (9, 10),
            17: (10, 12), 18: (12, 14), 19: (14, 16)}
RENEW_AT = {8: 9, 13: 14}
S_A, S_B, S_C, S_GP, S_G, S_CL, S_DL, S_Y, S_RHO, S_LEAD, S_HIST, S_BA, S_LA, S_LB, S_LA2, S_LB2, S_ERR, S_D, S_E, S_RHO0 = range(20)


def lanes():
    return lax.broadcasted_iota(jnp.int32, (8, 128), 1)


def rows8():
    return lax.broadcasted_iota(jnp.int32, (8, 128), 0)


def lane_sum(v):
    return jnp.broadcast_to(jnp.sum(v, axis=1, keepdims=True), (8, 128))


def full_sum(v):
    return jnp.broadcast_to(jnp.sum(jnp.sum(v, axis=0, keepdims=True), axis=1, keepdims=True), (8, 128))


def three(v):
    return jnp.concatenate([v, v, v], axis=0)


def kernel(s_h, b_h, x0_h, kx_h, ky_h, kz_h, out_h, hist_ref,
           Z, X0, D, KX, KY, KZ, PKS, H, KYP, KYH, HK, RS, RR, PT, ST, CO, YB,
           lsem, osem, is_s, is_r, hs, hr, rs, rr):
    px, py = lax.axis_index("px"), lax.axis_index("py")
    me = py * 4 + px
    lane, row = lanes(), rows8()
    lane24 = lax.broadcasted_iota(jnp.int32, (24, 128), 1)
    row24 = lax.broadcasted_iota(jnp.int32, (24, 128), 0)
    first, last = lane24 == 0, lane24 == 127
    has_lo, has_hi = px > 0, px < 3

    loads = []
    for n, (src, dst, base) in enumerate((
            (ky_h, KY, 0), (x0_h, X0, NZ), (kx_h, KX, NZ), (kz_h, KZ, 8), (s_h, D, 0), (b_h, None, NZ))):
        for t in range(2):
            to = Z.at[0, t, pl.ds(base, BODY), :] if dst is None else dst.at[t, pl.ds(base, BODY), :]
            cp = pltpu.make_async_copy(src.at[:, pl.ds(128 * t, 128)], to, lsem.at[2 * n + t])
            cp.start()
            loads.append(cp)

    zero_plane = jnp.zeros((NZ, 128), jnp.float32)
    for t in range(2):
        KX[t, pl.ds(0, NZ), :] = zero_plane
        X0[t, pl.ds(0, NZ), :] = zero_plane
        X0[t, pl.ds(HI, NZ), :] = zero_plane
        KZ[t, pl.ds(0, 8), :] = jnp.zeros((8, 128), jnp.float32)
    KYH[...] = jnp.zeros((2, 8, 128), jnp.float32)

    @pl.loop(0, ITERS + 1)
    def _(k):
        for t in range(2):
            Z[k, t, pl.ds(0, NZ), :] = zero_plane
            Z[k, t, pl.ds(HI, NZ), :] = zero_plane

    barrier = pltpu.get_barrier_semaphore()
    for dy, dx in OTHERS:
        pl.semaphore_signal(barrier, inc=1, device_id=(lax.rem(py + dy, 2), lax.rem(px + dx, 4)),
                            device_id_type=MESH)
    pl.semaphore_wait(barrier, len(OTHERS))

    def to_x(step):
        return (py, px + step)

    to_y = (1 - py, px)

    def remote(src, dst, ssem, rsem, dev):
        return pltpu.make_async_remote_copy(src_ref=src, dst_ref=dst, send_sem=ssem, recv_sem=rsem,
                                            device_id=dev, device_id_type=MESH)

    def init_up(t):
        cols = pl.ds(128 * t, 128)
        return (remote(kx_h.at[pl.ds(BODY - NZ, NZ), cols], KX.at[t, pl.ds(0, NZ), :], is_s.at[t], is_r.at[t], to_x(1)),
                remote(x0_h.at[pl.ds(BODY - NZ, NZ), cols], X0.at[t, pl.ds(0, NZ), :], is_s.at[2 + t], is_r.at[2 + t], to_x(1)))

    def init_down(t):
        cols = pl.ds(128 * t, 128)
        return (remote(x0_h.at[pl.ds(0, NZ), cols], X0.at[t, pl.ds(HI, NZ), :], is_s.at[4 + t], is_r.at[4 + t], to_x(-1)),)

    @pl.when(has_hi)
    def _():
        for t in range(2):
            for cp in init_up(t):
                cp.start()

    @pl.when(has_lo)
    def _():
        for t in range(2):
            for cp in init_down(t):
                cp.start()

    off = 1 - py

    def pack_into(acc, j, lo, hi):
        v = jnp.where(py == 0, hi, lo)
        for q in range(3):
            at = 3 * j + q
            moved = pltpu.roll(v[8 * q:8 * q + 8], lax.rem(at + 2 * off, 128), 1)
            acc = jnp.where(lane == at + off, moved, acc)
        return acc

    def pack(read, dst):
        for h in range(2):
            accs = [jnp.zeros((8, 128), jnp.float32)] * 4
            for j in range(32):
                lo, hi = read(32 * h + j)
                accs[j % 4] = pack_into(accs[j % 4], j, lo, hi)
            dst[h] = (accs[0] + accs[1]) + (accs[2] + accs[3])

    def unpack(tile, j):
        parts = [pltpu.roll(tile, 127 - (3 * j + q), 1) for q in range(3)]
        return jnp.concatenate(parts, axis=0)

    def rowsof(i):
        return pl.multiple_of(NZ * i, 8)

    loads[0].wait()
    loads[1].wait()
    pack(lambda i: (KY[0, pl.ds(rowsof(i), NZ), :], KY[1, pl.ds(rowsof(i), NZ), :]), KYP)
    ky_copy = remote(KYP, KYH, is_s.at[6], is_r.at[6], to_y)

    @pl.when(py == 0)
    def _():
        ky_copy.start()

    loads[2].wait()
    loads[3].wait()
    pack(lambda i: (X0[0, pl.ds(rowsof(i + 1), NZ), :], X0[1, pl.ds(rowsof(i + 1), NZ), :]), PKS.at[0])
    x0_copy = remote(PKS.at[0], H.at[0], is_s.at[7], is_r.at[7], to_y)
    x0_copy.start()

    for cp in loads[4:10]:
        cp.wait()

    keep_x = jnp.where(has_hi, 1.0, 0.0)
    for t in range(2):
        KX[t, pl.ds(BODY, NZ), :] = KX[t, pl.ds(BODY, NZ), :] * keep_x
    dead_y = last & (py == 1)
    dead_z = row24 == NZ - 1

    def mask_step(i, acc):
        s1, s2, kx1, ky1, kz1, k2 = acc
        r = rowsof(i)
        for t in range(2):
            s = D[t, pl.ds(r, NZ), :]
            kx = KX[t, pl.ds(r + NZ, NZ), :]
            ky = KY[t, pl.ds(r, NZ), :]
            kz = jnp.where(dead_z, 0.0, KZ[t, pl.ds(r + 8, NZ), :])
            if t == 1:
                ky = jnp.where(dead_y, 0.0, ky)
                KY[t, pl.ds(r, NZ), :] = ky
            KZ[t, pl.ds(r + 8, NZ), :] = kz
            s1, s2 = s1 + s, s2 + s * s
            kx1, ky1, kz1 = kx1 + kx, ky1 + ky, kz1 + kz
            k2 = k2 + (kx * kx + ky * ky + kz * kz)
        return s1, s2, kx1, ky1, kz1, k2

    sums = lax.fori_loop(0, NX, mask_step, (jnp.zeros((NZ, 128), jnp.float32),) * 6)
    stats = jnp.zeros((8, 128), jnp.float32)
    for n, v in enumerate(sums):
        stats = jnp.where((row == 2) & (lane == n), full_sum(v), stats)

    def sum_copies(e):
        return [remote(RS.at[e], RR.at[e, me], rs.at[e, n], rr.at[e],
                       (lax.rem(py + dy, 2), lax.rem(px + dx, 4))) for n, (dy, dx) in enumerate(OTHERS)]

    def sum_send(e, tile):
        RS[e] = tile
        RR[e, me] = tile
        for cp in sum_copies(e):
            cp.start()

    def sum_take(e):
        pltpu.make_async_copy(RR.at[e, pl.ds(0, 7)], RR.at[e, pl.ds(0, 7)], rr.at[e]).wait()
        total = RR[e, 0]
        for n in range(1, 8):
            total = total + RR[e, n]
        return total

    sum_send(0, stats)

    def up_copy(k):
        return remote(Z.at[k, :, pl.ds(BODY, NZ), :], Z.at[k, :, pl.ds(0, NZ), :], hs.at[k, 0], hr.at[k, 0], to_x(1))

    def down_copy(k):
        return remote(Z.at[k, :, pl.ds(NZ, NZ), :], Z.at[k, :, pl.ds(HI, NZ), :], hs.at[k, 1], hr.at[k, 1], to_x(-1))

    def y_copy(k):
        return remote(PKS.at[k + 1], H.at[k + 1], hs.at[k, 2], hr.at[k, 2], to_y)

    def send_x(k):
        @pl.when(has_hi)
        def _():
            up_copy(k).start()

        @pl.when(has_lo)
        def _():
            down_copy(k).start()

    def take_halo(k):
        @pl.when(has_lo)
        def _():
            up_copy(k).wait_recv()

        @pl.when(has_hi)
        def _():
            down_copy(k).wait_recv()

        y_copy(k).wait_recv()

    def neighbours(vec, i, j, tile_raw, tile_k):
        r = rowsof(i)
        u = [vec(t, r + NZ) for t in range(2)]
        ky = [KY[t, pl.ds(r, NZ), :] for t in range(2)]
        up = [pltpu.roll(u[t], 127, 1) for t in range(2)]
        down = [pltpu.roll(ky[t] * u[t], 1, 1) for t in range(2)]
        y_up = [jnp.where(last, up[1], up[0]), jnp.where(last, unpack(tile_raw, j), up[1])]
        y_down = [jnp.where(first, unpack(tile_k, j), down[0]), jnp.where(first, down[0], down[1])]
        out = []
        for t in range(2):
            part = ky[t] * y_up[t] + y_down[t]
            part = part + KX[t, pl.ds(r + NZ, NZ), :] * vec(t, r + 2 * NZ)
            part = part + KX[t, pl.ds(r, NZ), :] * vec(t, r)
            part = part + KZ[t, pl.ds(r + 8, NZ), :] * vec(t, r + NZ + 1)
            part = part + KZ[t, pl.ds(r + 7, NZ), :] * vec(t, r + NZ - 1)
            out.append(part)
        return u, out

    @pl.when(has_lo)
    def _():
        for t in range(2):
            for cp in init_up(t):
                cp.wait_recv()

    @pl.when(has_hi)
    def _():
        for t in range(2):
            for cp in init_down(t):
                cp.wait_recv()

    @pl.when(py == 1)
    def _():
        ky_copy.wait_recv()

    x0_copy.wait_recv()
    for h in range(2):
        HK[h] = H[0, h] * KYH[h]
    loads[10].wait()
    loads[11].wait()

    def start_plane(i, rho):
        h = i // 32
        j = lax.rem(i, 32)
        r = rowsof(i)
        u, nb = neighbours(lambda t, q: X0[t, pl.ds(q, NZ), :], i, j, H[0, h], HK[h])
        down = [pltpu.roll(KY[t, pl.ds(r, NZ), :], 1, 1) for t in range(2)]
        ky_lo = [jnp.where(first, unpack(KYH[h], j), down[0]), jnp.where(first, down[0], down[1])]
        for t in range(2):
            diag = D[t, pl.ds(r, NZ), :] + KY[t, pl.ds(r, NZ), :] + ky_lo[t]
            diag = diag + KX[t, pl.ds(r + NZ, NZ), :] + KX[t, pl.ds(r, NZ), :]
            diag = diag + KZ[t, pl.ds(r + 8, NZ), :] + KZ[t, pl.ds(r + 7, NZ), :]
            D[t, pl.ds(r, NZ), :] = diag
            res = Z[0, t, pl.ds(r + NZ, NZ), :] - (diag * u[t] - nb[t])
            Z[0, t, pl.ds(r + NZ, NZ), :] = res
            rho = rho + res * res
        return rho

    UNROLL = 6

    def sweep(plane, k, sums1, more):
        sums1 = plane(0, sums1)
        sums1 = plane(NX - 1, sums1)

        @pl.when(more)
        def _():
            send_x(k)

        sums1 = plane(1, sums1)
        sums1 = plane(NX - 2, sums1)
        sums1 = lax.fori_loop(0, 60 // UNROLL, lambda m, c: functools.reduce(
            lambda d, n: plane(2 + UNROLL * m + n, d), range(UNROLL), c), sums1)

        @pl.when(more)
        def _():
            pack(lambda i: (Z[k, 0, pl.ds(rowsof(i + 1), NZ), :], Z[k, 1, pl.ds(rowsof(i + 1), NZ), :]), PKS.at[k + 1])
            y_copy(k).start()

        return sums1

    zero24 = jnp.zeros((NZ, 128), jnp.float32)
    rho0 = sweep(start_plane, 0, zero24, px >= 0)
    PT[...] = jnp.where((row == 0) & (lane == 0), full_sum(rho0), 0.0)

    for n in range(20):
        ST[n] = jnp.zeros((8, 128), jnp.float32)
    totals = sum_take(0)
    cells = float(NX * 256 * NZ * 8)
    mean = [full_sum(jnp.where((row == 2) & (lane == n), totals, 0.0)) * (1.0 / cells) for n in range(6)]
    var_s = jnp.maximum(mean[1] - mean[0] * mean[0], 0.0)
    var_k = jnp.maximum(mean[5] - mean[2] * mean[2] - mean[3] * mean[3] - mean[4] * mean[4], 0.0)
    b_first = jnp.sqrt(3.0 * mean[5] + 1.5 * (var_s + 2.0 * var_k))
    a_first = jnp.maximum(mean[0] - 0.5 * jnp.sqrt(var_s), 0.3) + 2.0 * b_first

    def set_coefs(k0, a_new, b_new):
        old_b = ST[S_B]
        b_arr = jnp.where(lane >= k0, b_new, old_b)
        ST[S_A] = jnp.where(lane >= k0, a_new, ST[S_A])
        ST[S_B] = b_arr
        ST[S_C] = jnp.where(lane == 0, 0.0, pltpu.roll(b_arr, 1, 1))
        inv = 1.0 / b_new
        for k in range(k0, ITERS):
            CO[k, 0] = a_new
            if k > k0:
                CO[k, 1] = b_new
            elif k == 0:
                CO[k, 1] = jnp.zeros((8, 128), jnp.float32)
            else:
                CO[k, 1] = CO[k - 1, 3]
            CO[k, 2] = inv
            CO[k, 3] = b_new

    set_coefs(0, a_first, b_first)

    def gram_start(total):
        rho = full_sum(jnp.where((row == 0) & (lane == 0), total, 0.0))
        one = jnp.where(lane == 0, 1.0, 0.0)
        ST[S_G] = one * rho
        ST[S_CL] = one
        ST[S_DL] = one
        ST[S_LEAD] = jnp.ones((8, 128), jnp.float32)
        ST[S_RHO] = rho
        ST[S_RHO0] = rho
        ST[S_HIST] = one * rho

    def gram_load(total):
        ST[S_D] = jnp.broadcast_to(total[0:1], (8, 128))
        ST[S_E] = jnp.broadcast_to(total[1:2], (8, 128))

    def gram_step(k):
        a, b, c = ST[S_A], ST[S_B], ST[S_C]
        g, gp, cl, dl = ST[S_G], ST[S_GP], ST[S_CL], ST[S_DL]
        e_row, d_row = ST[S_E], ST[S_D]
        rho, lead = ST[S_RHO], ST[S_LEAD]
        b_k, c_k, a_k = CO[k, 3], CO[k, 1], CO[k, 0]
        at_k, at_k1 = lane == k, lane == k + 1
        rec = ((a - a_k) * g + b * pltpu.roll(g, 127, 1)
               + c * pltpu.roll(g, 1, 1) - c_k * gp) * CO[k, 2]
        g_new = jnp.where(lane < k, rec, jnp.where(at_k, e_row, jnp.where(at_k1, d_row, 0.0)))
        g_full = jnp.where(at_k1, pltpu.roll(e_row, 1, 1), g)
        image = a * dl + pltpu.roll(b * dl, 1, 1) + pltpu.roll(c * dl, 127, 1)
        delta = lead * lane_sum(image * g_full)
        alpha = rho / delta
        y = ST[S_Y] + alpha * dl
        cl = cl - alpha * image
        lead = -alpha * b_k * lead
        prod = cl * g_new
        rho_new = lead * lane_sum(prod)
        size = jnp.abs(lead) * lane_sum(jnp.abs(prod))
        beta = rho_new / rho
        dl = cl + beta * dl
        ST[S_G], ST[S_GP], ST[S_CL], ST[S_DL] = g_new, g, cl, dl
        ST[S_Y], ST[S_RHO], ST[S_LEAD] = y, rho_new, lead
        ST[S_HIST] = jnp.where(at_k1, rho_new, ST[S_HIST])
        inv_alpha = 1.0 / alpha
        ST[S_LA2], ST[S_LB2] = ST[S_LA], ST[S_LB]
        ST[S_LA] = inv_alpha + ST[S_BA]
        ST[S_LB] = jnp.sqrt(jnp.abs(beta)) * inv_alpha
        ST[S_BA] = beta * inv_alpha
        err = size / jnp.abs(rho_new) * jnp.sqrt(jnp.abs(rho_new) / ST[S_RHO0])
        err = jnp.where(rho_new > 0.0, err, 1e30)
        ST[S_ERR] = jnp.maximum(ST[S_ERR], jnp.where(err < 1e30, err, 1e30))

    def renew(k0):
        a_new = 0.5 * (ST[S_LA] + ST[S_LA2])
        b_new = 0.5 * (ST[S_LB] + ST[S_LB2])
        a_ok = (a_new > 0.3) & (a_new < 26.8)
        a_new = jnp.where(a_ok, a_new, a_first)
        b_new = jnp.where(a_ok & (b_new > 0.25 * b_first) & (b_new < 2.0 * b_first), b_new, b_first)
        set_coefs(k0, a_new, b_new)

    def apply_step(k):
        take_halo(k)
        for h in range(2):
            HK[h] = H[k + 1, h] * KYH[h]
        a_k, c_k, i_k = three(CO[k, 0]), three(CO[k, 1]), three(CO[k, 2])
        before = jnp.maximum(k - 1, 0)

        def plane(i, carry):
            dots, cross = carry
            h = i // 32
            j = lax.rem(i, 32)
            r = rowsof(i)
            u, nb = neighbours(lambda t, q: Z[k, t, pl.ds(q, NZ), :], i, j, H[k + 1, h], HK[h])
            for t in range(2):
                val = (D[t, pl.ds(r, NZ), :] - a_k) * u[t] - nb[t] - c_k * Z[before, t, pl.ds(r + NZ, NZ), :]
                val = val * i_k
                Z[k + 1, t, pl.ds(r + NZ, NZ), :] = val
                dots = dots + val * val
                cross = cross + val * u[t]
            return dots, cross

        dots, cross = sweep(plane, k + 1, (zero24, zero24), k < ITERS - 1)
        tile = jnp.where((row == 0) & (lane == k + 1), full_sum(dots), PT[...])
        tile = jnp.where((row == 1) & (lane == k), full_sum(cross), tile)
        PT[...] = tile
        for e, at in SEND_AT.items():
            @pl.when(k == at)
            def _():
                sum_send(e, tile)
        for at, e in TAKE_AT.items():
            @pl.when(k == at)
            def _():
                total = sum_take(e)
                gram_load(total)
                if e == 1:
                    gram_start(total)
        for at, (lo, hi) in STEPS_AT.items():
            @pl.when(k == at)
            def _():
                @pl.loop(lo, hi)
                def _(s):
                    gram_step(s)
        for at, k0 in RENEW_AT.items():
            @pl.when(k == at)
            def _():
                renew(k0)

    @pl.loop(0, ITERS)
    def _(k):
        apply_step(k)

    gram_load(sum_take(4))

    @pl.loop(16, ITERS)
    def _(s):
        gram_step(s)

    y = ST[S_Y]
    for k in range(ITERS):
        YB[k] = lane_sum(jnp.where(lane == k, y, 0.0))
    hist = jnp.sqrt(ST[S_HIST] * (1.0 / cells))
    hist_ref[...] = jnp.where(row == 0, hist, ST[S_ERR])

    def combine(i, c):
        r = rowsof(i + 1)
        acc = [X0[t, pl.ds(r, NZ), :] for t in range(2)]
        for k in range(ITERS):
            w = three(YB[k])
            for t in range(2):
                acc[t] = acc[t] + w * Z[k, t, pl.ds(r, NZ), :]
        for t in range(2):
            X0[t, pl.ds(r, NZ), :] = acc[t]
        return c

    outs = []
    for part in range(4):
        lax.fori_loop(16 * part, 16 * part + 16, combine, 0)
        for t in range(2):
            cp = pltpu.make_async_copy(X0.at[t, pl.ds(NZ + 16 * NZ * part, 16 * NZ), :],
                                       out_h.at[pl.ds(16 * NZ * part, 16 * NZ), pl.ds(128 * t, 128)],
                                       osem.at[2 * part + t])
            cp.start()
            outs.append(cp)

    @pl.when(has_hi)
    def _():
        for t in range(2):
            for cp in init_up(t):
                cp.wait_send()

    @pl.when(has_lo)
    def _():
        for t in range(2):
            for cp in init_down(t):
                cp.wait_send()

    @pl.when(py == 0)
    def _():
        ky_copy.wait_send()

    x0_copy.wait_send()

    @pl.loop(0, ITERS)
    def _(k):
        @pl.when(has_hi)
        def _():
            up_copy(k).wait_send()

        @pl.when(has_lo)
        def _():
            down_copy(k).wait_send()

        y_copy(k).wait_send()

    for e in range(5):
        for cp in sum_copies(e):
            cp.wait_send()
    for cp in outs:
        cp.wait()


def fused_solve(shift, rhs_field, x_init, cond_x, cond_y, cond_z):
    def flat(v):
        return jnp.transpose(v, (0, 2, 1)).reshape(BODY, 256)

    f32 = jnp.float32
    any_spec = pl.BlockSpec(memory_space=pl.ANY)
    x_rows, small = pl.pallas_call(
        kernel,
        out_shape=(jax.ShapeDtypeStruct((BODY, 256), f32), jax.ShapeDtypeStruct((8, 128), f32)),
        in_specs=[any_spec] * 6,
        out_specs=(any_spec, pl.BlockSpec(memory_space=pltpu.VMEM)),
        scratch_shapes=[
            pltpu.VMEM((ITERS + 1, 2, FULL, 128), f32),
            pltpu.VMEM((2, FULL, 128), f32),
            pltpu.VMEM((2, BODY, 128), f32),
            pltpu.VMEM((2, BODY + NZ, 128), f32),
            pltpu.VMEM((2, BODY, 128), f32),
            pltpu.VMEM((2, BODY + 8, 128), f32),
            pltpu.VMEM((ITERS + 2, 2, 8, 128), f32),
            pltpu.VMEM((ITERS + 2, 2, 8, 128), f32),
            pltpu.VMEM((2, 8, 128), f32),
            pltpu.VMEM((2, 8, 128), f32),
            pltpu.VMEM((2, 8, 128), f32),
            pltpu.VMEM((5, 8, 128), f32),
            pltpu.VMEM((5, 8, 8, 128), f32),
            pltpu.VMEM((8, 128), f32),
            pltpu.VMEM((20, 8, 128), f32),
            pltpu.VMEM((ITERS, 4, 8, 128), f32),
            pltpu.VMEM((ITERS, 8, 128), f32),
            pltpu.SemaphoreType.DMA((12,)),
            pltpu.SemaphoreType.DMA((8,)),
            pltpu.SemaphoreType.DMA((8,)),
            pltpu.SemaphoreType.DMA((8,)),
            pltpu.SemaphoreType.DMA((ITERS, 3)),
            pltpu.SemaphoreType.DMA((ITERS, 3)),
            pltpu.SemaphoreType.DMA((5, 7)),
            pltpu.SemaphoreType.DMA((5,)),
        ],
        compiler_params=pltpu.CompilerParams(collective_id=0, has_side_effects=True,
                                             vmem_limit_bytes=60 * 1024 * 1024),
    )(*(flat(v) for v in (shift, rhs_field, x_init, cond_x, cond_y, cond_z)))
    x_out = jnp.transpose(x_rows.reshape(NX, NZ, 256), (0, 2, 1))
    return x_out, small[0, :ITERS + 1], small[1, 0]


def solution(mesh):
    field_spec = P("px", "py", None)

    def local_solve(*fields):
        x_out, history, _ = fused_solve(*fields)
        return x_out, history

    return jax.shard_map(local_solve, mesh=mesh, in_specs=(field_spec,) * 6,
                         out_specs=(field_spec, P()), check_vma=False)
```

```python
import functools

import jax
import jax.numpy as jnp
from jax import lax
from jax.experimental import pallas as pl
from jax.experimental.pallas import tpu as pltpu
from jax.sharding import PartitionSpec as P

ITERS = 20
SUM_AXES = ("px", "py")
MESH = pl.DeviceIdType.MESH
NX, NZ = 64, 24
BODY = NX * NZ
FULL = BODY + 2 * NZ
HI = BODY + NZ
OTHERS = tuple((dy, dx) for dy in range(2) for dx in range(4) if (dy, dx) != (0, 0))
SEND_AT = {1: 4, 2: 9, 3: 15, 4: 19}
TAKE_AT = {6: 1, 11: 2, 17: 3}
STEPS_AT = {6: (0, 2), 7: (2, 4), 8: (4, 5), 11: (5, 7), 12: (7, 9), 13: (9, 10),
            17: (10, 12), 18: (12, 14), 19: (14, 16)}
RENEW_AT = {8: 9, 13: 14}
VREG = (8, 128)
SUB, LANES = VREG
TILES = range(2)


def turn(v, by):
    return pltpu.roll(v, by, 1)


def lift(v, by):
    return pltpu.roll(v, by, 0)


S_A, S_B, S_C, S_GP, S_G, S_CL, S_DL, S_Y, S_RHO, S_LEAD, S_HIST, S_BA, S_LA, S_LB, S_LA2, S_LB2, S_ERR, S_D, S_E, S_RHO0 = range(20)


def lanes():
    return lax.broadcasted_iota(jnp.int32, VREG, 1)


def rows8():
    return lax.broadcasted_iota(jnp.int32, VREG, 0)


def lane_sum(v):
    return jnp.broadcast_to(jnp.sum(v, axis=1, keepdims=True), VREG)


def full_sum(v):
    return jnp.broadcast_to(jnp.sum(jnp.sum(v, axis=0, keepdims=True), axis=1, keepdims=True), VREG)


def three(v):
    return jnp.concatenate([v, v, v], axis=0)


def kernel(s_h, b_h, x0_h, kx_h, ky_h, kz_h, out_h, hist_ref,
           Z, X0, D, KX, KY, KZ, PKS, H, KYP, KYH, HK, UI, CB, RS, RR, PT, ST, CO, YB,
           lsem, osem, is_s, is_r, hs, hr, rs, rr):
    px, py = lax.axis_index("px"), lax.axis_index("py")
    me = py * 4 + px
    lane, row = lanes(), rows8()
    lane24 = lax.broadcasted_iota(jnp.int32, (NZ, LANES), 1)
    row24 = lax.broadcasted_iota(jnp.int32, (NZ, LANES), 0)
    first, last = lane24 == 0, lane24 == 127
    has_lo, has_hi = px > 0, px < 3

    loads = []
    for n, (src, dst, base) in enumerate((
            (ky_h, KY, 0), (x0_h, X0, NZ), (kx_h, KX, NZ), (kz_h, KZ, 8), (s_h, D, 0), (b_h, None, NZ))):
        for t in TILES:
            to = Z.at[0, t, pl.ds(base, BODY), :] if dst is None else dst.at[t, pl.ds(base, BODY), :]
            cp = pltpu.make_async_copy(src.at[:, pl.ds(LANES * t, LANES)], to, lsem.at[2 * n + t])
            cp.start()
            loads.append(cp)

    zero_plane = jnp.zeros((NZ, LANES), jnp.float32)
    for t in TILES:
        KX[t, pl.ds(0, NZ), :] = zero_plane
        X0[t, pl.ds(0, NZ), :] = zero_plane
        X0[t, pl.ds(HI, NZ), :] = zero_plane
        KZ[t, pl.ds(0, 8), :] = jnp.zeros(VREG, jnp.float32)
    KYH[...] = jnp.zeros((2, *VREG), jnp.float32)

    @pl.loop(0, ITERS + 1)
    def _(k):
        for t in TILES:
            Z[k, t, pl.ds(0, NZ), :] = zero_plane
            Z[k, t, pl.ds(HI, NZ), :] = zero_plane

    barrier = pltpu.get_barrier_semaphore()
    for dy, dx in OTHERS:
        pl.semaphore_signal(barrier, inc=1, device_id=(lax.rem(py + dy, 2), lax.rem(px + dx, 4)),
                            device_id_type=MESH)
    pl.semaphore_wait(barrier, len(OTHERS))

    def to_x(step):
        return (py, px + step)

    to_y = (1 - py, px)

    def remote(src, dst, ssem, rsem, dev):
        return pltpu.make_async_remote_copy(src_ref=src, dst_ref=dst, send_sem=ssem, recv_sem=rsem,
                                            device_id=dev, device_id_type=MESH)

    def init_up(t):
        cols = pl.ds(LANES * t, LANES)
        return (remote(kx_h.at[pl.ds(BODY - NZ, NZ), cols], KX.at[t, pl.ds(0, NZ), :], is_s.at[t], is_r.at[t], to_x(1)),
                remote(x0_h.at[pl.ds(BODY - NZ, NZ), cols], X0.at[t, pl.ds(0, NZ), :], is_s.at[2 + t], is_r.at[2 + t], to_x(1)))

    def init_down(t):
        cols = pl.ds(LANES * t, LANES)
        return (remote(x0_h.at[pl.ds(0, NZ), cols], X0.at[t, pl.ds(HI, NZ), :], is_s.at[4 + t], is_r.at[4 + t], to_x(-1)),)

    @pl.when(has_hi)
    def _():
        for t in TILES:
            for cp in init_up(t):
                cp.start()

    @pl.when(has_lo)
    def _():
        for t in TILES:
            for cp in init_down(t):
                cp.start()

    off = 1 - py
    tb = 1 - py
    edge = 127 * (1 - py)
    inner = 126 + py * (1 - 126)

    def pack_one(items, bl):
        rel = lax.rem(lane - bl + LANES, LANES)
        s = 1
        while len(items) > 3:
            keep = rel < s
            items = [jnp.where(keep, items[n], turn(items[n + 1], s)) for n in range(0, len(items), 2)]
            s *= 2
        out = jnp.where(rel < s, items[0],
                        jnp.where(rel < 2 * s, turn(items[1], s), turn(items[2], 2 * s)))
        return out

    def pack(ref, base, bl, dst):
        for h in TILES:
            items = [ref[tb, pl.ds(base + 32 * NZ * h + 8 * a, 8), :] for a in range(96)]
            dst[h] = turn(pack_one(items, bl), lax.rem(3 + off - bl + LANES, LANES))

    low_ghost = (lane >= off) & (lane < off + 3)
    high_ghost = (lane >= off + 99) & (lane < off + 102)

    def with_ghosts(n0, n1, lo, hi):
        lo = turn(pack_one([lo[SUB * q:SUB * q + SUB] for q in range(3)], edge), lax.rem(off - edge + LANES, LANES))
        hi = turn(pack_one([hi[SUB * q:SUB * q + SUB] for q in range(3)], edge), lax.rem(99 + off - edge + LANES, LANES))
        return (jnp.where(low_ghost, lo, jnp.where(high_ghost, turn(n1, 96), n0)),
                jnp.where(low_ghost, turn(n0, 32), jnp.where(high_ghost, hi, n1)))

    def own_layout(v):
        return turn(v, 1 + py * 126)

    def z_up(v):
        return jnp.where(row == 7, lift(turn(v, 127), 7), lift(v, 7))

    def z_down(v):
        return jnp.where(row == 0, lift(turn(v, 1), 1), lift(v, 1))

    def unpack(tile, j):
        parts = [turn(tile, 124 - (3 * j + q)) for q in range(3)]
        return jnp.concatenate(parts, axis=0)

    def rowsof(i):
        return pl.multiple_of(NZ * i, 8)

    loads[0].wait()
    loads[1].wait()
    pack(KY, 0, edge, KYP)
    ky_copy = remote(KYP, KYH, is_s.at[6], is_r.at[6], to_y)

    @pl.when(py == 0)
    def _():
        ky_copy.start()

    loads[2].wait()
    loads[3].wait()
    pack(X0, NZ, edge, PKS.at[0])
    x0_copy = remote(PKS.at[0], H.at[0], is_s.at[7], is_r.at[7], to_y)
    x0_copy.start()

    for cp in loads[4:10]:
        cp.wait()

    keep_x = jnp.where(has_hi, 1.0, 0.0)
    for t in TILES:
        KX[t, pl.ds(BODY, NZ), :] = KX[t, pl.ds(BODY, NZ), :] * keep_x
    dead_y = last & (py == 1)
    dead_z = row24 == NZ - 1

    def mask_step(i, acc):
        s1, s2, kx1, ky1, kz1, k2 = acc
        r = rowsof(i)
        for t in TILES:
            s = D[t, pl.ds(r, NZ), :]
            kx = KX[t, pl.ds(r + NZ, NZ), :]
            ky = KY[t, pl.ds(r, NZ), :]
            kz = jnp.where(dead_z, 0.0, KZ[t, pl.ds(r + SUB, NZ), :])
            if t == 1:
                ky = jnp.where(dead_y, 0.0, ky)
                KY[t, pl.ds(r, NZ), :] = ky
            KZ[t, pl.ds(r + SUB, NZ), :] = kz
            s1, s2 = s1 + s, s2 + s * s
            kx1, ky1, kz1 = kx1 + kx, ky1 + ky, kz1 + kz
            k2 = k2 + (kx * kx + ky * ky + kz * kz)
        return s1, s2, kx1, ky1, kz1, k2

    sums = lax.fori_loop(0, NX, mask_step, (jnp.zeros((NZ, LANES), jnp.float32),) * 6)
    stats = jnp.zeros(VREG, jnp.float32)
    for n, v in enumerate(sums):
        stats = jnp.where((row == 2) & (lane == n), full_sum(v), stats)

    def sum_copies(e):
        return [remote(RS.at[e], RR.at[e, me], rs.at[e, n], rr.at[e],
                       (lax.rem(py + dy, 2), lax.rem(px + dx, 4))) for n, (dy, dx) in enumerate(OTHERS)]

    def sum_send(e, tile):
        RS[e] = tile
        RR[e, me] = tile
        for cp in sum_copies(e):
            cp.start()

    def sum_take(e):
        pltpu.make_async_copy(RR.at[e, pl.ds(0, 7)], RR.at[e, pl.ds(0, 7)], rr.at[e]).wait()
        total = RR[e, 0]
        for n in range(1, 8):
            total = total + RR[e, n]
        return total

    sum_send(0, stats)
    pack(KX, NZ, edge, CB.at[1])
    pack(KZ, 8, edge, CB.at[5])
    pack(KY, 0, inner, CB.at[4])
    pack(KY, 0, edge, CB.at[3])
    for h in TILES:
        CB[6, h] = z_down(CB[5, h])

    def up_copy(k):
        return remote(Z.at[k, :, pl.ds(BODY, NZ), :], Z.at[k, :, pl.ds(0, NZ), :], hs.at[k, 0], hr.at[k, 0], to_x(1))

    def down_copy(k):
        return remote(Z.at[k, :, pl.ds(NZ, NZ), :], Z.at[k, :, pl.ds(HI, NZ), :], hs.at[k, 1], hr.at[k, 1], to_x(-1))

    def y_copy(k):
        return remote(PKS.at[k + 1], H.at[k + 1], hs.at[k, 2], hr.at[k, 2], to_y)

    def send_x(k):
        @pl.when(has_hi)
        def _():
            up_copy(k).start()

        @pl.when(has_lo)
        def _():
            down_copy(k).start()

    def take_halo(k):
        @pl.when(has_lo)
        def _():
            up_copy(k).wait_recv()

        @pl.when(has_hi)
        def _():
            down_copy(k).wait_recv()

        y_copy(k).wait_recv()

    def first_state(vec, i):
        r = rowsof(i)
        return ([vec(t, r) for t in TILES], [vec(t, r + NZ) for t in TILES],
                [KX[t, pl.ds(r, NZ), :] for t in TILES])

    def neighbours(vec, i, j, tile_raw, tile_k, state):
        r = rowsof(i)
        x_down, u, kx_down = state
        x_up = [vec(t, r + 2 * NZ) for t in TILES]
        kx = [KX[t, pl.ds(r + NZ, NZ), :] for t in TILES]
        ky = [KY[t, pl.ds(r, NZ), :] for t in TILES]
        up = [turn(u[t], 127) for t in TILES]
        down = [turn(ky[t] * u[t], 1) for t in TILES]
        y_up = [jnp.where(last, up[1], up[0]), jnp.where(last, unpack(tile_raw, j), up[1])]
        y_down = [jnp.where(first, unpack(tile_k, j), down[0]), jnp.where(first, down[0], down[1])]
        out = []
        for t in TILES:
            part = ky[t] * y_up[t] + y_down[t]
            part = part + kx[t] * x_up[t]
            part = part + kx_down[t] * x_down[t]
            part = part + KZ[t, pl.ds(r + SUB, NZ), :] * vec(t, r + NZ + 1)
            part = part + KZ[t, pl.ds(r + 7, NZ), :] * vec(t, r + NZ - 1)
            out.append(part)
        return u, out, ky, kx, (u, x_up, kx)

    @pl.when(has_lo)
    def _():
        for t in TILES:
            for cp in init_up(t):
                cp.wait_recv()

    @pl.when(has_hi)
    def _():
        for t in TILES:
            for cp in init_down(t):
                cp.wait_recv()

    @pl.when(py == 1)
    def _():
        ky_copy.wait_recv()

    x0_copy.wait_recv()
    for h in TILES:
        HK[h] = H[0, h] * KYH[h]
    loads[10].wait()
    loads[11].wait()

    x0_vec = lambda t, q: X0[t, pl.ds(q, NZ), :]

    def start_plane(i, rho, state):
        h = i // 32
        j = lax.rem(i, 32)
        r = rowsof(i)
        kx_down = state[2]
        u, nb, ky, kx, state = neighbours(x0_vec, i, j, H[0, h], HK[h], state)
        down = [turn(ky[t], 1) for t in TILES]
        ky_lo = [jnp.where(first, unpack(KYH[h], j), down[0]), jnp.where(first, down[0], down[1])]
        for t in TILES:
            diag = D[t, pl.ds(r, NZ), :] + ky[t] + ky_lo[t] + kx[t] + kx_down[t]
            diag = diag + KZ[t, pl.ds(r + SUB, NZ), :] + KZ[t, pl.ds(r + 7, NZ), :]
            D[t, pl.ds(r, NZ), :] = diag
            res = Z[0, t, pl.ds(r + NZ, NZ), :] - (diag * u[t] - nb[t])
            Z[0, t, pl.ds(r + NZ, NZ), :] = res
            rho = rho + res * res
        return rho, state

    UNROLL = 10

    def sweep(vec, plane, k, sums1, more, send_y):
        def run(i, n, c):
            state = first_state(vec, i)
            for m in range(n):
                c, state = plane(i + m, c, state)
            return c

        sums1 = run(0, 2, sums1)

        @pl.when(more)
        def _():
            send_y()

        sums1 = run(NX - 2, 2, sums1)

        @pl.when(more)
        def _():
            send_x(k)

        return lax.fori_loop(0, 60 // UNROLL, lambda m, c: run(2 + UNROLL * m, UNROLL, c), sums1)

    zero24 = jnp.zeros((NZ, LANES), jnp.float32)
    zero_tile = jnp.zeros((NZ, LANES), jnp.float32)
    kx_cols = with_ghosts(CB[1, 0], CB[1, 1], KX[tb, pl.ds(0, NZ), :], zero_tile)
    for h in TILES:
        CB[2, h] = turn(kx_cols[h], 3)
        ky_edge, ky_in = CB[3, h], CB[4, h]
        CB[3, h] = jnp.where(py == 0, ky_edge, own_layout(KYH[h]))
        CB[4, h] = jnp.where(py == 0, ky_in, ky_edge)
    rho0 = sweep(x0_vec, start_plane, 0, zero24, px >= 0, lambda: None)
    pack(Z.at[0], NZ, edge, PKS.at[1])
    y_copy(0).start()
    pack(Z.at[0], NZ, inner, UI)
    pack(D, 0, edge, CB.at[0])
    PT[...] = jnp.where((row == 0) & (lane == 0), full_sum(rho0), 0.0)

    for n in range(20):
        ST[n] = jnp.zeros(VREG, jnp.float32)
    totals = sum_take(0)
    cells = float(NX * 256 * NZ * 8)
    mean = [full_sum(jnp.where((row == 2) & (lane == n), totals, 0.0)) * (1.0 / cells) for n in range(6)]
    var_s = jnp.maximum(mean[1] - mean[0] * mean[0], 0.0)
    var_k = jnp.maximum(mean[5] - mean[2] * mean[2] - mean[3] * mean[3] - mean[4] * mean[4], 0.0)
    b_first = jnp.sqrt(3.0 * mean[5] + 1.5 * (var_s + 2.0 * var_k))
    a_first = jnp.maximum(mean[0] - 0.5 * jnp.sqrt(var_s), 0.3) + 2.0 * b_first

    def set_coefs(k0, a_new, b_new):
        old_b = ST[S_B]
        b_arr = jnp.where(lane >= k0, b_new, old_b)
        ST[S_A] = jnp.where(lane >= k0, a_new, ST[S_A])
        ST[S_B] = b_arr
        ST[S_C] = jnp.where(lane == 0, 0.0, turn(b_arr, 1))
        inv = 1.0 / b_new
        for k in range(k0, ITERS):
            CO[k, 0] = a_new
            if k > k0:
                CO[k, 1] = b_new
            elif k == 0:
                CO[k, 1] = jnp.zeros(VREG, jnp.float32)
            else:
                CO[k, 1] = CO[k - 1, 3]
            CO[k, 2] = inv
            CO[k, 3] = b_new

    set_coefs(0, a_first, b_first)

    def gram_start(total):
        rho = full_sum(jnp.where((row == 0) & (lane == 0), total, 0.0))
        one = jnp.where(lane == 0, 1.0, 0.0)
        ST[S_G] = one * rho
        ST[S_CL] = one
        ST[S_DL] = one
        ST[S_LEAD] = jnp.ones(VREG, jnp.float32)
        ST[S_RHO] = rho
        ST[S_RHO0] = rho
        ST[S_HIST] = one * rho

    def gram_load(total):
        ST[S_D] = jnp.broadcast_to(total[0:1], VREG)
        ST[S_E] = jnp.broadcast_to(total[1:2], VREG)

    def gram_step(k):
        a, b, c = ST[S_A], ST[S_B], ST[S_C]
        g, gp, cl, dl = ST[S_G], ST[S_GP], ST[S_CL], ST[S_DL]
        e_row, d_row = ST[S_E], ST[S_D]
        rho, lead = ST[S_RHO], ST[S_LEAD]
        b_k, c_k, a_k = CO[k, 3], CO[k, 1], CO[k, 0]
        at_k, at_k1 = lane == k, lane == k + 1
        rec = ((a - a_k) * g + b * turn(g, 127)
               + c * turn(g, 1) - c_k * gp) * CO[k, 2]
        g_new = jnp.where(lane < k, rec, jnp.where(at_k, e_row, jnp.where(at_k1, d_row, 0.0)))
        g_full = jnp.where(at_k1, turn(e_row, 1), g)
        image = a * dl + turn(b * dl, 1) + turn(c * dl, 127)
        delta = lead * lane_sum(image * g_full)
        alpha = rho / delta
        y = ST[S_Y] + alpha * dl
        cl = cl - alpha * image
        lead = -alpha * b_k * lead
        prod = cl * g_new
        rho_new = lead * lane_sum(prod)
        size = jnp.abs(lead) * lane_sum(jnp.abs(prod))
        beta = rho_new / rho
        dl = cl + beta * dl
        ST[S_G], ST[S_GP], ST[S_CL], ST[S_DL] = g_new, g, cl, dl
        ST[S_Y], ST[S_RHO], ST[S_LEAD] = y, rho_new, lead
        ST[S_HIST] = jnp.where(at_k1, rho_new, ST[S_HIST])
        inv_alpha = 1.0 / alpha
        ST[S_LA2], ST[S_LB2] = ST[S_LA], ST[S_LB]
        ST[S_LA] = inv_alpha + ST[S_BA]
        ST[S_LB] = jnp.sqrt(jnp.abs(beta)) * inv_alpha
        ST[S_BA] = beta * inv_alpha
        err = size / jnp.abs(rho_new) * jnp.sqrt(jnp.abs(rho_new) / ST[S_RHO0])
        err = jnp.where(rho_new > 0.0, err, 1e30)
        ST[S_ERR] = jnp.maximum(ST[S_ERR], jnp.where(err < 1e30, err, 1e30))

    def renew(k0):
        a_new = 0.5 * (ST[S_LA] + ST[S_LA2])
        b_new = 0.5 * (ST[S_LB] + ST[S_LB2])
        a_ok = (a_new > 0.3) & (a_new < 26.8)
        a_new = jnp.where(a_ok, a_new, a_first)
        b_new = jnp.where(a_ok & (b_new > 0.25 * b_first) & (b_new < 2.0 * b_first), b_new, b_first)
        set_coefs(k0, a_new, b_new)

    def apply_step(k):
        take_halo(k)
        for h in TILES:
            HK[h] = H[k + 1, h] * KYH[h]
        before = jnp.maximum(k - 1, 0)
        cols = with_ghosts(PKS[k + 1, 0], PKS[k + 1, 1], Z[k, tb, pl.ds(0, NZ), :], Z[k, tb, pl.ds(HI, NZ), :])
        for h in TILES:
            u = cols[h]
            val = (CB[0, h] - CO[k, 0]) * u - CB[3, h] * own_layout(H[k + 1, h]) - CB[4, h] * UI[h]
            val = val - CB[1, h] * turn(u, 125) - CB[2, h] * turn(u, 3)
            val = val - CB[5, h] * z_up(u) - CB[6, h] * z_down(u) - CO[k, 1] * PKS[before + 1, h]
            PKS[k + 2, h] = val * CO[k, 2]
        a_k, c_k, i_k = three(CO[k, 0]), three(CO[k, 1]), three(CO[k, 2])

        def plane(i, carry, state):
            dots, cross = carry
            h = i // 32
            j = lax.rem(i, 32)
            r = rowsof(i)
            u, nb, ky, kx, state = neighbours(vec, i, j, H[k + 1, h], HK[h], state)
            for t in TILES:
                val = (D[t, pl.ds(r, NZ), :] - a_k) * u[t] - nb[t] - c_k * Z[before, t, pl.ds(r + NZ, NZ), :]
                val = val * i_k
                Z[k + 1, t, pl.ds(r + NZ, NZ), :] = val
                dots = dots + val * val
                cross = cross + val * u[t]
            return (dots, cross), state

        vec = lambda t, q: Z[k, t, pl.ds(q, NZ), :]
        more = k < ITERS - 1
        dots, cross = sweep(vec, plane, k + 1, (zero24, zero24), more, lambda: y_copy(k + 1).start())

        @pl.when(more)
        def _():
            pack(Z.at[k + 1], NZ, inner, UI)

        tile = jnp.where((row == 0) & (lane == k + 1), full_sum(dots), PT[...])
        tile = jnp.where((row == 1) & (lane == k), full_sum(cross), tile)
        PT[...] = tile
        for e, at in SEND_AT.items():
            @pl.when(k == at)
            def _():
                sum_send(e, tile)
        for at, e in TAKE_AT.items():
            @pl.when(k == at)
            def _():
                total = sum_take(e)
                gram_load(total)
                if e == 1:
                    gram_start(total)
        for at, (lo, hi) in STEPS_AT.items():
            @pl.when(k == at)
            def _():
                @pl.loop(lo, hi)
                def _(s):
                    gram_step(s)
        for at, k0 in RENEW_AT.items():
            @pl.when(k == at)
            def _():
                renew(k0)

    @pl.loop(0, ITERS)
    def _(k):
        apply_step(k)

    gram_load(sum_take(4))

    @pl.loop(16, ITERS)
    def _(s):
        gram_step(s)

    y = ST[S_Y]
    for k in range(ITERS):
        YB[k] = lane_sum(jnp.where(lane == k, y, 0.0))
    hist = jnp.sqrt(ST[S_HIST] * (1.0 / cells))
    hist_ref[...] = jnp.where(row == 0, hist, ST[S_ERR])

    def combine(i, c):
        r = rowsof(i + 1)
        acc = [X0[t, pl.ds(r, NZ), :] for t in TILES]
        for k in range(ITERS):
            w = three(YB[k])
            for t in TILES:
                acc[t] = acc[t] + w * Z[k, t, pl.ds(r, NZ), :]
        for t in TILES:
            X0[t, pl.ds(r, NZ), :] = acc[t]
        return c

    outs = []
    for part in range(4):
        lax.fori_loop(16 * part, 16 * part + 16, combine, 0)
        for t in TILES:
            cp = pltpu.make_async_copy(X0.at[t, pl.ds(NZ + 16 * NZ * part, 16 * NZ), :],
                                       out_h.at[pl.ds(16 * NZ * part, 16 * NZ), pl.ds(LANES * t, LANES)],
                                       osem.at[2 * part + t])
            cp.start()
            outs.append(cp)

    @pl.when(has_hi)
    def _():
        for t in TILES:
            for cp in init_up(t):
                cp.wait_send()

    @pl.when(has_lo)
    def _():
        for t in TILES:
            for cp in init_down(t):
                cp.wait_send()

    @pl.when(py == 0)
    def _():
        ky_copy.wait_send()

    x0_copy.wait_send()

    @pl.loop(0, ITERS)
    def _(k):
        @pl.when(has_hi)
        def _():
            up_copy(k).wait_send()

        @pl.when(has_lo)
        def _():
            down_copy(k).wait_send()

        y_copy(k).wait_send()

    for e in range(5):
        for cp in sum_copies(e):
            cp.wait_send()
    for cp in outs:
        cp.wait()


def fused_solve(shift, rhs_field, x_init, cond_x, cond_y, cond_z):
    def flat(v):
        return jnp.transpose(v, (0, 2, 1)).reshape(BODY, 256)

    f32 = jnp.float32
    any_spec = pl.BlockSpec(memory_space=pl.ANY)
    x_rows, small = pl.pallas_call(
        kernel,
        out_shape=(jax.ShapeDtypeStruct((BODY, 256), f32), jax.ShapeDtypeStruct(VREG, f32)),
        in_specs=[any_spec] * 6,
        out_specs=(any_spec, pl.BlockSpec(memory_space=pltpu.VMEM)),
        scratch_shapes=[
            pltpu.VMEM((ITERS + 1, 2, FULL, LANES), f32),
            pltpu.VMEM((2, FULL, LANES), f32),
            pltpu.VMEM((2, BODY, LANES), f32),
            pltpu.VMEM((2, BODY + NZ, LANES), f32),
            pltpu.VMEM((2, BODY, LANES), f32),
            pltpu.VMEM((2, BODY + 8, LANES), f32),
            pltpu.VMEM((ITERS + 2, 2, *VREG), f32),
            pltpu.VMEM((ITERS + 2, 2, *VREG), f32),
            pltpu.VMEM((2, *VREG), f32),
            pltpu.VMEM((2, *VREG), f32),
            pltpu.VMEM((2, *VREG), f32),
            pltpu.VMEM((2, *VREG), f32),
            pltpu.VMEM((7, 2, *VREG), f32),
            pltpu.VMEM((5, *VREG), f32),
            pltpu.VMEM((5, 8, *VREG), f32),
            pltpu.VMEM(VREG, f32),
            pltpu.VMEM((20, *VREG), f32),
            pltpu.VMEM((ITERS, 4, *VREG), f32),
            pltpu.VMEM((ITERS, *VREG), f32),
            pltpu.SemaphoreType.DMA((12,)),
            pltpu.SemaphoreType.DMA((8,)),
            pltpu.SemaphoreType.DMA((8,)),
            pltpu.SemaphoreType.DMA((8,)),
            pltpu.SemaphoreType.DMA((ITERS, 3)),
            pltpu.SemaphoreType.DMA((ITERS, 3)),
            pltpu.SemaphoreType.DMA((5, 7)),
            pltpu.SemaphoreType.DMA((5,)),
        ],
        compiler_params=pltpu.CompilerParams(collective_id=0, has_side_effects=True,
                                             vmem_limit_bytes=60 * 1024 * 1024),
    )(*(flat(v) for v in (shift, rhs_field, x_init, cond_x, cond_y, cond_z)))
    x_out = jnp.transpose(x_rows.reshape(NX, NZ, 256), (0, 2, 1))
    return x_out, small[0, :ITERS + 1], small[1, 0]


def solution(mesh):
    field_spec = P("px", "py", None)

    def local_solve(*fields):
        x_out, history, _ = fused_solve(*fields)
        return x_out, history

    return jax.shard_map(local_solve, mesh=mesh, in_specs=(field_spec,) * 6,
                         out_specs=(field_spec, P()), check_vma=False)
```

```python
import functools

import jax
import jax.numpy as jnp
from jax import lax
from jax.experimental import pallas as pl
from jax.experimental.pallas import tpu as pltpu
from jax.sharding import PartitionSpec as P

ITERS = 20
SUM_AXES = ("px", "py")
MESH = pl.DeviceIdType.MESH
NX, NZ = 64, 24
ROW = 256
ERR_LIMIT = 1000.0
HALF = NX // 2
CELLS = float(NX * 256 * NZ * 8)
BODY = NX * NZ
FULL = BODY + 2 * NZ
HI = BODY + NZ
OTHERS = tuple((dy, dx) for dy in range(2) for dx in range(4) if (dy, dx) != (0, 0))
SEND_AT = {1: 4, 2: 9, 3: 15, 4: 19}
TAKE_AT = {6: 1, 11: 2, 17: 3}
STEPS_AT = {6: (0, 2), 7: (2, 4), 8: (4, 5), 11: (5, 7), 12: (7, 9), 13: (9, 10),
            17: (10, 12), 18: (12, 14), 19: (14, 16)}
RENEW_AT = {8: 9, 13: 14}
VREG = (8, 128)
SUB, LANES = VREG
TILES = range(2)


C_D, C_UP, C_DOWN, C_OUT, C_IN, C_ZUP, C_ZDN = range(7)
K_A, K_C, K_INV, K_B = range(4)
NQ = 3
LAST, TOP, NIL = 127, 7, 0.0


def turn(v, by):
    return pltpu.roll(v, by, 1)


def lift(v, by):
    return pltpu.roll(v, by, 0)


S_A, S_B, S_C, S_GP, S_G, S_CL, S_DL, S_Y, S_RHO, S_LEAD, S_HIST, S_BA, S_LA, S_LB, S_LA2, S_LB2, S_ERR, S_D, S_E, S_RHO0 = range(20)


def lanes():
    return lax.broadcasted_iota(jnp.int32, VREG, 1)


def rows8():
    return lax.broadcasted_iota(jnp.int32, VREG, 0)


def lane_sum(v):
    return jnp.broadcast_to(jnp.sum(v, axis=1, keepdims=True), VREG)


def full_sum(v):
    return jnp.broadcast_to(jnp.sum(jnp.sum(v, axis=0, keepdims=True), axis=1, keepdims=True), VREG)


def three(v):
    return jnp.concatenate([v, v, v], axis=0)


def kernel(s_h, b_h, x0_h, kx_h, ky_h, kz_h, out_h, hist_ref,
           Z, X0, D, KX, KY, KZ, PKS, H, KYP, KYH, HK, UI, CB, PRE, RS, RR, PT, ST, CO, YB,
           lsem, osem, is_s, is_r, hs, hr, rs, rr):
    px, py = lax.axis_index("px"), lax.axis_index("py")
    me = py * 4 + px
    lane, row = lanes(), rows8()
    lane24 = lax.broadcasted_iota(jnp.int32, (NZ, LANES), 1)
    row24 = lax.broadcasted_iota(jnp.int32, (NZ, LANES), 0)
    first, last = lane24 == 0, lane24 == LAST
    has_lo, has_hi = px > 0, px < NQ

    loads = []
    for n, (src, dst, base) in enumerate((
            (ky_h, KY, 0), (x0_h, X0, NZ), (kx_h, KX, NZ), (kz_h, KZ, 8), (s_h, D, 0), (b_h, None, NZ))):
        for t in TILES:
            to = Z.at[0, t, pl.ds(base, BODY), :] if dst is None else dst.at[t, pl.ds(base, BODY), :]
            cp = pltpu.make_async_copy(src.at[:, pl.ds(LANES * t, LANES)], to, lsem.at[2 * n + t])
            cp.start()
            loads.append(cp)

    zero_plane = jnp.zeros((NZ, LANES), jnp.float32)
    for t in TILES:
        KX[t, pl.ds(0, NZ), :] = zero_plane
        X0[t, pl.ds(0, NZ), :] = zero_plane
        X0[t, pl.ds(HI, NZ), :] = zero_plane
        KZ[t, pl.ds(0, 8), :] = jnp.zeros(VREG, jnp.float32)
    KYH[...] = jnp.zeros((2, *VREG), jnp.float32)

    @pl.loop(0, ITERS + 1)
    def _(k):
        for t in TILES:
            Z[k, t, pl.ds(0, NZ), :] = zero_plane
            Z[k, t, pl.ds(HI, NZ), :] = zero_plane

    barrier = pltpu.get_barrier_semaphore()
    for dy, dx in OTHERS:
        pl.semaphore_signal(barrier, inc=1, device_id=(lax.rem(py + dy, 2), lax.rem(px + dx, 4)),
                            device_id_type=MESH)
    pl.semaphore_wait(barrier, len(OTHERS))

    def to_x(step):
        return (py, px + step)

    to_y = (1 - py, px)

    def remote(src, dst, ssem, rsem, dev):
        return pltpu.make_async_remote_copy(src_ref=src, dst_ref=dst, send_sem=ssem, recv_sem=rsem,
                                            device_id=dev, device_id_type=MESH)

    def init_up(t):
        cols = pl.ds(LANES * t, LANES)
        return (remote(kx_h.at[pl.ds(BODY - NZ, NZ), cols], KX.at[t, pl.ds(0, NZ), :], is_s.at[t], is_r.at[t], to_x(1)),
                remote(x0_h.at[pl.ds(BODY - NZ, NZ), cols], X0.at[t, pl.ds(0, NZ), :], is_s.at[2 + t], is_r.at[2 + t], to_x(1)))

    def init_down(t):
        cols = pl.ds(LANES * t, LANES)
        return (remote(x0_h.at[pl.ds(0, NZ), cols], X0.at[t, pl.ds(HI, NZ), :], is_s.at[4 + t], is_r.at[4 + t], to_x(-1)),)

    @pl.when(has_hi)
    def _():
        for t in TILES:
            for cp in init_up(t):
                cp.start()

    @pl.when(has_lo)
    def _():
        for t in TILES:
            for cp in init_down(t):
                cp.start()

    off = 1 - py
    tb = 1 - py
    edge = LAST * (1 - py)
    inner = 126 + py * (1 - 126)

    def pack_one(items, bl):
        rel = lax.rem(lane - bl + LANES, LANES)
        s = 1
        while len(items) > NQ:
            keep = rel < s
            items = [jnp.where(keep, items[n], turn(items[n + 1], s)) for n in range(0, len(items), 2)]
            s *= 2
        out = jnp.where(rel < s, items[0],
                        jnp.where(rel < 2 * s, turn(items[1], s), turn(items[2], 2 * s)))
        return out

    def pack(ref, base, bl, dst):
        start = NQ + off - bl + LANES
        for h in TILES:
            accs = [jnp.zeros(VREG, jnp.float32)] * NQ
            for a in range(NQ * HALF):
                v = ref[tb, pl.ds(base + HALF * NZ * h + SUB * a, SUB), :]
                moved = turn(v, lax.rem(start + a, LANES))
                accs[a % NQ] = jnp.where(lane == a + NQ + off, moved, accs[a % NQ])
            dst[h] = accs[0] + accs[1] + accs[2]

    low_ghost = (lane >= off) & (lane < off + NQ)
    high_ghost = (lane >= off + 99) & (lane < off + 102)

    def with_ghosts(n0, n1, lo, hi):
        lo = turn(pack_one([lo[SUB * q:SUB * q + SUB] for q in range(NQ)], edge), lax.rem(off - edge + LANES, LANES))
        hi = turn(pack_one([hi[SUB * q:SUB * q + SUB] for q in range(NQ)], edge), lax.rem(99 + off - edge + LANES, LANES))
        return (jnp.where(low_ghost, lo, jnp.where(high_ghost, turn(n1, 96), n0)),
                jnp.where(low_ghost, turn(n0, 32), jnp.where(high_ghost, hi, n1)))

    def own_layout(v):
        return turn(v, 1 + py * 126)

    def z_up(v):
        return jnp.where(row == TOP, lift(turn(v, LAST), TOP), lift(v, TOP))

    def z_down(v):
        return jnp.where(row == 0, lift(turn(v, 1), 1), lift(v, 1))

    def unpack(tile, j):
        parts = [turn(tile, 124 - (NQ * j + q)) for q in range(NQ)]
        return jnp.concatenate(parts, axis=0)

    def rowsof(i):
        return pl.multiple_of(NZ * i, 8)

    loads[0].wait()
    loads[1].wait()
    pack(KY, 0, edge, KYP)
    ky_copy = remote(KYP, KYH, is_s.at[6], is_r.at[6], to_y)

    @pl.when(py == 0)
    def _():
        ky_copy.start()

    loads[2].wait()
    loads[NQ].wait()
    pack(X0, NZ, edge, PKS.at[0])
    x0_copy = remote(PKS.at[0], H.at[0], is_s.at[TOP], is_r.at[TOP], to_y)
    x0_copy.start()

    for cp in loads[4:12]:
        cp.wait()

    keep_x = jnp.where(has_hi, 1.0, NIL)
    for t in TILES:
        KX[t, pl.ds(BODY, NZ), :] = KX[t, pl.ds(BODY, NZ), :] * keep_x
    dead_y = last & (py == 1)
    dead_z = row24 == NZ - 1

    def mask_step(i, acc):
        s1, s2, kx1, ky1, kz1, k2 = acc
        r = rowsof(i)
        for t in TILES:
            s = D[t, pl.ds(r, NZ), :]
            kx = KX[t, pl.ds(r + NZ, NZ), :]
            ky = KY[t, pl.ds(r, NZ), :]
            kz = jnp.where(dead_z, NIL, KZ[t, pl.ds(r + SUB, NZ), :])
            if t == 1:
                ky = jnp.where(dead_y, NIL, ky)
                KY[t, pl.ds(r, NZ), :] = ky
            KZ[t, pl.ds(r + SUB, NZ), :] = kz
            s1, s2 = s1 + s, s2 + s * s
            kx1, ky1, kz1 = kx1 + kx, ky1 + ky, kz1 + kz
            k2 = k2 + (kx * kx + ky * ky + kz * kz)
        return s1, s2, kx1, ky1, kz1, k2

    sums = lax.fori_loop(0, NX, mask_step, (zero_plane,) * 6, unroll=4)
    stats = jnp.zeros(VREG, jnp.float32)
    for n, v in enumerate(sums):
        stats = jnp.where((row == 2) & (lane == n), full_sum(v), stats)

    def sum_copies(e):
        return [remote(RS.at[e], RR.at[e, me], rs.at[e, n], rr.at[e],
                       (lax.rem(py + dy, 2), lax.rem(px + dx, 4))) for n, (dy, dx) in enumerate(OTHERS)]

    def sum_send(e, tile):
        RS[e] = tile
        RR[e, me] = tile
        for cp in sum_copies(e):
            cp.start()

    def sum_take(e):
        pltpu.make_async_copy(RR.at[e, pl.ds(0, TOP)], RR.at[e, pl.ds(0, TOP)], rr.at[e]).wait()
        total = RR[e, 0]
        for n in range(1, 8):
            total = total + RR[e, n]
        return total

    sum_send(0, stats)
    pack(D, 0, edge, CB.at[C_D])
    pack(Z.at[0], NZ, edge, PRE)
    pack(X0, NZ, inner, UI)
    pack(KX, NZ, edge, CB.at[C_UP])
    pack(KZ, 8, edge, CB.at[C_ZUP])
    pack(KY, 0, inner, CB.at[C_IN])
    pack(KY, 0, edge, CB.at[C_OUT])
    for h in TILES:
        CB[C_ZDN, h] = z_down(CB[C_ZUP, h])

    def up_copy(k):
        return remote(Z.at[k, :, pl.ds(BODY, NZ), :], Z.at[k, :, pl.ds(0, NZ), :], hs.at[k, 0], hr.at[k, 0], to_x(1))

    def down_copy(k):
        return remote(Z.at[k, :, pl.ds(NZ, NZ), :], Z.at[k, :, pl.ds(HI, NZ), :], hs.at[k, 1], hr.at[k, 1], to_x(-1))

    def y_copy(k):
        return remote(PKS.at[k + 1], H.at[k + 1], hs.at[k, 2], hr.at[k, 2], to_y)

    def send_x(k):
        @pl.when(has_hi)
        def _():
            up_copy(k).start()

        @pl.when(has_lo)
        def _():
            down_copy(k).start()

    def take_halo(k):
        @pl.when(has_lo)
        def _():
            up_copy(k).wait_recv()

        @pl.when(has_hi)
        def _():
            down_copy(k).wait_recv()

        y_copy(k).wait_recv()

    def first_state(vec, i):
        r = rowsof(i)
        return ([vec(t, r) for t in TILES], [vec(t, r + NZ) for t in TILES],
                [KX[t, pl.ds(r, NZ), :] for t in TILES])

    def neighbours(vec, i, j, tile_raw, tile_k, state):
        r = rowsof(i)
        x_down, u, kx_down = state
        x_up = [vec(t, r + 2 * NZ) for t in TILES]
        kx = [KX[t, pl.ds(r + NZ, NZ), :] for t in TILES]
        ky = [KY[t, pl.ds(r, NZ), :] for t in TILES]
        up = [turn(u[t], LAST) for t in TILES]
        down = [turn(ky[t] * u[t], 1) for t in TILES]
        y_up = [jnp.where(last, up[1], up[0]), jnp.where(last, unpack(tile_raw, j), up[1])]
        y_down = [jnp.where(first, unpack(tile_k, j), down[0]), jnp.where(first, down[0], down[1])]
        out = []
        for t in TILES:
            part = ky[t] * y_up[t] + y_down[t]
            part = part + kx[t] * x_up[t]
            part = part + kx_down[t] * x_down[t]
            part = part + KZ[t, pl.ds(r + SUB, NZ), :] * vec(t, r + NZ + 1)
            part = part + KZ[t, pl.ds(r + TOP, NZ), :] * vec(t, r + NZ - 1)
            out.append(part)
        return u, out, ky, kx, (u, x_up, kx)

    @pl.when(has_lo)
    def _():
        for t in TILES:
            for cp in init_up(t):
                cp.wait_recv()

    @pl.when(has_hi)
    def _():
        for t in TILES:
            for cp in init_down(t):
                cp.wait_recv()

    @pl.when(py == 1)
    def _():
        ky_copy.wait_recv()

    x0_copy.wait_recv()
    for h in TILES:
        HK[h] = H[0, h] * KYH[h]

    def own_faces(cols):
        n0, n1 = cols
        from_lo, from_hi = (lane >= off + NQ) & (lane < off + 6), (lane >= off + NQ * HALF) & (lane < off + NQ * HALF + NQ)
        down = (jnp.where(from_lo, NIL, turn(n0, NQ)), jnp.where(from_lo, turn(n0, 35), turn(n1, NQ)))
        up = (jnp.where(from_hi, turn(n1, 93), turn(n0, 125)), jnp.where(from_hi, NIL, turn(n1, 125)))
        return [CB[C_IN, h] * UI[h] + CB[C_UP, h] * up[h] + CB[C_DOWN, h] * down[h]
                + CB[C_ZUP, h] * z_up(u) + CB[C_ZDN, h] * z_down(u) for h, u in enumerate(cols)]

    def outer_faces(lo, hi, beyond):
        ghost = [jnp.zeros(VREG, jnp.float32)] * 2
        for q in range(NQ):
            for h, (v, at) in enumerate(((lo, NQ), (hi, NQ * HALF))):
                at = at + q + off
                moved = turn(v[SUB * q:SUB * q + SUB], lax.rem(at - edge + LANES, LANES))
                ghost[h] = jnp.where(lane == at, moved, ghost[h])
        return [CB[C_OUT, h] * own_layout(beyond[h]) + CB[C_DOWN - h, h] * ghost[h] for h in TILES]

    x0_vec = lambda t, q: X0[t, pl.ds(q, NZ), :]

    def start_plane(i, rho, state):
        h = i // 32
        j = lax.rem(i, 32)
        r = rowsof(i)
        kx_down = state[2]
        u, nb, ky, kx, state = neighbours(x0_vec, i, j, H[0, h], HK[h], state)
        down = [turn(ky[t], 1) for t in TILES]
        ky_lo = [jnp.where(first, unpack(KYH[h], j), down[0]), jnp.where(first, down[0], down[1])]
        for t in TILES:
            diag = D[t, pl.ds(r, NZ), :] + ky[t] + ky_lo[t] + kx[t] + kx_down[t]
            diag = diag + KZ[t, pl.ds(r + SUB, NZ), :] + KZ[t, pl.ds(r + TOP, NZ), :]
            D[t, pl.ds(r, NZ), :] = diag
            res = Z[0, t, pl.ds(r + NZ, NZ), :] - (diag * u[t] - nb[t])
            Z[0, t, pl.ds(r + NZ, NZ), :] = res
            rho = rho + res * res
        return rho, state

    UNROLL = 10

    def sweep(vec, plane, k, sums1, more):
        def run(i, n, c):
            state = first_state(vec, i)
            for m in range(n):
                c, state = plane(i + m, c, state)
            return c

        sums1 = run(NX - 1, 1, run(0, 1, sums1))

        @pl.when(more)
        def _():
            send_x(k)

        sums1 = run(NX - 2, 1, run(1, 1, sums1))
        return lax.fori_loop(0, 60 // UNROLL, lambda m, c: run(2 + UNROLL * m, UNROLL, c), sums1)

    zero24 = zero_plane
    zero_tile = zero_plane
    kx_cols = with_ghosts(CB[C_UP, 0], CB[C_UP, 1], KX[tb, pl.ds(0, NZ), :], zero_tile)
    for h in TILES:
        CB[C_DOWN, h] = turn(kx_cols[h], NQ)
        ky_edge, ky_in = CB[C_OUT, h], CB[C_IN, h]
        CB[C_OUT, h] = jnp.where(py == 0, ky_edge, own_layout(KYH[h]))
        CB[C_IN, h] = jnp.where(py == 0, ky_in, ky_edge)
    far = outer_faces(X0[tb, pl.ds(0, NZ), :], X0[tb, pl.ds(HI, NZ), :], (H[0, 0], H[0, 1]))
    own = own_faces((PKS[0, 0], PKS[0, 1]))
    for h in TILES:
        diag = CB[C_D, h] + CB[C_UP, h] + CB[C_DOWN, h] + CB[C_OUT, h] + CB[C_IN, h] + CB[C_ZUP, h] + CB[C_ZDN, h]
        CB[C_D, h] = diag
        PKS[1, h] = PRE[h] - (diag * PKS[0, h] - far[h] - own[h])
    y_copy(0).start()
    rho0 = sweep(x0_vec, start_plane, 0, zero24, px >= 0)
    pack(Z.at[0], NZ, inner, UI)
    PT[...] = jnp.where((row == 0) & (lane == 0), full_sum(rho0), NIL)

    for n in range(20):
        ST[n] = jnp.zeros(VREG, jnp.float32)
    totals = sum_take(0)
    cells = CELLS
    mean = [full_sum(jnp.where((row == 2) & (lane == n), totals, NIL)) * (1.0 / cells) for n in range(6)]
    var_s = jnp.maximum(mean[1] - mean[0] * mean[0], NIL)
    var_k = jnp.maximum(mean[5] - mean[2] * mean[2] - mean[NQ] * mean[NQ] - mean[4] * mean[4], NIL)
    b_first = jnp.sqrt(3.0 * mean[5] + var_s + 2.0 * var_k)
    a_first = jnp.maximum(mean[0] - 0.5 * jnp.sqrt(var_s), 0.3) + 2.0 * b_first

    def set_coefs(k0, a_new, b_new):
        old_b = ST[S_B]
        b_arr = jnp.where(lane >= k0, b_new, old_b)
        ST[S_A] = jnp.where(lane >= k0, a_new, ST[S_A])
        ST[S_B] = b_arr
        ST[S_C] = jnp.where(lane == 0, NIL, turn(b_arr, 1))
        inv = 1.0 / b_new
        for k in range(k0, ITERS):
            CO[k, K_A] = a_new
            if k > k0:
                CO[k, K_C] = b_new
            elif k == 0:
                CO[k, K_C] = jnp.zeros(VREG, jnp.float32)
            else:
                CO[k, K_C] = CO[k - 1, K_B]
            CO[k, K_INV] = inv
            CO[k, K_B] = b_new

    set_coefs(0, a_first, b_first)

    def gram_start(total):
        rho = full_sum(jnp.where((row == 0) & (lane == 0), total, NIL))
        one = jnp.where(lane == 0, 1.0, NIL)
        ST[S_G] = one * rho
        ST[S_CL] = one
        ST[S_DL] = one
        ST[S_LEAD] = jnp.ones(VREG, jnp.float32)
        ST[S_RHO] = rho
        ST[S_RHO0] = rho
        ST[S_HIST] = one * rho

    def gram_load(total):
        ST[S_D] = jnp.broadcast_to(total[0:1], VREG)
        ST[S_E] = jnp.broadcast_to(total[1:2], VREG)

    def gram_step(k):
        a, b, c = ST[S_A], ST[S_B], ST[S_C]
        g, gp, cl, dl = ST[S_G], ST[S_GP], ST[S_CL], ST[S_DL]
        e_row, d_row = ST[S_E], ST[S_D]
        rho, lead = ST[S_RHO], ST[S_LEAD]
        b_k, c_k, a_k = CO[k, K_B], CO[k, K_C], CO[k, K_A]
        at_k, at_k1 = lane == k, lane == k + 1
        rec = ((a - a_k) * g + b * turn(g, LAST)
               + c * turn(g, 1) - c_k * gp) * CO[k, K_INV]
        g_new = jnp.where(lane < k, rec, jnp.where(at_k, e_row, jnp.where(at_k1, d_row, NIL)))
        g_full = jnp.where(at_k1, turn(e_row, 1), g)
        image = a * dl + turn(b * dl, 1) + turn(c * dl, LAST)
        delta = lead * lane_sum(image * g_full)
        alpha = rho / delta
        y = ST[S_Y] + alpha * dl
        cl = cl - alpha * image
        lead = -alpha * b_k * lead
        prod = cl * g_new
        rho_new = lead * lane_sum(prod)
        size = lane_sum(jnp.abs(cl) * jnp.where(lane < k + 2, jnp.sqrt(jnp.maximum(d_row, NIL)), NIL))
        beta = rho_new / rho
        dl = cl + beta * dl
        ST[S_G], ST[S_GP], ST[S_CL], ST[S_DL] = g_new, g, cl, dl
        ST[S_Y], ST[S_RHO], ST[S_LEAD] = y, rho_new, lead
        ST[S_HIST] = jnp.where(at_k1, rho_new, ST[S_HIST])
        inv_alpha = 1.0 / alpha
        ST[S_LA2], ST[S_LB2] = ST[S_LA], ST[S_LB]
        ST[S_LA] = inv_alpha + ST[S_BA]
        ST[S_LB] = jnp.sqrt(jnp.abs(beta)) * inv_alpha
        ST[S_BA] = beta * inv_alpha
        err = size * size / jnp.sqrt(jnp.abs(rho_new) * ST[S_RHO0])
        err = jnp.where(rho_new > NIL, err, 1e30)
        ST[S_ERR] = jnp.maximum(ST[S_ERR], jnp.where(err < 1e30, err, 1e30))

    def renew(k0):
        a_new = 0.5 * (ST[S_LA] + ST[S_LA2])
        b_new = 0.5 * (ST[S_LB] + ST[S_LB2])
        a_ok = (a_new > 0.3) & (a_new < 26.8)
        a_new = jnp.where(a_ok, a_new, a_first)
        b_new = jnp.where(a_ok & (b_new > 0.25 * b_first) & (b_new < 2.0 * b_first), b_new, b_first)
        set_coefs(k0, a_new, b_new)

    def prepare(k):
        before = jnp.maximum(k - 1, 0)
        cols = (PKS[k + 1, 0], PKS[k + 1, 1])
        own = own_faces(cols)
        for h, u in enumerate(cols):
            PRE[h] = (CB[C_D, h] - CO[k, K_A]) * u - own[h] - CO[k, K_C] * PKS[before + 1, h]

    def apply_step(k):
        take_halo(k)
        for h in TILES:
            HK[h] = H[k + 1, h] * KYH[h]
        before = jnp.maximum(k - 1, 0)
        far = outer_faces(Z[k, tb, pl.ds(0, NZ), :], Z[k, tb, pl.ds(HI, NZ), :], (H[k + 1, 0], H[k + 1, 1]))
        for h in TILES:
            PKS[k + 2, h] = (PRE[h] - far[h]) * CO[k, K_INV]

        @pl.when(k < ITERS - 1)
        def _():
            y_copy(k + 1).start()

        a_k, c_k, i_k = three(CO[k, K_A]), three(CO[k, K_C]), three(CO[k, K_INV])

        def plane(i, carry, state):
            dots, cross = carry
            h = i // 32
            j = lax.rem(i, 32)
            r = rowsof(i)
            u, nb, ky, kx, state = neighbours(vec, i, j, H[k + 1, h], HK[h], state)
            for t in TILES:
                val = (D[t, pl.ds(r, NZ), :] - a_k) * u[t] - nb[t] - c_k * Z[before, t, pl.ds(r + NZ, NZ), :]
                val = val * i_k
                Z[k + 1, t, pl.ds(r + NZ, NZ), :] = val
                dots = dots + val * val
                cross = cross + val * u[t]
            return (dots, cross), state

        vec = lambda t, q: Z[k, t, pl.ds(q, NZ), :]
        dots, cross = sweep(vec, plane, k + 1, (zero24, zero24), k < ITERS - 1)

        pack(Z.at[k + 1], NZ, inner, UI)

        tile = jnp.where((row == 0) & (lane == k + 1), full_sum(dots), PT[...])
        tile = jnp.where((row == 1) & (lane == k), full_sum(cross), tile)
        PT[...] = tile
        for e, at in SEND_AT.items():
            @pl.when(k == at)
            def _():
                sum_send(e, tile)
        for at, e in TAKE_AT.items():
            @pl.when(k == at)
            def _():
                total = sum_take(e)
                gram_load(total)
                if e == 1:
                    gram_start(total)
        for at, (lo, hi) in STEPS_AT.items():
            @pl.when(k == at)
            def _():
                @pl.loop(lo, hi)
                def _(s):
                    gram_step(s)
        for at, k0 in RENEW_AT.items():
            @pl.when(k == at)
            def _():
                renew(k0)
        prepare(jnp.minimum(k + 1, ITERS - 1))

    prepare(0)

    @pl.loop(0, ITERS)
    def _(k):
        apply_step(k)

    gram_load(sum_take(4))

    @pl.loop(16, ITERS)
    def _(s):
        gram_step(s)

    y = ST[S_Y]
    for k in range(ITERS):
        YB[k] = lane_sum(jnp.where(lane == k, y, NIL))
    hist = jnp.sqrt(ST[S_HIST] * (1.0 / cells))
    hist_ref[...] = jnp.where(row == 0, hist, ST[S_ERR])

    def combine(i, c):
        r = rowsof(2 * i + 1)
        acc = [X0[t, pl.ds(r, 2 * NZ), :] for t in TILES]
        for k in range(ITERS):
            w = jnp.concatenate([YB[k]] * 6, axis=0)
            for t in TILES:
                acc[t] = acc[t] + w * Z[k, t, pl.ds(r, 2 * NZ), :]
        for t in TILES:
            X0[t, pl.ds(r, 2 * NZ), :] = acc[t]
        return c

    outs = []
    for part in range(4):
        lax.fori_loop(8 * part, 8 * part + 8, combine, 0)
        for t in TILES:
            cp = pltpu.make_async_copy(X0.at[t, pl.ds(NZ + 16 * NZ * part, 16 * NZ), :],
                                       out_h.at[pl.ds(16 * NZ * part, 16 * NZ), pl.ds(LANES * t, LANES)],
                                       osem.at[2 * part + t])
            cp.start()
            outs.append(cp)

    @pl.when(has_hi)
    def _():
        for t in TILES:
            for cp in init_up(t):
                cp.wait_send()

    @pl.when(has_lo)
    def _():
        for t in TILES:
            for cp in init_down(t):
                cp.wait_send()

    @pl.when(py == 0)
    def _():
        ky_copy.wait_send()

    x0_copy.wait_send()

    @pl.loop(0, ITERS)
    def _(k):
        @pl.when(has_hi)
        def _():
            up_copy(k).wait_send()

        @pl.when(has_lo)
        def _():
            down_copy(k).wait_send()

        y_copy(k).wait_send()

    for e in range(5):
        for cp in sum_copies(e):
            cp.wait_send()
    for cp in outs:
        cp.wait()


def fused_solve(shift, rhs_field, x_init, cond_x, cond_y, cond_z):
    def flat(v):
        return jnp.transpose(v, (0, 2, 1)).reshape(BODY, 256)

    f32 = jnp.float32
    any_spec = pl.BlockSpec(memory_space=pl.ANY)
    x_rows, small = pl.pallas_call(
        kernel,
        out_shape=(jax.ShapeDtypeStruct((BODY, 256), f32), jax.ShapeDtypeStruct(VREG, f32)),
        in_specs=[any_spec] * 6,
        out_specs=(any_spec, pl.BlockSpec(memory_space=pltpu.VMEM)),
        scratch_shapes=[
            pltpu.VMEM((ITERS + 1, 2, FULL, LANES), f32),
            pltpu.VMEM((2, FULL, LANES), f32),
            pltpu.VMEM((2, BODY, LANES), f32),
            pltpu.VMEM((2, BODY + 32, LANES), f32),
            pltpu.VMEM((2, BODY, LANES), f32),
            pltpu.VMEM((2, BODY + 16, LANES), f32),
            pltpu.VMEM((ITERS + 2, 2, *VREG), f32),
            pltpu.VMEM((ITERS + 2, 2, *VREG), f32),
            pltpu.VMEM((2, *VREG), f32),
            pltpu.VMEM((2, *VREG), f32),
            pltpu.VMEM((2, *VREG), f32),
            pltpu.VMEM((2, *VREG), f32),
            pltpu.VMEM((TOP, 2, *VREG), f32),
            pltpu.VMEM((2, *VREG), f32),
            pltpu.VMEM((5, *VREG), f32),
            pltpu.VMEM((5, 8, *VREG), f32),
            pltpu.VMEM(VREG, f32),
            pltpu.VMEM((20, *VREG), f32),
            pltpu.VMEM((ITERS, 4, *VREG), f32),
            pltpu.VMEM((ITERS, *VREG), f32),
            pltpu.SemaphoreType.DMA((12,)),
            pltpu.SemaphoreType.DMA((8,)),
            pltpu.SemaphoreType.DMA((8,)),
            pltpu.SemaphoreType.DMA((8,)),
            pltpu.SemaphoreType.DMA((ITERS, NQ)),
            pltpu.SemaphoreType.DMA((ITERS, NQ)),
            pltpu.SemaphoreType.DMA((5, TOP)),
            pltpu.SemaphoreType.DMA((5,)),
        ],
        compiler_params=pltpu.CompilerParams(collective_id=0, has_side_effects=True,
                                             vmem_limit_bytes=65011712),
    )(*(flat(v) for v in (shift, rhs_field, x_init, cond_x, cond_y, cond_z)))
    x_out = jnp.transpose(x_rows.reshape(NX, NZ, 256), (0, 2, 1))
    return x_out, small[0, :ITERS + 1], small[1, 0]


def classic_solve(shift, rhs_field, x_init, cond_x, cond_y, cond_z):
    count_x, count_y = 4, 2
    fwd_x = [(src, src + 1) for src in range(count_x - 1)]
    back_x = [(src + 1, src) for src in range(count_x - 1)]
    pos_x, pos_y = lax.axis_index("px"), lax.axis_index("py")
    plane_x = lax.broadcasted_iota(jnp.int32, (NX, 1, 1), 0)
    plane_y = lax.broadcasted_iota(jnp.int32, (1, ROW, 1), 1)
    plane_z = lax.broadcasted_iota(jnp.int32, (1, 1, NZ), 2)
    plus_x = jnp.where((pos_x == count_x - 1) & (plane_x == NX - 1), NIL, cond_x)
    plus_y = jnp.where((pos_y == count_y - 1) & (plane_y == ROW - 1), NIL, cond_y)
    plus_z = jnp.where(plane_z == NZ - 1, NIL, cond_z)

    def shifted(vec, axis, ahead, halo):
        size = vec.shape[axis]
        if ahead:
            return jnp.concatenate([lax.slice_in_dim(vec, 1, size, axis=axis), halo], axis=axis)
        return jnp.concatenate([halo, lax.slice_in_dim(vec, 0, size - 1, axis=axis)], axis=axis)

    def below(vec):
        low_x = lax.ppermute(vec[-1:], "px", fwd_x)
        low_y = lax.ppermute(vec[:, -1:], "py", [(0, 1)])
        return (shifted(vec, 0, False, low_x), shifted(vec, 1, False, low_y),
                shifted(vec, 2, False, jnp.zeros_like(vec[:, :, :1])))

    def above(vec):
        high_x = lax.ppermute(vec[:1], "px", back_x)
        high_y = lax.ppermute(vec[:, :1], "py", [(1, 0)])
        return (shifted(vec, 0, True, high_x), shifted(vec, 1, True, high_y),
                shifted(vec, 2, True, jnp.zeros_like(vec[:, :, :1])))

    minus_x, minus_y, minus_z = below(plus_x)[0], below(plus_y)[1], below(plus_z)[2]
    diag = shift + plus_x + minus_x + plus_y + minus_y + plus_z + minus_z

    def apply_op(vec):
        up_x, up_y, up_z = above(vec)
        down_x, down_y, down_z = below(vec)
        return (diag * vec - plus_x * up_x - minus_x * down_x
                - plus_y * up_y - minus_y * down_y - plus_z * up_z - minus_z * down_z)

    def global_dot(left, right):
        return lax.psum(jnp.sum(left * right), SUM_AXES)

    res = rhs_field - apply_op(x_init)
    rho = global_dot(res, res)
    history = jnp.where(jnp.arange(ITERS + 1) == 0, rho, NIL)

    def step(k, state):
        x, res, p, rho, history = state
        q = apply_op(p)
        alpha = rho / global_dot(p, q)
        x = x + alpha * p
        res = res - alpha * q
        rho_new = global_dot(res, res)
        p = res + (rho_new / rho) * p
        return x, res, p, rho_new, jnp.where(jnp.arange(ITERS + 1) == k + 1, rho_new, history)

    x, _, _, _, history = lax.fori_loop(0, ITERS, step, (jnp.zeros_like(res), res, res, rho, history))
    return x_init + x, jnp.sqrt(history / CELLS)


def solution(mesh):
    field_spec = P("px", "py", None)

    def local_solve(*fields):
        x_out, history, err = fused_solve(*fields)
        return lax.cond(err < ERR_LIMIT, lambda: (x_out, history), lambda: classic_solve(*fields))

    return jax.shard_map(local_solve, mesh=mesh, in_specs=(field_spec,) * 6,
                         out_specs=(field_spec, P()), check_vma=False)
```

```python
import functools

import jax
import jax.numpy as jnp
from jax import lax
from jax.experimental import pallas as pl
from jax.experimental.pallas import tpu as pltpu
from jax.sharding import PartitionSpec as P

ITERS = 20
SUM_AXES = ("px", "py")
MESH = pl.DeviceIdType.MESH
NX, NZ = 64, 24
ROW = 256
ERR_LIMIT = 1000.0
HALF = NX // 2
CELLS = float(NX * 256 * NZ * 8)
BODY = NX * NZ
FULL = BODY + 2 * NZ
HI = BODY + NZ
OTHERS = tuple((dy, dx) for dy in range(2) for dx in range(4) if (dy, dx) != (0, 0))
RENEW_AT = (7, 12)
VREG = (8, 128)
SUB, LANES = VREG
TILES = range(2)


C_D, C_UP, C_DOWN, C_OUT, C_IN, C_ZUP, C_ZDN = range(7)
K_A, K_C, K_INV, K_B = range(4)
NQ = 3
LAST, TOP, NIL = 127, 7, 0.0


def turn(v, by):
    return pltpu.roll(v, by, 1)


def lift(v, by):
    return pltpu.roll(v, by, 0)


S_A, S_B, S_C, S_GP, S_G, S_CL, S_DL, S_Y, S_RHO, S_LEAD, S_HIST, S_BA, S_LA, S_LB, S_LA2, S_LB2, S_ERR, S_D, S_AL, S_RHO0 = range(20)


def lanes():
    return lax.broadcasted_iota(jnp.int32, VREG, 1)


def rows8():
    return lax.broadcasted_iota(jnp.int32, VREG, 0)


def lane_sum(v):
    return jnp.broadcast_to(jnp.sum(v, axis=1, keepdims=True), VREG)


def full_sum(v):
    return jnp.broadcast_to(jnp.sum(jnp.sum(v, axis=0, keepdims=True), axis=1, keepdims=True), VREG)


def three(v):
    return jnp.concatenate([v, v, v], axis=0)


def kernel(s_h, b_h, x0_h, kx_h, ky_h, kz_h, out_h, hist_ref,
           Z, X0, D, KX, KY, KZ, PKS, H, KYP, KYH, HK, UI, CB, PRE, XS, XG, RS, RR, PT, ST, CO, YB,
           lsem, osem, is_s, is_r, hs, hr, rs, rr):
    px, py = lax.axis_index("px"), lax.axis_index("py")
    me = py * 4 + px
    lane, row = lanes(), rows8()
    lane24 = lax.broadcasted_iota(jnp.int32, (NZ, LANES), 1)
    row24 = lax.broadcasted_iota(jnp.int32, (NZ, LANES), 0)
    first, last = lane24 == 0, lane24 == LAST
    has_lo, has_hi = px > 0, px < NQ

    loads = []
    for n, (src, dst, base) in enumerate((
            (ky_h, KY, 0), (x0_h, X0, NZ), (kx_h, KX, NZ), (s_h, D, 0), (b_h, None, NZ), (kz_h, KZ, 8))):
        for t in TILES:
            to = Z.at[0, t, pl.ds(base, BODY), :] if dst is None else dst.at[t, pl.ds(base, BODY), :]
            cp = pltpu.make_async_copy(src.at[:, pl.ds(LANES * t, LANES)], to, lsem.at[2 * n + t])
            loads.append(cp)
    for cp in loads[:4]:
        cp.start()

    zero_plane = jnp.zeros((NZ, LANES), jnp.float32)
    for t in TILES:
        KX[t, pl.ds(0, NZ), :] = zero_plane
        X0[t, pl.ds(0, NZ), :] = zero_plane
        X0[t, pl.ds(HI, NZ), :] = zero_plane
        KZ[t, pl.ds(0, 8), :] = jnp.zeros(VREG, jnp.float32)
    KYH[...] = jnp.zeros((2, *VREG), jnp.float32)
    for t in TILES:
        for k in range(ITERS + 2):
            XG[k, t] = jnp.zeros(VREG, jnp.float32)

    @pl.loop(0, ITERS + 1)
    def _(k):
        for t in TILES:
            Z[k, t, pl.ds(0, NZ), :] = zero_plane
            Z[k, t, pl.ds(HI, NZ), :] = zero_plane

    barrier = pltpu.get_barrier_semaphore()
    for dy, dx in OTHERS:
        pl.semaphore_signal(barrier, inc=1, device_id=(lax.rem(py + dy, 2), lax.rem(px + dx, 4)),
                            device_id_type=MESH)
    pl.semaphore_wait(barrier, len(OTHERS))

    def to_x(step):
        return (py, px + step)

    to_y = (1 - py, px)

    def remote(src, dst, ssem, rsem, dev):
        return pltpu.make_async_remote_copy(src_ref=src, dst_ref=dst, send_sem=ssem, recv_sem=rsem,
                                            device_id=dev, device_id_type=MESH)

    def init_up(t):
        cols = pl.ds(LANES * t, LANES)
        return (remote(kx_h.at[pl.ds(BODY - NZ, NZ), cols], KX.at[t, pl.ds(0, NZ), :], is_s.at[t], is_r.at[t], to_x(1)),
                remote(x0_h.at[pl.ds(BODY - NZ, NZ), cols], X0.at[t, pl.ds(0, NZ), :], is_s.at[2 + t], is_r.at[2 + t], to_x(1)))

    def init_down(t):
        cols = pl.ds(LANES * t, LANES)
        return (remote(x0_h.at[pl.ds(0, NZ), cols], X0.at[t, pl.ds(HI, NZ), :], is_s.at[4 + t], is_r.at[4 + t], to_x(-1)),)

    @pl.when(has_hi)
    def _():
        for t in TILES:
            for cp in init_up(t):
                cp.start()

    @pl.when(has_lo)
    def _():
        for t in TILES:
            for cp in init_down(t):
                cp.start()

    tb = 1 - py
    edge = LAST * (1 - py)
    inner = 126 + py * (1 - 126)

    def pack_one(items, bl):
        rel = lax.rem(lane - bl + LANES, LANES)
        s = 1
        while len(items) > NQ:
            keep = rel < s
            items = [jnp.where(keep, items[n], turn(items[n + 1], s)) for n in range(0, len(items), 2)]
            s *= 2
        out = jnp.where(rel < s, items[0],
                        jnp.where(rel < 2 * s, turn(items[1], s), turn(items[2], 2 * s)))
        return out

    def pack(ref, base, bl, dst):
        start = NQ - bl + LANES
        for h in TILES:
            accs = [jnp.zeros(VREG, jnp.float32)] * NQ
            for a in range(NQ * HALF):
                v = ref[tb, pl.ds(base + HALF * NZ * h + SUB * a, SUB), :]
                moved = turn(v, lax.rem(start + a, LANES))
                accs[a % NQ] = jnp.where(lane == a + NQ, moved, accs[a % NQ])
            dst[h] = accs[0] + accs[1] + accs[2]

    from_lo, from_hi = (lane >= NQ) & (lane < 6), (lane >= NQ * HALF) & (lane < NQ * HALF + NQ)
    low_ghost = lane < NQ
    high_ghost = (lane >= 99) & (lane < 102)

    def with_ghosts(n0, n1, lo, hi):
        lo = turn(pack_one([lo[SUB * q:SUB * q + SUB] for q in range(NQ)], edge), lax.rem(LANES - edge, LANES))
        hi = turn(pack_one([hi[SUB * q:SUB * q + SUB] for q in range(NQ)], edge), lax.rem(99 - edge + LANES, LANES))
        return (jnp.where(low_ghost, lo, jnp.where(high_ghost, turn(n1, 96), n0)),
                jnp.where(low_ghost, turn(n0, 32), jnp.where(high_ghost, hi, n1)))

    def z_up(v):
        return jnp.where(row == TOP, lift(turn(v, LAST), TOP), lift(v, TOP))

    def z_down(v):
        return jnp.where(row == 0, lift(turn(v, 1), 1), lift(v, 1))

    def unpack(tile, j):
        parts = [turn(tile, 124 + py - (NQ * j + q)) for q in range(NQ)]
        return jnp.concatenate(parts, axis=0)

    def rowsof(i):
        return pl.multiple_of(NZ * i, 8)

    for cp in loads[:4]:
        cp.wait()
    for cp in loads[4:]:
        cp.start()
    pack(KY, 0, edge, KYP)
    ky_copy = remote(KYP, KYH, is_s.at[6], is_r.at[6], to_y)

    @pl.when(py == 0)
    def _():
        ky_copy.start()

    pack(X0, NZ, edge, PKS.at[0])
    x0_copy = remote(PKS.at[0], H.at[0], is_s.at[TOP], is_r.at[TOP], to_y)
    x0_copy.start()

    pack(X0, NZ, inner, UI)
    pack(KY, 0, inner, CB.at[C_IN])
    for cp in loads[4:6]:
        cp.wait()
    pack(KX, NZ, edge, CB.at[C_UP])
    for cp in loads[6:8]:
        cp.wait()
    pack(D, 0, edge, CB.at[C_D])
    for cp in loads[8:10]:
        cp.wait()
    pack(Z.at[0], NZ, edge, PRE)
    for cp in loads[10:]:
        cp.wait()

    keep_x = jnp.where(has_hi, 1.0, NIL)
    for t in TILES:
        KX[t, pl.ds(BODY, NZ), :] = KX[t, pl.ds(BODY, NZ), :] * keep_x
    dead_y = last & (py == 1)
    dead_z = row24 == NZ - 1

    def mask_step(i, acc):
        s1, s2, kx1, ky1, kz1, k2 = acc
        r = rowsof(i)
        for t in TILES:
            s = D[t, pl.ds(r, NZ), :]
            kx = KX[t, pl.ds(r + NZ, NZ), :]
            ky = KY[t, pl.ds(r, NZ), :]
            kz = jnp.where(dead_z, NIL, KZ[t, pl.ds(r + SUB, NZ), :])
            if t == 1:
                ky = jnp.where(dead_y, NIL, ky)
                KY[t, pl.ds(r, NZ), :] = ky
            KZ[t, pl.ds(r + SUB, NZ), :] = kz
            s1, s2 = s1 + s, s2 + s * s
            kx1, ky1, kz1 = kx1 + kx, ky1 + ky, kz1 + kz
            k2 = k2 + (kx * kx + ky * ky + kz * kz)
        return s1, s2, kx1, ky1, kz1, k2

    sums = lax.fori_loop(0, NX, mask_step, (zero_plane,) * 6, unroll=4)
    stats = jnp.zeros(VREG, jnp.float32)
    for n, v in enumerate(sums):
        stats = jnp.where((row == 2) & (lane == n), full_sum(v), stats)

    def sum_copies(e):
        return [remote(RS.at[e], RR.at[e, me], rs.at[e, n], rr.at[e],
                       (lax.rem(py + dy, 2), lax.rem(px + dx, 4))) for n, (dy, dx) in enumerate(OTHERS)]

    def sum_send(e, tile):
        RS[e] = tile
        RR[e, me] = tile
        for cp in sum_copies(e):
            cp.start()

    def sum_wait(e):
        pltpu.make_async_copy(RR.at[e, pl.ds(0, TOP)], RR.at[e, pl.ds(0, TOP)], rr.at[e]).wait()

    def sum_total(e):
        total = RR[e, 0]
        for n in range(1, 8):
            total = total + RR[e, n]
        return total

    def sum_take(e):
        sum_wait(e)
        return sum_total(e)

    sum_send(0, stats)
    for h in TILES:
        last_x = (lane >= NQ * HALF) & (lane < NQ * HALF + NQ)
        if h == 1:
            CB[C_UP, h] = jnp.where(last_x, CB[C_UP, h] * keep_x, CB[C_UP, h])
        CB[C_OUT, h] = KYP[h]
    pack(KZ, 8, edge, CB.at[C_ZUP])
    for h in TILES:
        CB[C_ZDN, h] = z_down(CB[C_ZUP, h])

    def up_copy(k):
        return remote(Z.at[k, :, pl.ds(BODY, NZ), :], Z.at[k, :, pl.ds(0, NZ), :], hs.at[k, 0], hr.at[k, 0], to_x(1))

    def down_copy(k):
        return remote(Z.at[k, :, pl.ds(NZ, NZ), :], Z.at[k, :, pl.ds(HI, NZ), :], hs.at[k, 1], hr.at[k, 1], to_x(-1))

    def y_copy(k):
        return remote(PKS.at[k + 1], H.at[k + 1], hs.at[k, 2], hr.at[k, 2], to_y)

    def edge_up(k):
        return remote(XS.at[k + 1, 0], XG.at[k + 1, 0], hs.at[k, NQ], hr.at[k, NQ], to_x(1))

    def edge_down(k):
        return remote(XS.at[k + 1, 1], XG.at[k + 1, 1], hs.at[k, 4], hr.at[k, 4], to_x(-1))

    def send_column(k):
        y_copy(k).start()
        XS[k + 1, 0] = jnp.where(from_lo, turn(PKS[k + 1, 1], 35), NIL)
        XS[k + 1, 1] = jnp.where(from_hi, turn(PKS[k + 1, 0], 93), NIL)

        @pl.when(has_hi)
        def _():
            edge_up(k).start()

        @pl.when(has_lo)
        def _():
            edge_down(k).start()

    def take_column(k):
        @pl.when(has_lo)
        def _():
            edge_up(k).wait_recv()

        @pl.when(has_hi)
        def _():
            edge_down(k).wait_recv()

        y_copy(k).wait_recv()

    def send_x(k):
        @pl.when(has_hi)
        def _():
            up_copy(k).start()

        @pl.when(has_lo)
        def _():
            down_copy(k).start()

    def take_halo(k):
        @pl.when(has_lo)
        def _():
            up_copy(k).wait_recv()

        @pl.when(has_hi)
        def _():
            down_copy(k).wait_recv()


    def first_state(vec, i):
        r = rowsof(i)
        return ([vec(t, r) for t in TILES], [vec(t, r + NZ) for t in TILES],
                [KX[t, pl.ds(r, NZ), :] for t in TILES])

    def neighbours(vec, i, j, tile_raw, tile_k, state):
        r = rowsof(i)
        x_down, u, kx_down = state
        x_up = [vec(t, r + 2 * NZ) for t in TILES]
        kx = [KX[t, pl.ds(r + NZ, NZ), :] for t in TILES]
        ky = [KY[t, pl.ds(r, NZ), :] for t in TILES]
        up = [turn(u[t], LAST) for t in TILES]
        down = [turn(ky[t] * u[t], 1) for t in TILES]
        y_up = [jnp.where(last, up[1], up[0]), jnp.where(last, unpack(tile_raw, j), up[1])]
        y_down = [jnp.where(first, unpack(tile_k, j), down[0]), jnp.where(first, down[0], down[1])]
        out = []
        for t in TILES:
            part = ky[t] * y_up[t] + y_down[t]
            part = part + kx[t] * x_up[t]
            part = part + kx_down[t] * x_down[t]
            part = part + KZ[t, pl.ds(r + SUB, NZ), :] * vec(t, r + NZ + 1)
            part = part + KZ[t, pl.ds(r + TOP, NZ), :] * vec(t, r + NZ - 1)
            out.append(part)
        return u, out, ky, kx, (u, x_up, kx)

    @pl.when(has_lo)
    def _():
        for t in TILES:
            for cp in init_up(t):
                cp.wait_recv()

    @pl.when(has_hi)
    def _():
        for t in TILES:
            for cp in init_down(t):
                cp.wait_recv()

    @pl.when(py == 1)
    def _():
        ky_copy.wait_recv()

    x0_copy.wait_recv()
    for h in TILES:
        HK[h] = H[0, h] * KYH[h]

    def own_faces(cols):
        n0, n1 = cols
        down = (jnp.where(from_lo, NIL, turn(n0, NQ)), jnp.where(from_lo, turn(n0, 35), turn(n1, NQ)))
        up = (jnp.where(from_hi, turn(n1, 93), turn(n0, 125)), jnp.where(from_hi, NIL, turn(n1, 125)))
        return [CB[C_IN, h] * UI[h] + CB[C_UP, h] * up[h] + CB[C_DOWN, h] * down[h]
                + CB[C_ZUP, h] * z_up(u) + CB[C_ZDN, h] * z_down(u) for h, u in enumerate(cols)]

    def outer_faces(lo, hi, beyond):
        ghost = [jnp.zeros(VREG, jnp.float32)] * 2
        for q in range(NQ):
            for h, (v, at) in enumerate(((lo, NQ), (hi, NQ * HALF))):
                at = at + q
                moved = turn(v[SUB * q:SUB * q + SUB], lax.rem(at - edge + LANES, LANES))
                ghost[h] = jnp.where(lane == at, moved, ghost[h])
        return [CB[C_OUT, h] * beyond[h] + CB[C_DOWN - h, h] * ghost[h] for h in TILES]

    x0_vec = lambda t, q: X0[t, pl.ds(q, NZ), :]

    def start_plane(i, rho, state):
        h = i // 32
        j = lax.rem(i, 32)
        r = rowsof(i)
        kx_down = state[2]
        u, nb, ky, kx, state = neighbours(x0_vec, i, j, H[0, h], HK[h], state)
        down = [turn(ky[t], 1) for t in TILES]
        ky_lo = [jnp.where(first, unpack(KYH[h], j), down[0]), jnp.where(first, down[0], down[1])]
        for t in TILES:
            diag = D[t, pl.ds(r, NZ), :] + ky[t] + ky_lo[t] + kx[t] + kx_down[t]
            diag = diag + KZ[t, pl.ds(r + SUB, NZ), :] + KZ[t, pl.ds(r + TOP, NZ), :]
            D[t, pl.ds(r, NZ), :] = diag
            res = Z[0, t, pl.ds(r + NZ, NZ), :] - (diag * u[t] - nb[t])
            Z[0, t, pl.ds(r + NZ, NZ), :] = res
            rho = rho + res * res
        return rho, state

    UNROLL = 31

    def sweep(vec, plane, k, sums1, more):
        def run(i, n, c):
            state = first_state(vec, i)
            for m in range(n):
                c, state = plane(i + m, c, state)
            return c

        sums1 = run(NX - 1, 1, run(0, 1, sums1))

        @pl.when(more)
        def _():
            send_x(k)

        return lax.fori_loop(0, (NX - 2) // UNROLL, lambda m, c: run(1 + UNROLL * m, UNROLL, c), sums1)

    zero24 = zero_plane
    zero_tile = zero_plane
    kx_cols = with_ghosts(CB[C_UP, 0], CB[C_UP, 1], KX[tb, pl.ds(0, NZ), :], zero_tile)
    for h in TILES:
        CB[C_DOWN, h] = turn(kx_cols[h], NQ)
        ky_edge, ky_in = CB[C_OUT, h], CB[C_IN, h]
        CB[C_OUT, h] = jnp.where(py == 0, ky_edge, KYH[h])
        CB[C_IN, h] = jnp.where(py == 0, ky_in, ky_edge)
    far = outer_faces(X0[tb, pl.ds(0, NZ), :], X0[tb, pl.ds(HI, NZ), :], (H[0, 0], H[0, 1]))
    own = own_faces((PKS[0, 0], PKS[0, 1]))
    for h in TILES:
        diag = CB[C_D, h] + CB[C_UP, h] + CB[C_DOWN, h] + CB[C_OUT, h] + CB[C_IN, h] + CB[C_ZUP, h] + CB[C_ZDN, h]
        CB[C_D, h] = diag
        PKS[1, h] = PRE[h] - (diag * PKS[0, h] - far[h] - own[h])
    send_column(0)
    rho0 = sweep(x0_vec, start_plane, 0, zero24, px >= 0)
    pack(Z.at[0], NZ, inner, UI)
    PT[...] = jnp.where((row == 0) & (lane == 0), full_sum(rho0), NIL)

    for n in range(20):
        ST[n] = jnp.zeros(VREG, jnp.float32)
    totals = sum_take(0)
    cells = CELLS
    mean = [full_sum(jnp.where((row == 2) & (lane == n), totals, NIL)) * (1.0 / cells) for n in range(6)]
    var_s = jnp.maximum(mean[1] - mean[0] * mean[0], NIL)
    var_k = jnp.maximum(mean[5] - mean[2] * mean[2] - mean[NQ] * mean[NQ] - mean[4] * mean[4], NIL)
    b_first = jnp.sqrt(3.0 * mean[5] + var_s + 2.0 * var_k)
    a_first = jnp.maximum(mean[0] - 0.5 * jnp.sqrt(var_s), 0.3) + 2.0 * b_first

    def set_coefs(k0, a_new, b_new):
        old_b = ST[S_B]
        b_arr = jnp.where(lane >= k0, b_new, old_b)
        ST[S_A] = jnp.where(lane >= k0, a_new, ST[S_A])
        ST[S_B] = b_arr
        ST[S_C] = jnp.where(lane == 0, NIL, turn(b_arr, 1))
        inv = 1.0 / b_new
        for k in range(k0, ITERS):
            CO[k, K_A] = a_new
            if k > k0:
                CO[k, K_C] = b_new
            elif k == 0:
                CO[k, K_C] = jnp.zeros(VREG, jnp.float32)
            else:
                CO[k, K_C] = CO[k - 1, K_B]
            CO[k, K_INV] = inv
            CO[k, K_B] = b_new

    set_coefs(0, a_first, b_first)

    def gram_start(total):
        rho = full_sum(jnp.where((row == 0) & (lane == 0), total, NIL))
        one = jnp.where(lane == 0, 1.0, NIL)
        for n in (S_GP, S_Y, S_BA, S_LA, S_LB, S_LA2, S_LB2, S_ERR):
            ST[n] = jnp.zeros(VREG, jnp.float32)
        ST[S_G] = one * rho
        ST[S_CL] = one
        ST[S_DL] = one
        ST[S_LEAD] = jnp.ones(VREG, jnp.float32)
        ST[S_RHO] = rho
        ST[S_RHO0] = rho
        ST[S_HIST] = one * rho

    def gram_step(k, total):
        a, b, c = ST[S_A], ST[S_B], ST[S_C]
        g, gp, cl, dl = ST[S_G], ST[S_GP], ST[S_CL], ST[S_DL]
        d_row, e_row = jnp.broadcast_to(total[0:1], VREG), jnp.broadcast_to(total[1:2], VREG)
        rho, lead = ST[S_RHO], ST[S_LEAD]
        b_k, c_k, a_k = CO[k, K_B], CO[k, K_C], CO[k, K_A]
        at_k, at_k1 = lane == k, lane == k + 1
        rec = ((a - a_k) * g + b * turn(g, LAST)
               + c * turn(g, 1) - c_k * gp) * CO[k, K_INV]
        g_new = jnp.where(lane < k, rec, jnp.where(at_k, e_row, jnp.where(at_k1, d_row, NIL)))
        g_full = jnp.where(at_k1, turn(e_row, 1), g)
        image = a * dl + turn(b * dl, 1) + turn(c * dl, LAST)
        delta = lead * lane_sum(image * g_full)
        alpha = rho / delta
        ST[S_AL] = alpha
        y = ST[S_Y] + alpha * dl
        cl = cl - alpha * image
        lead = -alpha * b_k * lead
        prod = cl * g_new
        rho_new = lead * lane_sum(prod)
        size = lane_sum(jnp.abs(cl) * jnp.where(lane < k + 2, jnp.sqrt(jnp.maximum(d_row, NIL)), NIL))
        beta = rho_new / rho
        dl = cl + beta * dl
        ST[S_G], ST[S_GP], ST[S_CL], ST[S_DL] = g_new, g, cl, dl
        ST[S_Y], ST[S_RHO], ST[S_LEAD] = y, rho_new, lead
        ST[S_HIST] = jnp.where(at_k1, rho_new, ST[S_HIST])
        inv_alpha = 1.0 / alpha
        ST[S_LA2], ST[S_LB2] = ST[S_LA], ST[S_LB]
        ST[S_LA] = inv_alpha + ST[S_BA]
        ST[S_LB] = jnp.sqrt(jnp.abs(beta)) * inv_alpha
        ST[S_BA] = beta * inv_alpha
        err = size * size / jnp.sqrt(jnp.abs(rho_new) * ST[S_RHO0])
        err = jnp.where(rho_new > NIL, err, 1e30)
        ST[S_ERR] = jnp.maximum(ST[S_ERR], jnp.where(err < 1e30, err, 1e30))

    def renew(k0):
        a_new = 0.5 * (ST[S_LA] + ST[S_LA2])
        b_new = 0.5 * (ST[S_LB] + ST[S_LB2])
        a_ok = (a_new > 0.3) & (a_new < 26.8)
        a_new = jnp.where(a_ok, a_new, a_first)
        b_new = jnp.where(a_ok & (b_new > 0.25 * b_first) & (b_new < 2.0 * b_first), b_new, b_first)
        set_coefs(k0, a_new, b_new)

    def prepare(k):
        before = jnp.maximum(k - 1, 0)
        cols = (PKS[k + 1, 0], PKS[k + 1, 1])
        own = own_faces(cols)
        for h, u in enumerate(cols):
            PRE[h] = (CB[C_D, h] - CO[k, K_A]) * u - own[h] - CO[k, K_C] * PKS[before + 1, h]

    def apply_step(k):
        take_column(k)
        before = jnp.maximum(k - 1, 0)
        for h in TILES:
            far = CB[C_OUT, h] * H[k + 1, h] + CB[C_DOWN - h, h] * XG[k + 1, h]
            PKS[k + 2, h] = (PRE[h] - far) * CO[k, K_INV]

        @pl.when(k < ITERS - 1)
        def _():
            send_column(k + 1)

        for h in TILES:
            HK[h] = H[k + 1, h] * KYH[h]
        take_halo(k)
        a_k, c_k, i_k = three(CO[k, K_A]), three(CO[k, K_C]), three(CO[k, K_INV])

        def plane(i, carry, state):
            dots, cross = carry
            h = i // 32
            j = lax.rem(i, 32)
            r = rowsof(i)
            u, nb, ky, kx, state = neighbours(vec, i, j, H[k + 1, h], HK[h], state)
            for t in TILES:
                val = (D[t, pl.ds(r, NZ), :] - a_k) * u[t] - nb[t] - c_k * Z[before, t, pl.ds(r + NZ, NZ), :]
                val = val * i_k
                Z[k + 1, t, pl.ds(r + NZ, NZ), :] = val
                dots = dots + val * val
                cross = cross + val * u[t]
            return (dots, cross), state

        vec = lambda t, q: Z[k, t, pl.ds(q, NZ), :]
        dots, cross = sweep(vec, plane, k + 1, (zero24, zero24), k < ITERS - 1)

        step = k - 2

        @pl.when(step > 0)
        def _():
            sum_wait(step + 1)

        total = sum_total(jnp.maximum(step + 1, 0))
        pack(Z.at[k + 1], NZ, inner, UI)
        tile = jnp.where((row == 0) & (lane == k + 1), full_sum(dots), PT[...])
        tile = jnp.where((row == 1) & (lane == k), full_sum(cross), tile)
        PT[...] = tile
        gram_step(jnp.maximum(step, 0), total)
        prepare(jnp.minimum(k + 1, ITERS - 1))
        sum_send(k + 1, tile)

        @pl.when(k == 1)
        def _():
            gram_start(sum_take(1))

        for at in RENEW_AT:
            @pl.when(k == at)
            def _():
                renew(at + 2)

    prepare(0)

    @pl.loop(0, ITERS)
    def _(k):
        apply_step(k)

    gram_step(ITERS - 2, sum_take(ITERS - 1))

    y, d = ST[S_Y], ST[S_DL]
    for k in range(ITERS):
        YB[k] = lane_sum(jnp.where(lane == k, y, NIL))
        YB[ITERS + k] = lane_sum(jnp.where(lane == k, d, NIL))

    AHEAD = 32

    def combine(i, c):
        r = rowsof(i + 1)
        acc = [X0[t, pl.ds(r, NZ), :] for t in TILES]
        way = [zero_plane, zero_plane]
        for k in range(ITERS):
            w, v = three(YB[k]), three(YB[ITERS + k])
            for t in TILES:
                z = Z[k, t, pl.ds(r, NZ), :]
                way[t] = way[t] + v * z
                if k < ITERS - 1:
                    acc[t] = acc[t] + w * z
        for t in TILES:
            X0[t, pl.ds(r, NZ), :] = acc[t]
            Z[ITERS, t, pl.ds(r, NZ), :] = way[t]
        return c

    lax.fori_loop(0, AHEAD, combine, 0, unroll=2)
    gram_step(ITERS - 1, sum_take(ITERS))
    y = ST[S_Y]
    for k in range(ITERS):
        YB[k] = lane_sum(jnp.where(lane == k, y, NIL))
    hist = jnp.sqrt(ST[S_HIST] * (1.0 / cells))
    hist_ref[...] = jnp.where(row == 0, hist, ST[S_ERR])
    alpha = three(ST[S_AL])

    def last_step(i, c):
        r = rowsof(i + 1)
        for t in TILES:
            X0[t, pl.ds(r, NZ), :] = X0[t, pl.ds(r, NZ), :] + alpha * Z[ITERS, t, pl.ds(r, NZ), :]
        return c

    def whole_step(i, c):
        r = rowsof(i + 1)
        acc = [X0[t, pl.ds(r, NZ), :] for t in TILES]
        for k in range(ITERS):
            w = three(YB[k])
            for t in TILES:
                acc[t] = acc[t] + w * Z[k, t, pl.ds(r, NZ), :]
        for t in TILES:
            X0[t, pl.ds(r, NZ), :] = acc[t]
        return c

    outs = []
    for part in range(4):
        if part < NQ:
            lax.fori_loop(16 * part, min(16 * part + 16, AHEAD), last_step, 0, unroll=4)
        if 16 * part + 16 > AHEAD:
            lax.fori_loop(max(16 * part, AHEAD), 16 * part + 16, whole_step, 0, unroll=2)
        for t in TILES:
            cp = pltpu.make_async_copy(X0.at[t, pl.ds(NZ + 16 * NZ * part, 16 * NZ), :],
                                       out_h.at[pl.ds(16 * NZ * part, 16 * NZ), pl.ds(LANES * t, LANES)],
                                       osem.at[2 * part + t])
            cp.start()
            outs.append(cp)

    @pl.when(has_hi)
    def _():
        for t in TILES:
            for cp in init_up(t):
                cp.wait_send()

    @pl.when(has_lo)
    def _():
        for t in TILES:
            for cp in init_down(t):
                cp.wait_send()

    @pl.when(py == 0)
    def _():
        ky_copy.wait_send()

    x0_copy.wait_send()

    @pl.loop(0, ITERS)
    def _(k):
        @pl.when(has_hi)
        def _():
            up_copy(k).wait_send()
            edge_up(k).wait_send()

        @pl.when(has_lo)
        def _():
            down_copy(k).wait_send()
            edge_down(k).wait_send()

        y_copy(k).wait_send()

    @pl.loop(0, ITERS + 1)
    def _(e):
        for cp in sum_copies(e):
            cp.wait_send()

    for cp in outs:
        cp.wait()


def fused_solve(shift, rhs_field, x_init, cond_x, cond_y, cond_z):
    def flat(v):
        return jnp.transpose(v, (0, 2, 1)).reshape(BODY, 256)

    f32 = jnp.float32
    any_spec = pl.BlockSpec(memory_space=pl.ANY)
    x_rows, small = pl.pallas_call(
        kernel,
        out_shape=(jax.ShapeDtypeStruct((BODY, 256), f32), jax.ShapeDtypeStruct(VREG, f32)),
        in_specs=[any_spec] * 6,
        out_specs=(any_spec, pl.BlockSpec(memory_space=pltpu.VMEM)),
        scratch_shapes=[
            pltpu.VMEM((ITERS + 1, 2, FULL, LANES), f32),
            pltpu.VMEM((2, FULL, LANES), f32),
            pltpu.VMEM((2, BODY, LANES), f32),
            pltpu.VMEM((2, BODY + 32, LANES), f32),
            pltpu.VMEM((2, BODY, LANES), f32),
            pltpu.VMEM((2, BODY + 16, LANES), f32),
            pltpu.VMEM((ITERS + 2, 2, *VREG), f32),
            pltpu.VMEM((ITERS + 2, 2, *VREG), f32),
            pltpu.VMEM((2, *VREG), f32),
            pltpu.VMEM((2, *VREG), f32),
            pltpu.VMEM((2, *VREG), f32),
            pltpu.VMEM((2, *VREG), f32),
            pltpu.VMEM((TOP, 2, *VREG), f32),
            pltpu.VMEM((2, *VREG), f32),
            pltpu.VMEM((ITERS + 2, 2, *VREG), f32),
            pltpu.VMEM((ITERS + 2, 2, *VREG), f32),
            pltpu.VMEM((ITERS + 1, *VREG), f32),
            pltpu.VMEM((ITERS + 1, 8, *VREG), f32),
            pltpu.VMEM(VREG, f32),
            pltpu.VMEM((20, *VREG), f32),
            pltpu.VMEM((ITERS, 4, *VREG), f32),
            pltpu.VMEM((2 * ITERS, *VREG), f32),
            pltpu.SemaphoreType.DMA((12,)),
            pltpu.SemaphoreType.DMA((8,)),
            pltpu.SemaphoreType.DMA((8,)),
            pltpu.SemaphoreType.DMA((8,)),
            pltpu.SemaphoreType.DMA((ITERS, 5)),
            pltpu.SemaphoreType.DMA((ITERS, 5)),
            pltpu.SemaphoreType.DMA((ITERS + 1, TOP)),
            pltpu.SemaphoreType.DMA((ITERS + 1,)),
        ],
        compiler_params=pltpu.CompilerParams(collective_id=0, has_side_effects=True,
                                             vmem_limit_bytes=65011712),
    )(*(flat(v) for v in (shift, rhs_field, x_init, cond_x, cond_y, cond_z)))
    x_out = jnp.transpose(x_rows.reshape(NX, NZ, 256), (0, 2, 1))
    return x_out, small[0, :ITERS + 1], small[1, 0]


def classic_solve(shift, rhs_field, x_init, cond_x, cond_y, cond_z):
    count_x, count_y = 4, 2
    fwd_x = [(src, src + 1) for src in range(count_x - 1)]
    back_x = [(src + 1, src) for src in range(count_x - 1)]
    pos_x, pos_y = lax.axis_index("px"), lax.axis_index("py")
    plane_x = lax.broadcasted_iota(jnp.int32, (NX, 1, 1), 0)
    plane_y = lax.broadcasted_iota(jnp.int32, (1, ROW, 1), 1)
    plane_z = lax.broadcasted_iota(jnp.int32, (1, 1, NZ), 2)
    plus_x = jnp.where((pos_x == count_x - 1) & (plane_x == NX - 1), NIL, cond_x)
    plus_y = jnp.where((pos_y == count_y - 1) & (plane_y == ROW - 1), NIL, cond_y)
    plus_z = jnp.where(plane_z == NZ - 1, NIL, cond_z)

    def shifted(vec, axis, ahead, halo):
        size = vec.shape[axis]
        if ahead:
            return jnp.concatenate([lax.slice_in_dim(vec, 1, size, axis=axis), halo], axis=axis)
        return jnp.concatenate([halo, lax.slice_in_dim(vec, 0, size - 1, axis=axis)], axis=axis)

    def below(vec):
        low_x = lax.ppermute(vec[-1:], "px", fwd_x)
        low_y = lax.ppermute(vec[:, -1:], "py", [(0, 1)])
        return (shifted(vec, 0, False, low_x), shifted(vec, 1, False, low_y),
                shifted(vec, 2, False, jnp.zeros_like(vec[:, :, :1])))

    def above(vec):
        high_x = lax.ppermute(vec[:1], "px", back_x)
        high_y = lax.ppermute(vec[:, :1], "py", [(1, 0)])
        return (shifted(vec, 0, True, high_x), shifted(vec, 1, True, high_y),
                shifted(vec, 2, True, jnp.zeros_like(vec[:, :, :1])))

    minus_x, minus_y, minus_z = below(plus_x)[0], below(plus_y)[1], below(plus_z)[2]
    diag = shift + plus_x + minus_x + plus_y + minus_y + plus_z + minus_z

    def apply_op(vec):
        up_x, up_y, up_z = above(vec)
        down_x, down_y, down_z = below(vec)
        return (diag * vec - plus_x * up_x - minus_x * down_x
                - plus_y * up_y - minus_y * down_y - plus_z * up_z - minus_z * down_z)

    def global_dot(left, right):
        return lax.psum(jnp.sum(left * right), SUM_AXES)

    res = rhs_field - apply_op(x_init)
    rho = global_dot(res, res)
    history = jnp.where(jnp.arange(ITERS + 1) == 0, rho, NIL)

    def step(k, state):
        x, res, p, rho, history = state
        q = apply_op(p)
        alpha = rho / global_dot(p, q)
        x = x + alpha * p
        res = res - alpha * q
        rho_new = global_dot(res, res)
        p = res + (rho_new / rho) * p
        return x, res, p, rho_new, jnp.where(jnp.arange(ITERS + 1) == k + 1, rho_new, history)

    x, _, _, _, history = lax.fori_loop(0, ITERS, step, (jnp.zeros_like(res), res, res, rho, history))
    return x_init + x, jnp.sqrt(history / CELLS)


def solution(mesh):
    field_spec = P("px", "py", None)

    def local_solve(*fields):
        x_out, history, err = fused_solve(*fields)
        return lax.cond(err < ERR_LIMIT, lambda: (x_out, history), lambda: classic_solve(*fields))

    return jax.shard_map(local_solve, mesh=mesh, in_specs=(field_spec,) * 6,
                         out_specs=(field_spec, P()), check_vma=False)
```

```python
import functools

import jax
import jax.numpy as jnp
from jax import lax
from jax.experimental import pallas as pl
from jax.experimental.pallas import tpu as pltpu
from jax.sharding import PartitionSpec as P

ITERS = 20
SUM_AXES = ("px", "py")
MESH = pl.DeviceIdType.MESH
NX, NZ = 64, 24
ROW = 256
ERR_LIMIT = 1000.0
HALF = NX // 2
CELLS = float(NX * 256 * NZ * 8)
BODY = NX * NZ
FULL = BODY + 2 * NZ
HI = BODY + NZ
OTHERS = tuple((dy, dx) for dy in range(2) for dx in range(4) if (dy, dx) != (0, 0))
RENEW_AT = (7, 12)
VREG = (8, 128)
SUB, LANES = VREG
TILES = range(2)


C_D, C_UP, C_DOWN, C_OUT, C_IN, C_ZUP, C_ZDN = range(7)
K_A, K_C, K_INV, K_B = range(4)
NQ = 3
LAST, TOP, NIL = 127, 7, 0.0


def turn(v, by):
    return pltpu.roll(v, by, 1)


def lift(v, by):
    return pltpu.roll(v, by, 0)


S_A, S_B, S_C, S_GP, S_G, S_CL, S_DL, S_Y, S_RHO, S_LEAD, S_HIST, S_BA, S_LA, S_LB, S_LA2, S_LB2, S_ERR, S_D, S_AL, S_RHO0 = range(20)


def lanes():
    return lax.broadcasted_iota(jnp.int32, VREG, 1)


def rows8():
    return lax.broadcasted_iota(jnp.int32, VREG, 0)


def lane_sum(v):
    return jnp.broadcast_to(jnp.sum(v, axis=1, keepdims=True), VREG)


def full_sum(v):
    return jnp.broadcast_to(jnp.sum(jnp.sum(v, axis=0, keepdims=True), axis=1, keepdims=True), VREG)


def three(v):
    return jnp.concatenate([v, v, v], axis=0)


def kernel(s_h, b_h, x0_h, kx_h, ky_h, kz_h, out_ref, hist_ref,
           Z, X0, D, KX, KY, KZ, PKS, H, KYP, KYH, HK, UI, CB, PRE, XS, XG, RS, RR, PT, ST, CO, YB,
           lsem, is_s, is_r, hs, hr, rs, rr):
    px, py = lax.axis_index("px"), lax.axis_index("py")
    me = py * 4 + px
    lane, row = lanes(), rows8()
    lane24 = lax.broadcasted_iota(jnp.int32, (NZ, LANES), 1)
    row24 = lax.broadcasted_iota(jnp.int32, (NZ, LANES), 0)
    first, last = lane24 == 0, lane24 == LAST
    has_lo, has_hi = px > 0, px < NQ

    loads = []
    for n, (src, dst, base) in enumerate((
            (ky_h, KY, 0), (x0_h, X0, NZ), (kx_h, KX, NZ), (s_h, D, 0), (b_h, None, NZ), (kz_h, KZ, 8))):
        for t in TILES:
            to = Z.at[0, t, pl.ds(base, BODY), :] if dst is None else dst.at[t, pl.ds(base, BODY), :]
            cp = pltpu.make_async_copy(src.at[:, pl.ds(LANES * t, LANES)], to, lsem.at[2 * n + t])
            loads.append(cp)
    for cp in loads[:4]:
        cp.start()

    zero_plane = jnp.zeros((NZ, LANES), jnp.float32)
    for t in TILES:
        KX[t, pl.ds(0, NZ), :] = zero_plane
        X0[t, pl.ds(0, NZ), :] = zero_plane
        X0[t, pl.ds(HI, NZ), :] = zero_plane
        KZ[t, pl.ds(0, 8), :] = jnp.zeros(VREG, jnp.float32)
    KYH[...] = jnp.zeros((2, *VREG), jnp.float32)
    for t in TILES:
        for k in range(ITERS + 2):
            XG[k, t] = jnp.zeros(VREG, jnp.float32)

    @pl.loop(0, ITERS + 1)
    def _(k):
        for t in TILES:
            Z[k, t, pl.ds(0, NZ), :] = zero_plane
            Z[k, t, pl.ds(HI, NZ), :] = zero_plane

    barrier = pltpu.get_barrier_semaphore()
    for dy, dx in OTHERS:
        pl.semaphore_signal(barrier, inc=1, device_id=(lax.rem(py + dy, 2), lax.rem(px + dx, 4)),
                            device_id_type=MESH)
    pl.semaphore_wait(barrier, len(OTHERS))

    def to_x(step):
        return (py, px + step)

    to_y = (1 - py, px)

    def remote(src, dst, ssem, rsem, dev):
        return pltpu.make_async_remote_copy(src_ref=src, dst_ref=dst, send_sem=ssem, recv_sem=rsem,
                                            device_id=dev, device_id_type=MESH)

    def init_up(t):
        cols = pl.ds(LANES * t, LANES)
        return (remote(kx_h.at[pl.ds(BODY - NZ, NZ), cols], KX.at[t, pl.ds(0, NZ), :], is_s.at[t], is_r.at[t], to_x(1)),
                remote(x0_h.at[pl.ds(BODY - NZ, NZ), cols], X0.at[t, pl.ds(0, NZ), :], is_s.at[2 + t], is_r.at[2 + t], to_x(1)))

    def init_down(t):
        cols = pl.ds(LANES * t, LANES)
        return (remote(x0_h.at[pl.ds(0, NZ), cols], X0.at[t, pl.ds(HI, NZ), :], is_s.at[4 + t], is_r.at[4 + t], to_x(-1)),)

    @pl.when(has_hi)
    def _():
        for t in TILES:
            for cp in init_up(t):
                cp.start()

    @pl.when(has_lo)
    def _():
        for t in TILES:
            for cp in init_down(t):
                cp.start()

    tb = 1 - py
    edge = LAST * (1 - py)
    inner = 126 + py * (1 - 126)

    def pack_one(items, bl):
        rel = lax.rem(lane - bl + LANES, LANES)
        s = 1
        while len(items) > NQ:
            keep = rel < s
            items = [jnp.where(keep, items[n], turn(items[n + 1], s)) for n in range(0, len(items), 2)]
            s *= 2
        out = jnp.where(rel < s, items[0],
                        jnp.where(rel < 2 * s, turn(items[1], s), turn(items[2], 2 * s)))
        return out

    def pack(ref, base, bl, dst):
        start = NQ - bl + LANES
        for h in TILES:
            accs = [jnp.zeros(VREG, jnp.float32)] * NQ
            for a in range(NQ * HALF):
                v = ref[tb, pl.ds(base + HALF * NZ * h + SUB * a, SUB), :]
                moved = turn(v, lax.rem(start + a, LANES))
                accs[a % NQ] = jnp.where(lane == a + NQ, moved, accs[a % NQ])
            dst[h] = accs[0] + accs[1] + accs[2]

    from_lo, from_hi = (lane >= NQ) & (lane < 6), (lane >= NQ * HALF) & (lane < NQ * HALF + NQ)
    low_ghost = lane < NQ
    high_ghost = (lane >= 99) & (lane < 102)

    def with_ghosts(n0, n1, lo, hi):
        lo = turn(pack_one([lo[SUB * q:SUB * q + SUB] for q in range(NQ)], edge), lax.rem(LANES - edge, LANES))
        hi = turn(pack_one([hi[SUB * q:SUB * q + SUB] for q in range(NQ)], edge), lax.rem(99 - edge + LANES, LANES))
        return (jnp.where(low_ghost, lo, jnp.where(high_ghost, turn(n1, 96), n0)),
                jnp.where(low_ghost, turn(n0, 32), jnp.where(high_ghost, hi, n1)))

    def z_up(v):
        return jnp.where(row == TOP, lift(turn(v, LAST), TOP), lift(v, TOP))

    def z_down(v):
        return jnp.where(row == 0, lift(turn(v, 1), 1), lift(v, 1))

    def unpack(tile, j):
        parts = [turn(tile, 124 + py - (NQ * j + q)) for q in range(NQ)]
        return jnp.concatenate(parts, axis=0)

    def rowsof(i):
        return pl.multiple_of(NZ * i, 8)

    for cp in loads[:4]:
        cp.wait()
    for cp in loads[4:]:
        cp.start()
    pack(KY, 0, edge, KYP)
    ky_copy = remote(KYP, KYH, is_s.at[6], is_r.at[6], to_y)

    @pl.when(py == 0)
    def _():
        ky_copy.start()

    pack(X0, NZ, edge, PKS.at[0])
    x0_copy = remote(PKS.at[0], H.at[0], is_s.at[TOP], is_r.at[TOP], to_y)
    x0_copy.start()

    pack(X0, NZ, inner, UI)
    pack(KY, 0, inner, CB.at[C_IN])
    for cp in loads[4:6]:
        cp.wait()
    pack(KX, NZ, edge, CB.at[C_UP])
    for cp in loads[6:8]:
        cp.wait()
    pack(D, 0, edge, CB.at[C_D])
    for cp in loads[8:10]:
        cp.wait()
    pack(Z.at[0], NZ, edge, PRE)
    for cp in loads[10:]:
        cp.wait()

    keep_x = jnp.where(has_hi, 1.0, NIL)
    for t in TILES:
        KX[t, pl.ds(BODY, NZ), :] = KX[t, pl.ds(BODY, NZ), :] * keep_x
    dead_y = last & (py == 1)
    dead_z = row24 == NZ - 1

    def mask_step(i, acc):
        s1, s2, kx1, ky1, kz1, k2 = acc
        r = rowsof(i)
        for t in TILES:
            s = D[t, pl.ds(r, NZ), :]
            kx = KX[t, pl.ds(r + NZ, NZ), :]
            ky = KY[t, pl.ds(r, NZ), :]
            kz = jnp.where(dead_z, NIL, KZ[t, pl.ds(r + SUB, NZ), :])
            if t == 1:
                ky = jnp.where(dead_y, NIL, ky)
                KY[t, pl.ds(r, NZ), :] = ky
            KZ[t, pl.ds(r + SUB, NZ), :] = kz
            s1, s2 = s1 + s, s2 + s * s
            kx1, ky1, kz1 = kx1 + kx, ky1 + ky, kz1 + kz
            k2 = k2 + (kx * kx + ky * ky + kz * kz)
        return s1, s2, kx1, ky1, kz1, k2

    sums = lax.fori_loop(0, NX, mask_step, (zero_plane,) * 6, unroll=4)
    stats = jnp.zeros(VREG, jnp.float32)
    for n, v in enumerate(sums):
        stats = jnp.where((row == 2) & (lane == n), full_sum(v), stats)

    def sum_copies(e):
        return [remote(RS.at[e], RR.at[e, me], rs.at[e, n], rr.at[e],
                       (lax.rem(py + dy, 2), lax.rem(px + dx, 4))) for n, (dy, dx) in enumerate(OTHERS)]

    def sum_send(e, tile):
        RS[e] = tile
        RR[e, me] = tile
        for cp in sum_copies(e):
            cp.start()

    def sum_wait(e):
        pltpu.make_async_copy(RR.at[e, pl.ds(0, TOP)], RR.at[e, pl.ds(0, TOP)], rr.at[e]).wait()

    def sum_total(e):
        total = RR[e, 0]
        for n in range(1, 8):
            total = total + RR[e, n]
        return total

    def sum_take(e):
        sum_wait(e)
        return sum_total(e)

    sum_send(0, stats)
    for h in TILES:
        last_x = (lane >= NQ * HALF) & (lane < NQ * HALF + NQ)
        if h == 1:
            CB[C_UP, h] = jnp.where(last_x, CB[C_UP, h] * keep_x, CB[C_UP, h])
        CB[C_OUT, h] = KYP[h]
    pack(KZ, 8, edge, CB.at[C_ZUP])
    for h in TILES:
        CB[C_ZDN, h] = z_down(CB[C_ZUP, h])

    def up_copy(k):
        return remote(Z.at[k, :, pl.ds(BODY, NZ), :], Z.at[k, :, pl.ds(0, NZ), :], hs.at[k, 0], hr.at[k, 0], to_x(1))

    def down_copy(k):
        return remote(Z.at[k, :, pl.ds(NZ, NZ), :], Z.at[k, :, pl.ds(HI, NZ), :], hs.at[k, 1], hr.at[k, 1], to_x(-1))

    def y_copy(k):
        return remote(PKS.at[k + 1], H.at[k + 1], hs.at[k, 2], hr.at[k, 2], to_y)

    def edge_up(k):
        return remote(XS.at[k + 1, 0], XG.at[k + 1, 0], hs.at[k, NQ], hr.at[k, NQ], to_x(1))

    def edge_down(k):
        return remote(XS.at[k + 1, 1], XG.at[k + 1, 1], hs.at[k, 4], hr.at[k, 4], to_x(-1))

    def send_column(k):
        y_copy(k).start()
        XS[k + 1, 0] = jnp.where(from_lo, turn(PKS[k + 1, 1], 35), NIL)
        XS[k + 1, 1] = jnp.where(from_hi, turn(PKS[k + 1, 0], 93), NIL)

        @pl.when(has_hi)
        def _():
            edge_up(k).start()

        @pl.when(has_lo)
        def _():
            edge_down(k).start()

    def take_column(k):
        @pl.when(has_lo)
        def _():
            edge_up(k).wait_recv()

        @pl.when(has_hi)
        def _():
            edge_down(k).wait_recv()

        y_copy(k).wait_recv()

    def send_x(k):
        @pl.when(has_hi)
        def _():
            up_copy(k).start()

        @pl.when(has_lo)
        def _():
            down_copy(k).start()

    def take_halo(k):
        @pl.when(has_lo)
        def _():
            up_copy(k).wait_recv()

        @pl.when(has_hi)
        def _():
            down_copy(k).wait_recv()


    def first_state(vec, i):
        r = rowsof(i)
        return ([vec(t, r) for t in TILES], [vec(t, r + NZ) for t in TILES],
                [KX[t, pl.ds(r, NZ), :] for t in TILES])

    def neighbours(vec, i, j, tile_raw, tile_k, state):
        r = rowsof(i)
        x_down, u, kx_down = state
        x_up = [vec(t, r + 2 * NZ) for t in TILES]
        kx = [KX[t, pl.ds(r + NZ, NZ), :] for t in TILES]
        ky = [KY[t, pl.ds(r, NZ), :] for t in TILES]
        up = [turn(u[t], LAST) for t in TILES]
        down = [turn(ky[t] * u[t], 1) for t in TILES]
        y_up = [jnp.where(last, up[1], up[0]), jnp.where(last, unpack(tile_raw, j), up[1])]
        y_down = [jnp.where(first, unpack(tile_k, j), down[0]), jnp.where(first, down[0], down[1])]
        out = []
        for t in TILES:
            part = ky[t] * y_up[t] + y_down[t]
            part = part + kx[t] * x_up[t]
            part = part + kx_down[t] * x_down[t]
            part = part + KZ[t, pl.ds(r + SUB, NZ), :] * vec(t, r + NZ + 1)
            part = part + KZ[t, pl.ds(r + TOP, NZ), :] * vec(t, r + NZ - 1)
            out.append(part)
        return u, out, ky, kx, (u, x_up, kx)

    @pl.when(has_lo)
    def _():
        for t in TILES:
            for cp in init_up(t):
                cp.wait_recv()

    @pl.when(has_hi)
    def _():
        for t in TILES:
            for cp in init_down(t):
                cp.wait_recv()

    @pl.when(py == 1)
    def _():
        ky_copy.wait_recv()

    x0_copy.wait_recv()
    for h in TILES:
        HK[h] = H[0, h] * KYH[h]

    def own_faces(cols):
        n0, n1 = cols
        down = (jnp.where(from_lo, NIL, turn(n0, NQ)), jnp.where(from_lo, turn(n0, 35), turn(n1, NQ)))
        up = (jnp.where(from_hi, turn(n1, 93), turn(n0, 125)), jnp.where(from_hi, NIL, turn(n1, 125)))
        return [CB[C_IN, h] * UI[h] + CB[C_UP, h] * up[h] + CB[C_DOWN, h] * down[h]
                + CB[C_ZUP, h] * z_up(u) + CB[C_ZDN, h] * z_down(u) for h, u in enumerate(cols)]

    def outer_faces(lo, hi, beyond):
        ghost = [jnp.zeros(VREG, jnp.float32)] * 2
        for q in range(NQ):
            for h, (v, at) in enumerate(((lo, NQ), (hi, NQ * HALF))):
                at = at + q
                moved = turn(v[SUB * q:SUB * q + SUB], lax.rem(at - edge + LANES, LANES))
                ghost[h] = jnp.where(lane == at, moved, ghost[h])
        return [CB[C_OUT, h] * beyond[h] + CB[C_DOWN - h, h] * ghost[h] for h in TILES]

    x0_vec = lambda t, q: X0[t, pl.ds(q, NZ), :]

    def start_plane(i, rho, state):
        h = i // 32
        j = lax.rem(i, 32)
        r = rowsof(i)
        kx_down = state[2]
        u, nb, ky, kx, state = neighbours(x0_vec, i, j, H[0, h], HK[h], state)
        down = [turn(ky[t], 1) for t in TILES]
        ky_lo = [jnp.where(first, unpack(KYH[h], j), down[0]), jnp.where(first, down[0], down[1])]
        for t in TILES:
            diag = D[t, pl.ds(r, NZ), :] + ky[t] + ky_lo[t] + kx[t] + kx_down[t]
            diag = diag + KZ[t, pl.ds(r + SUB, NZ), :] + KZ[t, pl.ds(r + TOP, NZ), :]
            D[t, pl.ds(r, NZ), :] = diag
            res = Z[0, t, pl.ds(r + NZ, NZ), :] - (diag * u[t] - nb[t])
            Z[0, t, pl.ds(r + NZ, NZ), :] = res
            rho = rho + res * res
        return rho, state

    UNROLL = 31

    def sweep(vec, plane, k, sums1, more):
        def run(i, n, c):
            state = first_state(vec, i)
            for m in range(n):
                c, state = plane(i + m, c, state)
            return c

        sums1 = run(NX - 1, 1, run(0, 1, sums1))

        @pl.when(more)
        def _():
            send_x(k)

        return lax.fori_loop(0, (NX - 2) // UNROLL, lambda m, c: run(1 + UNROLL * m, UNROLL, c), sums1)

    zero24 = zero_plane
    zero_tile = zero_plane
    kx_cols = with_ghosts(CB[C_UP, 0], CB[C_UP, 1], KX[tb, pl.ds(0, NZ), :], zero_tile)
    for h in TILES:
        CB[C_DOWN, h] = turn(kx_cols[h], NQ)
        ky_edge, ky_in = CB[C_OUT, h], CB[C_IN, h]
        CB[C_OUT, h] = jnp.where(py == 0, ky_edge, KYH[h])
        CB[C_IN, h] = jnp.where(py == 0, ky_in, ky_edge)
    far = outer_faces(X0[tb, pl.ds(0, NZ), :], X0[tb, pl.ds(HI, NZ), :], (H[0, 0], H[0, 1]))
    own = own_faces((PKS[0, 0], PKS[0, 1]))
    for h in TILES:
        diag = CB[C_D, h] + CB[C_UP, h] + CB[C_DOWN, h] + CB[C_OUT, h] + CB[C_IN, h] + CB[C_ZUP, h] + CB[C_ZDN, h]
        CB[C_D, h] = diag
        PKS[1, h] = PRE[h] - (diag * PKS[0, h] - far[h] - own[h])
    send_column(0)
    rho0 = sweep(x0_vec, start_plane, 0, zero24, px >= 0)
    pack(Z.at[0], NZ, inner, UI)
    PT[...] = jnp.where((row == 0) & (lane == 0), full_sum(rho0), NIL)

    for n in range(20):
        ST[n] = jnp.zeros(VREG, jnp.float32)
    totals = sum_take(0)
    cells = CELLS
    mean = [full_sum(jnp.where((row == 2) & (lane == n), totals, NIL)) * (1.0 / cells) for n in range(6)]
    var_s = jnp.maximum(mean[1] - mean[0] * mean[0], NIL)
    var_k = jnp.maximum(mean[5] - mean[2] * mean[2] - mean[NQ] * mean[NQ] - mean[4] * mean[4], NIL)
    b_first = jnp.sqrt(3.0 * mean[5] + var_s + 2.0 * var_k)
    a_first = jnp.maximum(mean[0] - 0.5 * jnp.sqrt(var_s), 0.3) + 2.0 * b_first

    def set_coefs(k0, a_new, b_new):
        old_b = ST[S_B]
        b_arr = jnp.where(lane >= k0, b_new, old_b)
        ST[S_A] = jnp.where(lane >= k0, a_new, ST[S_A])
        ST[S_B] = b_arr
        ST[S_C] = jnp.where(lane == 0, NIL, turn(b_arr, 1))
        inv = 1.0 / b_new
        for k in range(k0, ITERS):
            CO[k, K_A] = a_new
            if k > k0:
                CO[k, K_C] = b_new
            elif k == 0:
                CO[k, K_C] = jnp.zeros(VREG, jnp.float32)
            else:
                CO[k, K_C] = CO[k - 1, K_B]
            CO[k, K_INV] = inv
            CO[k, K_B] = b_new

    set_coefs(0, a_first, b_first)

    def gram_start(total):
        rho = full_sum(jnp.where((row == 0) & (lane == 0), total, NIL))
        one = jnp.where(lane == 0, 1.0, NIL)
        for n in (S_GP, S_Y, S_BA, S_LA, S_LB, S_LA2, S_LB2, S_ERR):
            ST[n] = jnp.zeros(VREG, jnp.float32)
        ST[S_G] = one * rho
        ST[S_CL] = one
        ST[S_DL] = one
        ST[S_LEAD] = jnp.ones(VREG, jnp.float32)
        ST[S_RHO] = rho
        ST[S_RHO0] = rho
        ST[S_HIST] = one * rho

    def gram_step(k, total):
        a, b, c = ST[S_A], ST[S_B], ST[S_C]
        g, gp, cl, dl = ST[S_G], ST[S_GP], ST[S_CL], ST[S_DL]
        d_row, e_row = jnp.broadcast_to(total[0:1], VREG), jnp.broadcast_to(total[1:2], VREG)
        rho, lead = ST[S_RHO], ST[S_LEAD]
        b_k, c_k, a_k = CO[k, K_B], CO[k, K_C], CO[k, K_A]
        at_k, at_k1 = lane == k, lane == k + 1
        rec = ((a - a_k) * g + b * turn(g, LAST)
               + c * turn(g, 1) - c_k * gp) * CO[k, K_INV]
        g_new = jnp.where(lane < k, rec, jnp.where(at_k, e_row, jnp.where(at_k1, d_row, NIL)))
        g_full = jnp.where(at_k1, turn(e_row, 1), g)
        image = a * dl + turn(b * dl, 1) + turn(c * dl, LAST)
        delta = lead * lane_sum(image * g_full)
        alpha = rho / delta
        ST[S_AL] = alpha
        y = ST[S_Y] + alpha * dl
        cl = cl - alpha * image
        lead = -alpha * b_k * lead
        prod = cl * g_new
        rho_new = lead * lane_sum(prod)
        size = lane_sum(jnp.abs(cl) * jnp.where(lane < k + 2, jnp.sqrt(jnp.maximum(d_row, NIL)), NIL))
        beta = rho_new / rho
        dl = cl + beta * dl
        ST[S_G], ST[S_GP], ST[S_CL], ST[S_DL] = g_new, g, cl, dl
        ST[S_Y], ST[S_RHO], ST[S_LEAD] = y, rho_new, lead
        ST[S_HIST] = jnp.where(at_k1, rho_new, ST[S_HIST])
        inv_alpha = 1.0 / alpha
        ST[S_LA2], ST[S_LB2] = ST[S_LA], ST[S_LB]
        ST[S_LA] = inv_alpha + ST[S_BA]
        ST[S_LB] = jnp.sqrt(jnp.abs(beta)) * inv_alpha
        ST[S_BA] = beta * inv_alpha
        err = size * size / jnp.sqrt(jnp.abs(rho_new) * ST[S_RHO0])
        err = jnp.where(rho_new > NIL, err, 1e30)
        ST[S_ERR] = jnp.maximum(ST[S_ERR], jnp.where(err < 1e30, err, 1e30))

    def renew(k0):
        a_new = 0.5 * (ST[S_LA] + ST[S_LA2])
        b_new = 0.5 * (ST[S_LB] + ST[S_LB2])
        a_ok = (a_new > 0.3) & (a_new < 26.8)
        a_new = jnp.where(a_ok, a_new, a_first)
        b_new = jnp.where(a_ok & (b_new > 0.25 * b_first) & (b_new < 2.0 * b_first), b_new, b_first)
        set_coefs(k0, a_new, b_new)

    def prepare(k):
        before = jnp.maximum(k - 1, 0)
        cols = (PKS[k + 1, 0], PKS[k + 1, 1])
        own = own_faces(cols)
        for h, u in enumerate(cols):
            PRE[h] = (CB[C_D, h] - CO[k, K_A]) * u - own[h] - CO[k, K_C] * PKS[before + 1, h]

    def apply_step(k):
        take_column(k)
        before = jnp.maximum(k - 1, 0)
        for h in TILES:
            far = CB[C_OUT, h] * H[k + 1, h] + CB[C_DOWN - h, h] * XG[k + 1, h]
            PKS[k + 2, h] = (PRE[h] - far) * CO[k, K_INV]

        @pl.when(k < ITERS - 1)
        def _():
            send_column(k + 1)

        for h in TILES:
            HK[h] = H[k + 1, h] * KYH[h]
        take_halo(k)
        a_k, c_k, i_k = three(CO[k, K_A]), three(CO[k, K_C]), three(CO[k, K_INV])

        def plane(i, carry, state):
            dots, cross = carry
            h = i // 32
            j = lax.rem(i, 32)
            r = rowsof(i)
            u, nb, ky, kx, state = neighbours(vec, i, j, H[k + 1, h], HK[h], state)
            for t in TILES:
                val = (D[t, pl.ds(r, NZ), :] - a_k) * u[t] - nb[t] - c_k * Z[before, t, pl.ds(r + NZ, NZ), :]
                val = val * i_k
                Z[k + 1, t, pl.ds(r + NZ, NZ), :] = val
                dots = dots + val * val
                cross = cross + val * u[t]
            return (dots, cross), state

        vec = lambda t, q: Z[k, t, pl.ds(q, NZ), :]
        dots, cross = sweep(vec, plane, k + 1, (zero24, zero24), k < ITERS - 1)

        step = k - 2

        @pl.when(step > 0)
        def _():
            sum_wait(step + 1)

        total = sum_total(jnp.maximum(step + 1, 0))
        pack(Z.at[k + 1], NZ, inner, UI)
        tile = jnp.where((row == 0) & (lane == k + 1), full_sum(dots), PT[...])
        tile = jnp.where((row == 1) & (lane == k), full_sum(cross), tile)
        PT[...] = tile
        gram_step(jnp.maximum(step, 0), total)
        prepare(jnp.minimum(k + 1, ITERS - 1))
        sum_send(k + 1, tile)

        @pl.when(k == 1)
        def _():
            gram_start(sum_take(1))

        for at in RENEW_AT:
            @pl.when(k == at)
            def _():
                renew(at + 2)

    prepare(0)

    @pl.loop(0, ITERS)
    def _(k):
        apply_step(k)

    gram_step(ITERS - 2, sum_take(ITERS - 1))

    y, d = ST[S_Y], ST[S_DL]
    for k in range(ITERS):
        YB[k] = lane_sum(jnp.where(lane == k, y, NIL))
        YB[ITERS + k] = lane_sum(jnp.where(lane == k, d, NIL))

    AHEAD = 32

    def combine(i, c):
        r = rowsof(i + 1)
        acc = [X0[t, pl.ds(r, NZ), :] for t in TILES]
        way = [zero_plane, zero_plane]
        for k in range(ITERS):
            w, v = three(YB[k]), three(YB[ITERS + k])
            for t in TILES:
                z = Z[k, t, pl.ds(r, NZ), :]
                way[t] = way[t] + v * z
                if k < ITERS - 1:
                    acc[t] = acc[t] + w * z
        for t in TILES:
            X0[t, pl.ds(r, NZ), :] = acc[t]
            Z[ITERS, t, pl.ds(r, NZ), :] = way[t]
        return c

    lax.fori_loop(0, AHEAD, combine, 0, unroll=2)
    gram_step(ITERS - 1, sum_take(ITERS))
    y = ST[S_Y]
    for k in range(ITERS):
        YB[k] = lane_sum(jnp.where(lane == k, y, NIL))
    hist = jnp.sqrt(ST[S_HIST] * (1.0 / cells))
    hist_ref[...] = jnp.where(row == 0, hist, ST[S_ERR])
    alpha = three(ST[S_AL])

    def last_step(i, c):
        r = rowsof(i + 1)
        for t in TILES:
            out_ref[pl.ds(rowsof(i), NZ), LANES * t:LANES * t + LANES] = X0[t, pl.ds(r, NZ), :] + alpha * Z[ITERS, t, pl.ds(r, NZ), :]
        return c

    def whole_step(i, c):
        r = rowsof(i + 1)
        acc = [X0[t, pl.ds(r, NZ), :] for t in TILES]
        for k in range(ITERS):
            w = three(YB[k])
            for t in TILES:
                acc[t] = acc[t] + w * Z[k, t, pl.ds(r, NZ), :]
        for t in TILES:
            out_ref[pl.ds(rowsof(i), NZ), LANES * t:LANES * t + LANES] = acc[t]
        return c

    lax.fori_loop(0, AHEAD, last_step, 0, unroll=4)
    lax.fori_loop(AHEAD, NX, whole_step, 0, unroll=2)

    @pl.when(has_hi)
    def _():
        for t in TILES:
            for cp in init_up(t):
                cp.wait_send()

    @pl.when(has_lo)
    def _():
        for t in TILES:
            for cp in init_down(t):
                cp.wait_send()

    @pl.when(py == 0)
    def _():
        ky_copy.wait_send()

    x0_copy.wait_send()

    @pl.loop(0, ITERS)
    def _(k):
        @pl.when(has_hi)
        def _():
            up_copy(k).wait_send()
            edge_up(k).wait_send()

        @pl.when(has_lo)
        def _():
            down_copy(k).wait_send()
            edge_down(k).wait_send()

        y_copy(k).wait_send()

    @pl.loop(0, ITERS + 1)
    def _(e):
        for cp in sum_copies(e):
            cp.wait_send()


def hand_over(src, dst, sem):
    cp = pltpu.make_async_copy(src, dst, sem.at[0])
    cp.start()
    cp.wait()


def publish(x_rows):
    rows = pl.pallas_call(
        hand_over, out_shape=jax.ShapeDtypeStruct(x_rows.shape, jnp.float32),
        in_specs=[pl.BlockSpec(memory_space=pltpu.VMEM)], out_specs=pl.BlockSpec(memory_space=pl.ANY),
        scratch_shapes=[pltpu.SemaphoreType.DMA((1,))])(x_rows)
    return jnp.transpose(rows.reshape(NX, NZ, ROW), (0, 2, 1))


def fused_solve(shift, rhs_field, x_init, cond_x, cond_y, cond_z):
    def flat(v):
        return jnp.transpose(v, (0, 2, 1)).reshape(BODY, 256)

    f32 = jnp.float32
    any_spec = pl.BlockSpec(memory_space=pl.ANY)
    x_rows, small = pl.pallas_call(
        kernel,
        out_shape=(pltpu.VMEM((BODY, 256), f32), jax.ShapeDtypeStruct(VREG, f32)),
        in_specs=[any_spec] * 6,
        out_specs=(pl.BlockSpec(memory_space=pltpu.VMEM), pl.BlockSpec(memory_space=pltpu.VMEM)),
        scratch_shapes=[
            pltpu.VMEM((ITERS + 1, 2, FULL, LANES), f32),
            pltpu.VMEM((2, FULL, LANES), f32),
            pltpu.VMEM((2, BODY, LANES), f32),
            pltpu.VMEM((2, BODY + 32, LANES), f32),
            pltpu.VMEM((2, BODY, LANES), f32),
            pltpu.VMEM((2, BODY + 16, LANES), f32),
            pltpu.VMEM((ITERS + 2, 2, *VREG), f32),
            pltpu.VMEM((ITERS + 2, 2, *VREG), f32),
            pltpu.VMEM((2, *VREG), f32),
            pltpu.VMEM((2, *VREG), f32),
            pltpu.VMEM((2, *VREG), f32),
            pltpu.VMEM((2, *VREG), f32),
            pltpu.VMEM((TOP, 2, *VREG), f32),
            pltpu.VMEM((2, *VREG), f32),
            pltpu.VMEM((ITERS + 2, 2, *VREG), f32),
            pltpu.VMEM((ITERS + 2, 2, *VREG), f32),
            pltpu.VMEM((ITERS + 1, *VREG), f32),
            pltpu.VMEM((ITERS + 1, 8, *VREG), f32),
            pltpu.VMEM(VREG, f32),
            pltpu.VMEM((20, *VREG), f32),
            pltpu.VMEM((ITERS, 4, *VREG), f32),
            pltpu.VMEM((2 * ITERS, *VREG), f32),
            pltpu.SemaphoreType.DMA((12,)),
            pltpu.SemaphoreType.DMA((8,)),
            pltpu.SemaphoreType.DMA((8,)),
            pltpu.SemaphoreType.DMA((ITERS, 5)),
            pltpu.SemaphoreType.DMA((ITERS, 5)),
            pltpu.SemaphoreType.DMA((ITERS + 1, TOP)),
            pltpu.SemaphoreType.DMA((ITERS + 1,)),
        ],
        compiler_params=pltpu.CompilerParams(collective_id=0, has_side_effects=True,
                                             vmem_limit_bytes=65011712),
    )(*(flat(v) for v in (shift, rhs_field, x_init, cond_x, cond_y, cond_z)))
    return x_rows, small[0, :ITERS + 1], small[1, 0]


def classic_solve(shift, rhs_field, x_init, cond_x, cond_y, cond_z):
    count_x, count_y = 4, 2
    fwd_x = [(src, src + 1) for src in range(count_x - 1)]
    back_x = [(src + 1, src) for src in range(count_x - 1)]
    pos_x, pos_y = lax.axis_index("px"), lax.axis_index("py")
    plane_x = lax.broadcasted_iota(jnp.int32, (NX, 1, 1), 0)
    plane_y = lax.broadcasted_iota(jnp.int32, (1, ROW, 1), 1)
    plane_z = lax.broadcasted_iota(jnp.int32, (1, 1, NZ), 2)
    plus_x = jnp.where((pos_x == count_x - 1) & (plane_x == NX - 1), NIL, cond_x)
    plus_y = jnp.where((pos_y == count_y - 1) & (plane_y == ROW - 1), NIL, cond_y)
    plus_z = jnp.where(plane_z == NZ - 1, NIL, cond_z)

    def shifted(vec, axis, ahead, halo):
        size = vec.shape[axis]
        if ahead:
            return jnp.concatenate([lax.slice_in_dim(vec, 1, size, axis=axis), halo], axis=axis)
        return jnp.concatenate([halo, lax.slice_in_dim(vec, 0, size - 1, axis=axis)], axis=axis)

    def below(vec):
        low_x = lax.ppermute(vec[-1:], "px", fwd_x)
        low_y = lax.ppermute(vec[:, -1:], "py", [(0, 1)])
        return (shifted(vec, 0, False, low_x), shifted(vec, 1, False, low_y),
                shifted(vec, 2, False, jnp.zeros_like(vec[:, :, :1])))

    def above(vec):
        high_x = lax.ppermute(vec[:1], "px", back_x)
        high_y = lax.ppermute(vec[:, :1], "py", [(1, 0)])
        return (shifted(vec, 0, True, high_x), shifted(vec, 1, True, high_y),
                shifted(vec, 2, True, jnp.zeros_like(vec[:, :, :1])))

    minus_x, minus_y, minus_z = below(plus_x)[0], below(plus_y)[1], below(plus_z)[2]
    diag = shift + plus_x + minus_x + plus_y + minus_y + plus_z + minus_z

    def apply_op(vec):
        up_x, up_y, up_z = above(vec)
        down_x, down_y, down_z = below(vec)
        return (diag * vec - plus_x * up_x - minus_x * down_x
                - plus_y * up_y - minus_y * down_y - plus_z * up_z - minus_z * down_z)

    def global_dot(left, right):
        return lax.psum(jnp.sum(left * right), SUM_AXES)

    res = rhs_field - apply_op(x_init)
    rho = global_dot(res, res)
    history = jnp.where(jnp.arange(ITERS + 1) == 0, rho, NIL)

    def step(k, state):
        x, res, p, rho, history = state
        q = apply_op(p)
        alpha = rho / global_dot(p, q)
        x = x + alpha * p
        res = res - alpha * q
        rho_new = global_dot(res, res)
        p = res + (rho_new / rho) * p
        return x, res, p, rho_new, jnp.where(jnp.arange(ITERS + 1) == k + 1, rho_new, history)

    x, _, _, _, history = lax.fori_loop(0, ITERS, step, (jnp.zeros_like(res), res, res, rho, history))
    return x_init + x, jnp.sqrt(history / CELLS)


def solution(mesh):
    field_spec = P("px", "py", None)

    def local_solve(*fields):
        x_rows, history, err = fused_solve(*fields)
        return lax.cond(err < ERR_LIMIT, lambda: (publish(x_rows), history), lambda: classic_solve(*fields))

    return jax.shard_map(local_solve, mesh=mesh, in_specs=(field_spec,) * 6,
                         out_specs=(field_spec, P()), check_vma=False)
```

```python
import functools

import jax
import jax.numpy as jnp
from jax import lax
from jax.experimental import pallas as pl
from jax.experimental.pallas import tpu as pltpu
from jax.sharding import PartitionSpec as P

ITERS = 20
SUM_AXES = ("px", "py")
MESH = pl.DeviceIdType.MESH
NX, NZ = 64, 24
ROW = 256
ERR_LIMIT = 1000.0
HALF = NX // 2
CELLS = float(NX * 256 * NZ * 8)
BODY = NX * NZ
FULL = BODY + 2 * NZ
HI = BODY + NZ
OTHERS = tuple((dy, dx) for dy in range(2) for dx in range(4) if (dy, dx) != (0, 0))
RENEW_AT = (7, 12)
VREG = (8, 128)
SUB, LANES = VREG
TILES = range(2)


C_D, C_UP, C_DOWN, C_OUT, C_IN, C_ZUP, C_ZDN = range(7)
K_A, K_C, K_INV, K_B = range(4)
NQ = 3
LAST, TOP, NIL = 127, 7, 0.0


def turn(v, by):
    return pltpu.roll(v, by, 1)


def lift(v, by):
    return pltpu.roll(v, by, 0)


S_A, S_B, S_C, S_GP, S_G, S_CL, S_DL, S_Y, S_RHO, S_LEAD, S_HIST, S_BA, S_LA, S_LB, S_LA2, S_LB2, S_ERR, S_D, S_AL, S_RHO0 = range(20)


def lanes():
    return lax.broadcasted_iota(jnp.int32, VREG, 1)


def rows8():
    return lax.broadcasted_iota(jnp.int32, VREG, 0)


def lane_sum(v):
    return jnp.broadcast_to(jnp.sum(v, axis=1, keepdims=True), VREG)


def full_sum(v):
    return jnp.broadcast_to(jnp.sum(jnp.sum(v, axis=0, keepdims=True), axis=1, keepdims=True), VREG)


def three(v):
    return jnp.concatenate([v, v, v], axis=0)


def kernel(s_h, b_h, x0_h, kx_h, ky_h, kz_h, out_ref, hist_ref,
           Z, X0, D, KX, KY, KZ, PKS, H, KYP, KYH, HK, UI, CB, PRE, XS, XG, RS, RR, PT, ST, CO, YB,
           lsem, is_s, is_r, hs, hr, rs, rr):
    px, py = lax.axis_index("px"), lax.axis_index("py")
    me = py * 4 + px
    lane, row = lanes(), rows8()
    lane24 = lax.broadcasted_iota(jnp.int32, (NZ, LANES), 1)
    row24 = lax.broadcasted_iota(jnp.int32, (NZ, LANES), 0)
    first, last = lane24 == 0, lane24 == LAST
    has_lo, has_hi = px > 0, px < NQ

    loads = []
    for n, (src, dst, base) in enumerate((
            (ky_h, KY, 0), (x0_h, X0, NZ), (kx_h, KX, NZ), (s_h, D, 0), (b_h, None, NZ), (kz_h, KZ, 8))):
        for t in TILES:
            to = Z.at[0, t, pl.ds(base, BODY), :] if dst is None else dst.at[t, pl.ds(base, BODY), :]
            cp = pltpu.make_async_copy(src.at[:, pl.ds(LANES * t, LANES)], to, lsem.at[2 * n + t])
            loads.append(cp)
    for cp in loads:
        cp.start()

    zero_plane = jnp.zeros((NZ, LANES), jnp.float32)
    for t in TILES:
        KX[t, pl.ds(0, NZ), :] = zero_plane
        X0[t, pl.ds(0, NZ), :] = zero_plane
        X0[t, pl.ds(HI, NZ), :] = zero_plane
        KZ[t, pl.ds(0, 8), :] = jnp.zeros(VREG, jnp.float32)
    KYH[...] = jnp.zeros((2, *VREG), jnp.float32)
    for t in TILES:
        for k in range(ITERS + 2):
            XG[k, t] = jnp.zeros(VREG, jnp.float32)

    @pl.loop(0, ITERS + 1)
    def _(k):
        for t in TILES:
            Z[k, t, pl.ds(0, NZ), :] = zero_plane
            Z[k, t, pl.ds(HI, NZ), :] = zero_plane

    barrier = pltpu.get_barrier_semaphore()
    for dy, dx in OTHERS:
        pl.semaphore_signal(barrier, inc=1, device_id=(lax.rem(py + dy, 2), lax.rem(px + dx, 4)),
                            device_id_type=MESH)
    pl.semaphore_wait(barrier, len(OTHERS))

    def to_x(step):
        return (py, px + step)

    to_y = (1 - py, px)

    def remote(src, dst, ssem, rsem, dev):
        return pltpu.make_async_remote_copy(src_ref=src, dst_ref=dst, send_sem=ssem, recv_sem=rsem,
                                            device_id=dev, device_id_type=MESH)

    def init_up(t):
        cols = pl.ds(LANES * t, LANES)
        return (remote(kx_h.at[pl.ds(BODY - NZ, NZ), cols], KX.at[t, pl.ds(0, NZ), :], is_s.at[t], is_r.at[t], to_x(1)),
                remote(x0_h.at[pl.ds(BODY - NZ, NZ), cols], X0.at[t, pl.ds(0, NZ), :], is_s.at[2 + t], is_r.at[2 + t], to_x(1)))

    def init_down(t):
        cols = pl.ds(LANES * t, LANES)
        return (remote(x0_h.at[pl.ds(0, NZ), cols], X0.at[t, pl.ds(HI, NZ), :], is_s.at[4 + t], is_r.at[4 + t], to_x(-1)),)

    @pl.when(has_hi)
    def _():
        for t in TILES:
            for cp in init_up(t):
                cp.start()

    @pl.when(has_lo)
    def _():
        for t in TILES:
            for cp in init_down(t):
                cp.start()

    tb = 1 - py
    edge = LAST * (1 - py)
    inner = 126 + py * (1 - 126)

    def pack_one(items, bl):
        rel = lax.rem(lane - bl + LANES, LANES)
        s = 1
        while len(items) > NQ:
            keep = rel < s
            items = [jnp.where(keep, items[n], turn(items[n + 1], s)) for n in range(0, len(items), 2)]
            s *= 2
        out = jnp.where(rel < s, items[0],
                        jnp.where(rel < 2 * s, turn(items[1], s), turn(items[2], 2 * s)))
        return out

    def pack(ref, base, bl, dst):
        start = NQ - bl + LANES
        for h in TILES:
            accs = [jnp.zeros(VREG, jnp.float32)] * NQ
            for a in range(NQ * HALF):
                v = ref[tb, pl.ds(base + HALF * NZ * h + SUB * a, SUB), :]
                moved = turn(v, lax.rem(start + a, LANES))
                accs[a % NQ] = jnp.where(lane == a + NQ, moved, accs[a % NQ])
            dst[h] = accs[0] + accs[1] + accs[2]

    from_lo, from_hi = (lane >= NQ) & (lane < 6), (lane >= NQ * HALF) & (lane < NQ * HALF + NQ)
    low_ghost = lane < NQ
    high_ghost = (lane >= 99) & (lane < 102)

    def with_ghosts(n0, n1, lo, hi):
        lo = turn(pack_one([lo[SUB * q:SUB * q + SUB] for q in range(NQ)], edge), lax.rem(LANES - edge, LANES))
        hi = turn(pack_one([hi[SUB * q:SUB * q + SUB] for q in range(NQ)], edge), lax.rem(99 - edge + LANES, LANES))
        return (jnp.where(low_ghost, lo, jnp.where(high_ghost, turn(n1, 96), n0)),
                jnp.where(low_ghost, turn(n0, 32), jnp.where(high_ghost, hi, n1)))

    def z_up(v):
        return jnp.where(row == TOP, lift(turn(v, LAST), TOP), lift(v, TOP))

    def z_down(v):
        return jnp.where(row == 0, lift(turn(v, 1), 1), lift(v, 1))

    def unpack(tile, j):
        parts = [turn(tile, 124 + py - (NQ * j + q)) for q in range(NQ)]
        return jnp.concatenate(parts, axis=0)

    def rowsof(i):
        return pl.multiple_of(NZ * i, 8)

    for cp in loads[:4]:
        cp.wait()
    pack(KY, 0, edge, KYP)
    ky_copy = remote(KYP, KYH, is_s.at[6], is_r.at[6], to_y)

    @pl.when(py == 0)
    def _():
        ky_copy.start()

    pack(X0, NZ, edge, PKS.at[0])
    x0_copy = remote(PKS.at[0], H.at[0], is_s.at[TOP], is_r.at[TOP], to_y)
    x0_copy.start()

    pack(X0, NZ, inner, UI)
    pack(KY, 0, inner, CB.at[C_IN])
    for cp in loads[4:6]:
        cp.wait()
    pack(KX, NZ, edge, CB.at[C_UP])
    for cp in loads[6:8]:
        cp.wait()
    pack(D, 0, edge, CB.at[C_D])
    for cp in loads[8:10]:
        cp.wait()
    pack(Z.at[0], NZ, edge, PRE)
    for cp in loads[10:]:
        cp.wait()

    keep_x = jnp.where(has_hi, 1.0, NIL)
    for t in TILES:
        KX[t, pl.ds(BODY, NZ), :] = KX[t, pl.ds(BODY, NZ), :] * keep_x
    dead_y = last & (py == 1)
    dead_z = row24 == NZ - 1

    def mask_step(i, acc):
        s1, s2, kx1, ky1, kz1, k2 = acc
        r = rowsof(i)
        for t in TILES:
            s = D[t, pl.ds(r, NZ), :]
            kx = KX[t, pl.ds(r + NZ, NZ), :]
            ky = KY[t, pl.ds(r, NZ), :]
            kz = jnp.where(dead_z, NIL, KZ[t, pl.ds(r + SUB, NZ), :])
            if t == 1:
                ky = jnp.where(dead_y, NIL, ky)
                KY[t, pl.ds(r, NZ), :] = ky
            KZ[t, pl.ds(r + SUB, NZ), :] = kz
            s1, s2 = s1 + s, s2 + s * s
            kx1, ky1, kz1 = kx1 + kx, ky1 + ky, kz1 + kz
            k2 = k2 + (kx * kx + ky * ky + kz * kz)
        return s1, s2, kx1, ky1, kz1, k2

    sums = lax.fori_loop(0, NX, mask_step, (zero_plane,) * 6, unroll=4)
    stats = jnp.zeros(VREG, jnp.float32)
    for n, v in enumerate(sums):
        stats = jnp.where((row == 2) & (lane == n), full_sum(v), stats)

    def sum_copies(e):
        return [remote(RS.at[e], RR.at[e, me], rs.at[e, n], rr.at[e],
                       (lax.rem(py + dy, 2), lax.rem(px + dx, 4))) for n, (dy, dx) in enumerate(OTHERS)]

    def sum_send(e, tile):
        RS[e] = tile
        RR[e, me] = tile
        for cp in sum_copies(e):
            cp.start()

    def sum_wait(e):
        pltpu.make_async_copy(RR.at[e, pl.ds(0, TOP)], RR.at[e, pl.ds(0, TOP)], rr.at[e]).wait()

    def sum_total(e):
        total = RR[e, 0]
        for n in range(1, 8):
            total = total + RR[e, n]
        return total

    def sum_take(e):
        sum_wait(e)
        return sum_total(e)

    sum_send(0, stats)
    for h in TILES:
        last_x = (lane >= NQ * HALF) & (lane < NQ * HALF + NQ)
        if h == 1:
            CB[C_UP, h] = jnp.where(last_x, CB[C_UP, h] * keep_x, CB[C_UP, h])
        CB[C_OUT, h] = KYP[h]
    pack(KZ, 8, edge, CB.at[C_ZUP])
    for h in TILES:
        CB[C_ZDN, h] = z_down(CB[C_ZUP, h])

    def up_copy(k):
        return remote(Z.at[k, :, pl.ds(BODY, NZ), :], Z.at[k, :, pl.ds(0, NZ), :], hs.at[k, 0], hr.at[k, 0], to_x(1))

    def down_copy(k):
        return remote(Z.at[k, :, pl.ds(NZ, NZ), :], Z.at[k, :, pl.ds(HI, NZ), :], hs.at[k, 1], hr.at[k, 1], to_x(-1))

    def y_copy(k):
        return remote(PKS.at[k + 1], H.at[k + 1], hs.at[k, 2], hr.at[k, 2], to_y)

    def edge_up(k):
        return remote(XS.at[k + 1, 0], XG.at[k + 1, 0], hs.at[k, NQ], hr.at[k, NQ], to_x(1))

    def edge_down(k):
        return remote(XS.at[k + 1, 1], XG.at[k + 1, 1], hs.at[k, 4], hr.at[k, 4], to_x(-1))

    def send_column(k):
        y_copy(k).start()
        XS[k + 1, 0] = jnp.where(from_lo, turn(PKS[k + 1, 1], 35), NIL)
        XS[k + 1, 1] = jnp.where(from_hi, turn(PKS[k + 1, 0], 93), NIL)

        @pl.when(has_hi)
        def _():
            edge_up(k).start()

        @pl.when(has_lo)
        def _():
            edge_down(k).start()

    def take_column(k):
        @pl.when(has_lo)
        def _():
            edge_up(k).wait_recv()

        @pl.when(has_hi)
        def _():
            edge_down(k).wait_recv()

        y_copy(k).wait_recv()

    def send_x(k):
        @pl.when(has_hi)
        def _():
            up_copy(k).start()

        @pl.when(has_lo)
        def _():
            down_copy(k).start()

    def take_halo(k):
        @pl.when(has_lo)
        def _():
            up_copy(k).wait_recv()

        @pl.when(has_hi)
        def _():
            down_copy(k).wait_recv()


    def first_state(vec, i):
        r = rowsof(i)
        return ([vec(t, r) for t in TILES], [vec(t, r + NZ) for t in TILES],
                [KX[t, pl.ds(r, NZ), :] for t in TILES])

    def neighbours(vec, i, j, tile_raw, tile_k, state):
        r = rowsof(i)
        x_down, u, kx_down = state
        x_up = [vec(t, r + 2 * NZ) for t in TILES]
        kx = [KX[t, pl.ds(r + NZ, NZ), :] for t in TILES]
        ky = [KY[t, pl.ds(r, NZ), :] for t in TILES]
        up = [turn(u[t], LAST) for t in TILES]
        down = [turn(ky[t] * u[t], 1) for t in TILES]
        y_up = [jnp.where(last, up[1], up[0]), jnp.where(last, unpack(tile_raw, j), up[1])]
        y_down = [jnp.where(first, unpack(tile_k, j), down[0]), jnp.where(first, down[0], down[1])]
        out = []
        for t in TILES:
            part = ky[t] * y_up[t] + y_down[t]
            part = part + kx[t] * x_up[t]
            part = part + kx_down[t] * x_down[t]
            part = part + KZ[t, pl.ds(r + SUB, NZ), :] * vec(t, r + NZ + 1)
            part = part + KZ[t, pl.ds(r + TOP, NZ), :] * vec(t, r + NZ - 1)
            out.append(part)
        return u, out, ky, kx, (u, x_up, kx)

    @pl.when(has_lo)
    def _():
        for t in TILES:
            for cp in init_up(t):
                cp.wait_recv()

    @pl.when(has_hi)
    def _():
        for t in TILES:
            for cp in init_down(t):
                cp.wait_recv()

    @pl.when(py == 1)
    def _():
        ky_copy.wait_recv()

    x0_copy.wait_recv()
    for h in TILES:
        HK[h] = H[0, h] * KYH[h]

    def own_faces(cols):
        n0, n1 = cols
        down = (jnp.where(from_lo, NIL, turn(n0, NQ)), jnp.where(from_lo, turn(n0, 35), turn(n1, NQ)))
        up = (jnp.where(from_hi, turn(n1, 93), turn(n0, 125)), jnp.where(from_hi, NIL, turn(n1, 125)))
        return [CB[C_IN, h] * UI[h] + CB[C_UP, h] * up[h] + CB[C_DOWN, h] * down[h]
                + CB[C_ZUP, h] * z_up(u) + CB[C_ZDN, h] * z_down(u) for h, u in enumerate(cols)]

    def outer_faces(lo, hi, beyond):
        ghost = [jnp.zeros(VREG, jnp.float32)] * 2
        for q in range(NQ):
            for h, (v, at) in enumerate(((lo, NQ), (hi, NQ * HALF))):
                at = at + q
                moved = turn(v[SUB * q:SUB * q + SUB], lax.rem(at - edge + LANES, LANES))
                ghost[h] = jnp.where(lane == at, moved, ghost[h])
        return [CB[C_OUT, h] * beyond[h] + CB[C_DOWN - h, h] * ghost[h] for h in TILES]

    x0_vec = lambda t, q: X0[t, pl.ds(q, NZ), :]

    def start_plane(i, rho, state):
        h = i // 32
        j = lax.rem(i, 32)
        r = rowsof(i)
        kx_down = state[2]
        u, nb, ky, kx, state = neighbours(x0_vec, i, j, H[0, h], HK[h], state)
        down = [turn(ky[t], 1) for t in TILES]
        ky_lo = [jnp.where(first, unpack(KYH[h], j), down[0]), jnp.where(first, down[0], down[1])]
        for t in TILES:
            diag = D[t, pl.ds(r, NZ), :] + ky[t] + ky_lo[t] + kx[t] + kx_down[t]
            diag = diag + KZ[t, pl.ds(r + SUB, NZ), :] + KZ[t, pl.ds(r + TOP, NZ), :]
            D[t, pl.ds(r, NZ), :] = diag
            res = Z[0, t, pl.ds(r + NZ, NZ), :] - (diag * u[t] - nb[t])
            Z[0, t, pl.ds(r + NZ, NZ), :] = res
            rho = rho + res * res
        return rho, state

    UNROLL = 31

    def sweep(vec, plane, k, sums1, more):
        def run(i, n, c):
            state = first_state(vec, i)
            for m in range(n):
                c, state = plane(i + m, c, state)
            return c

        sums1 = run(NX - 1, 1, run(0, 1, sums1))

        @pl.when(more)
        def _():
            send_x(k)

        return lax.fori_loop(0, (NX - 2) // UNROLL, lambda m, c: run(1 + UNROLL * m, UNROLL, c), sums1)

    zero24 = zero_plane
    zero_tile = zero_plane
    kx_cols = with_ghosts(CB[C_UP, 0], CB[C_UP, 1], KX[tb, pl.ds(0, NZ), :], zero_tile)
    for h in TILES:
        CB[C_DOWN, h] = turn(kx_cols[h], NQ)
        ky_edge, ky_in = CB[C_OUT, h], CB[C_IN, h]
        CB[C_OUT, h] = jnp.where(py == 0, ky_edge, KYH[h])
        CB[C_IN, h] = jnp.where(py == 0, ky_in, ky_edge)
    far = outer_faces(X0[tb, pl.ds(0, NZ), :], X0[tb, pl.ds(HI, NZ), :], (H[0, 0], H[0, 1]))
    own = own_faces((PKS[0, 0], PKS[0, 1]))
    for h in TILES:
        diag = CB[C_D, h] + CB[C_UP, h] + CB[C_DOWN, h] + CB[C_OUT, h] + CB[C_IN, h] + CB[C_ZUP, h] + CB[C_ZDN, h]
        CB[C_D, h] = diag
        PKS[1, h] = PRE[h] - (diag * PKS[0, h] - far[h] - own[h])
    send_column(0)
    rho0 = sweep(x0_vec, start_plane, 0, zero24, px >= 0)
    pack(Z.at[0], NZ, inner, UI)
    PT[...] = jnp.where((row == 0) & (lane == 0), full_sum(rho0), NIL)

    for n in range(20):
        ST[n] = jnp.zeros(VREG, jnp.float32)
    totals = sum_take(0)
    cells = CELLS
    mean = [full_sum(jnp.where((row == 2) & (lane == n), totals, NIL)) * (1.0 / cells) for n in range(6)]
    var_s = jnp.maximum(mean[1] - mean[0] * mean[0], NIL)
    var_k = jnp.maximum(mean[5] - mean[2] * mean[2] - mean[NQ] * mean[NQ] - mean[4] * mean[4], NIL)
    b_first = jnp.sqrt(3.0 * mean[5] + var_s + 2.0 * var_k)
    a_first = jnp.maximum(mean[0] - 0.5 * jnp.sqrt(var_s), 0.3) + 2.0 * b_first

    def set_coefs(k0, a_new, b_new):
        old_b = ST[S_B]
        b_arr = jnp.where(lane >= k0, b_new, old_b)
        ST[S_A] = jnp.where(lane >= k0, a_new, ST[S_A])
        ST[S_B] = b_arr
        ST[S_C] = jnp.where(lane == 0, NIL, turn(b_arr, 1))
        inv = 1.0 / b_new
        for k in range(k0, ITERS):
            CO[k, K_A] = a_new
            if k > k0:
                CO[k, K_C] = b_new
            elif k == 0:
                CO[k, K_C] = jnp.zeros(VREG, jnp.float32)
            else:
                CO[k, K_C] = CO[k - 1, K_B]
            CO[k, K_INV] = inv
            CO[k, K_B] = b_new

    set_coefs(0, a_first, b_first)

    def gram_start(total):
        rho = full_sum(jnp.where((row == 0) & (lane == 0), total, NIL))
        one = jnp.where(lane == 0, 1.0, NIL)
        for n in (S_GP, S_Y, S_BA, S_LA, S_LB, S_LA2, S_LB2, S_ERR):
            ST[n] = jnp.zeros(VREG, jnp.float32)
        ST[S_G] = one * rho
        ST[S_CL] = one
        ST[S_DL] = one
        ST[S_LEAD] = jnp.ones(VREG, jnp.float32)
        ST[S_RHO] = rho
        ST[S_RHO0] = rho
        ST[S_HIST] = one * rho

    def gram_step(k, total):
        a, b, c = ST[S_A], ST[S_B], ST[S_C]
        g, gp, cl, dl = ST[S_G], ST[S_GP], ST[S_CL], ST[S_DL]
        d_row, e_row = jnp.broadcast_to(total[0:1], VREG), jnp.broadcast_to(total[1:2], VREG)
        rho, lead = ST[S_RHO], ST[S_LEAD]
        b_k, c_k, a_k = CO[k, K_B], CO[k, K_C], CO[k, K_A]
        at_k, at_k1 = lane == k, lane == k + 1
        rec = ((a - a_k) * g + b * turn(g, LAST)
               + c * turn(g, 1) - c_k * gp) * CO[k, K_INV]
        g_new = jnp.where(lane < k, rec, jnp.where(at_k, e_row, jnp.where(at_k1, d_row, NIL)))
        g_full = jnp.where(at_k1, turn(e_row, 1), g)
        image = a * dl + turn(b * dl, 1) + turn(c * dl, LAST)
        delta = lead * lane_sum(image * g_full)
        alpha = rho / delta
        ST[S_AL] = alpha
        y = ST[S_Y] + alpha * dl
        cl = cl - alpha * image
        lead = -alpha * b_k * lead
        prod = cl * g_new
        rho_new = lead * lane_sum(prod)
        size = lane_sum(jnp.abs(cl) * jnp.where(lane < k + 2, jnp.sqrt(jnp.maximum(d_row, NIL)), NIL))
        beta = rho_new / rho
        dl = cl + beta * dl
        ST[S_G], ST[S_GP], ST[S_CL], ST[S_DL] = g_new, g, cl, dl
        ST[S_Y], ST[S_RHO], ST[S_LEAD] = y, rho_new, lead
        ST[S_HIST] = jnp.where(at_k1, rho_new, ST[S_HIST])
        inv_alpha = 1.0 / alpha
        ST[S_LA2], ST[S_LB2] = ST[S_LA], ST[S_LB]
        ST[S_LA] = inv_alpha + ST[S_BA]
        ST[S_LB] = jnp.sqrt(jnp.abs(beta)) * inv_alpha
        ST[S_BA] = beta * inv_alpha
        err = size * size / jnp.sqrt(jnp.abs(rho_new) * ST[S_RHO0])
        err = jnp.where(rho_new > NIL, err, 1e30)
        ST[S_ERR] = jnp.maximum(ST[S_ERR], jnp.where(err < 1e30, err, 1e30))

    def renew(k0):
        a_new = 0.5 * (ST[S_LA] + ST[S_LA2])
        b_new = 0.5 * (ST[S_LB] + ST[S_LB2])
        a_ok = (a_new > 0.3) & (a_new < 26.8)
        a_new = jnp.where(a_ok, a_new, a_first)
        b_new = jnp.where(a_ok & (b_new > 0.25 * b_first) & (b_new < 2.0 * b_first), b_new, b_first)
        set_coefs(k0, a_new, b_new)

    def prepare(k):
        before = jnp.maximum(k - 1, 0)
        cols = (PKS[k + 1, 0], PKS[k + 1, 1])
        own = own_faces(cols)
        for h, u in enumerate(cols):
            PRE[h] = (CB[C_D, h] - CO[k, K_A]) * u - own[h] - CO[k, K_C] * PKS[before + 1, h]

    def apply_step(k):
        take_column(k)
        before = jnp.maximum(k - 1, 0)
        for h in TILES:
            far = CB[C_OUT, h] * H[k + 1, h] + CB[C_DOWN - h, h] * XG[k + 1, h]
            PKS[k + 2, h] = (PRE[h] - far) * CO[k, K_INV]

        @pl.when(k < ITERS - 1)
        def _():
            send_column(k + 1)

        for h in TILES:
            HK[h] = H[k + 1, h] * KYH[h]
        take_halo(k)
        a_k, c_k, i_k = three(CO[k, K_A]), three(CO[k, K_C]), three(CO[k, K_INV])

        def plane(i, carry, state):
            dots, cross = carry
            h = i // 32
            j = lax.rem(i, 32)
            r = rowsof(i)
            u, nb, ky, kx, state = neighbours(vec, i, j, H[k + 1, h], HK[h], state)
            for t in TILES:
                val = (D[t, pl.ds(r, NZ), :] - a_k) * u[t] - nb[t] - c_k * Z[before, t, pl.ds(r + NZ, NZ), :]
                val = val * i_k
                Z[k + 1, t, pl.ds(r + NZ, NZ), :] = val
                dots = dots + val * val
                cross = cross + val * u[t]
            return (dots, cross), state

        vec = lambda t, q: Z[k, t, pl.ds(q, NZ), :]
        dots, cross = sweep(vec, plane, k + 1, (zero24, zero24), k < ITERS - 1)

        step = k - 2

        @pl.when(step > 0)
        def _():
            sum_wait(step + 1)

        total = sum_total(jnp.maximum(step + 1, 0))
        pack(Z.at[k + 1], NZ, inner, UI)
        tile = jnp.where((row == 0) & (lane == k + 1), full_sum(dots), PT[...])
        tile = jnp.where((row == 1) & (lane == k), full_sum(cross), tile)
        PT[...] = tile
        gram_step(jnp.maximum(step, 0), total)
        prepare(jnp.minimum(k + 1, ITERS - 1))
        sum_send(k + 1, tile)

        @pl.when(k == 1)
        def _():
            gram_start(sum_take(1))

        for at in RENEW_AT:
            @pl.when(k == at)
            def _():
                renew(at + 2)

    prepare(0)

    @pl.loop(0, ITERS)
    def _(k):
        apply_step(k)

    gram_step(ITERS - 2, sum_take(ITERS - 1))

    y, d = ST[S_Y], ST[S_DL]
    for k in range(ITERS):
        YB[k] = lane_sum(jnp.where(lane == k, y, NIL))
        YB[ITERS + k] = lane_sum(jnp.where(lane == k, d, NIL))

    AHEAD = 24

    def combine(i, c):
        r = rowsof(i + 1)
        acc = [X0[t, pl.ds(r, NZ), :] for t in TILES]
        way = [zero_plane, zero_plane]
        for k in range(ITERS):
            w, v = three(YB[k]), three(YB[ITERS + k])
            for t in TILES:
                z = Z[k, t, pl.ds(r, NZ), :]
                way[t] = way[t] + v * z
                if k < ITERS - 1:
                    acc[t] = acc[t] + w * z
        for t in TILES:
            X0[t, pl.ds(r, NZ), :] = acc[t]
            Z[ITERS, t, pl.ds(r, NZ), :] = way[t]
        return c

    lax.fori_loop(0, AHEAD, combine, 0, unroll=2)
    gram_step(ITERS - 1, sum_take(ITERS))
    y = ST[S_Y]
    for k in range(ITERS):
        YB[k] = lane_sum(jnp.where(lane == k, y, NIL))
    hist = jnp.sqrt(ST[S_HIST] * (1.0 / cells))
    hist_ref[...] = jnp.where(row == 0, hist, ST[S_ERR])
    alpha = three(ST[S_AL])

    def last_step(i, c):
        r = rowsof(i + 1)
        for t in TILES:
            out_ref[pl.ds(rowsof(i), NZ), LANES * t:LANES * t + LANES] = X0[t, pl.ds(r, NZ), :] + alpha * Z[ITERS, t, pl.ds(r, NZ), :]
        return c

    def whole_step(i, c):
        r = rowsof(i + 1)
        acc = [X0[t, pl.ds(r, NZ), :] for t in TILES]
        for k in range(ITERS):
            w = three(YB[k])
            for t in TILES:
                acc[t] = acc[t] + w * Z[k, t, pl.ds(r, NZ), :]
        for t in TILES:
            out_ref[pl.ds(rowsof(i), NZ), LANES * t:LANES * t + LANES] = acc[t]
        return c

    lax.fori_loop(0, AHEAD, last_step, 0, unroll=4)
    lax.fori_loop(AHEAD, NX, whole_step, 0, unroll=2)

    @pl.when(has_hi)
    def _():
        for t in TILES:
            for cp in init_up(t):
                cp.wait_send()

    @pl.when(has_lo)
    def _():
        for t in TILES:
            for cp in init_down(t):
                cp.wait_send()

    @pl.when(py == 0)
    def _():
        ky_copy.wait_send()

    x0_copy.wait_send()

    @pl.loop(0, ITERS)
    def _(k):
        @pl.when(has_hi)
        def _():
            up_copy(k).wait_send()
            edge_up(k).wait_send()

        @pl.when(has_lo)
        def _():
            down_copy(k).wait_send()
            edge_down(k).wait_send()

        y_copy(k).wait_send()

    @pl.loop(0, ITERS + 1)
    def _(e):
        for cp in sum_copies(e):
            cp.wait_send()


def hand_over(src, dst, sem):
    cp = pltpu.make_async_copy(src, dst, sem.at[0])
    cp.start()
    cp.wait()


def publish(x_rows):
    rows = pl.pallas_call(
        hand_over, out_shape=jax.ShapeDtypeStruct(x_rows.shape, jnp.float32),
        in_specs=[pl.BlockSpec(memory_space=pltpu.VMEM)], out_specs=pl.BlockSpec(memory_space=pl.ANY),
        scratch_shapes=[pltpu.SemaphoreType.DMA((1,))])(x_rows)
    return jnp.transpose(rows.reshape(NX, NZ, ROW), (0, 2, 1))


def fused_solve(shift, rhs_field, x_init, cond_x, cond_y, cond_z):
    def flat(v):
        return jnp.transpose(v, (0, 2, 1)).reshape(BODY, 256)

    f32 = jnp.float32
    any_spec = pl.BlockSpec(memory_space=pl.ANY)
    x_rows, small = pl.pallas_call(
        kernel,
        out_shape=(pltpu.VMEM((BODY, 256), f32), jax.ShapeDtypeStruct(VREG, f32)),
        in_specs=[any_spec] * 6,
        out_specs=(pl.BlockSpec(memory_space=pltpu.VMEM), pl.BlockSpec(memory_space=pltpu.VMEM)),
        scratch_shapes=[
            pltpu.VMEM((ITERS + 1, 2, FULL, LANES), f32),
            pltpu.VMEM((2, FULL, LANES), f32),
            pltpu.VMEM((2, BODY, LANES), f32),
            pltpu.VMEM((2, BODY + 32, LANES), f32),
            pltpu.VMEM((2, BODY, LANES), f32),
            pltpu.VMEM((2, BODY + 16, LANES), f32),
            pltpu.VMEM((ITERS + 2, 2, *VREG), f32),
            pltpu.VMEM((ITERS + 2, 2, *VREG), f32),
            pltpu.VMEM((2, *VREG), f32),
            pltpu.VMEM((2, *VREG), f32),
            pltpu.VMEM((2, *VREG), f32),
            pltpu.VMEM((2, *VREG), f32),
            pltpu.VMEM((TOP, 2, *VREG), f32),
            pltpu.VMEM((2, *VREG), f32),
            pltpu.VMEM((ITERS + 2, 2, *VREG), f32),
            pltpu.VMEM((ITERS + 2, 2, *VREG), f32),
            pltpu.VMEM((ITERS + 1, *VREG), f32),
            pltpu.VMEM((ITERS + 1, 8, *VREG), f32),
            pltpu.VMEM(VREG, f32),
            pltpu.VMEM((20, *VREG), f32),
            pltpu.VMEM((ITERS, 4, *VREG), f32),
            pltpu.VMEM((2 * ITERS, *VREG), f32),
            pltpu.SemaphoreType.DMA((12,)),
            pltpu.SemaphoreType.DMA((8,)),
            pltpu.SemaphoreType.DMA((8,)),
            pltpu.SemaphoreType.DMA((ITERS, 5)),
            pltpu.SemaphoreType.DMA((ITERS, 5)),
            pltpu.SemaphoreType.DMA((ITERS + 1, TOP)),
            pltpu.SemaphoreType.DMA((ITERS + 1,)),
        ],
        compiler_params=pltpu.CompilerParams(collective_id=0, has_side_effects=True,
                                             vmem_limit_bytes=65011712),
    )(*(flat(v) for v in (shift, rhs_field, x_init, cond_x, cond_y, cond_z)))
    return x_rows, small[0, :ITERS + 1], small[1, 0]


def classic_solve(shift, rhs_field, x_init, cond_x, cond_y, cond_z):
    count_x, count_y = 4, 2
    fwd_x = [(src, src + 1) for src in range(count_x - 1)]
    back_x = [(src + 1, src) for src in range(count_x - 1)]
    pos_x, pos_y = lax.axis_index("px"), lax.axis_index("py")
    plane_x = lax.broadcasted_iota(jnp.int32, (NX, 1, 1), 0)
    plane_y = lax.broadcasted_iota(jnp.int32, (1, ROW, 1), 1)
    plane_z = lax.broadcasted_iota(jnp.int32, (1, 1, NZ), 2)
    plus_x = jnp.where((pos_x == count_x - 1) & (plane_x == NX - 1), NIL, cond_x)
    plus_y = jnp.where((pos_y == count_y - 1) & (plane_y == ROW - 1), NIL, cond_y)
    plus_z = jnp.where(plane_z == NZ - 1, NIL, cond_z)

    def shifted(vec, axis, ahead, halo):
        size = vec.shape[axis]
        if ahead:
            return jnp.concatenate([lax.slice_in_dim(vec, 1, size, axis=axis), halo], axis=axis)
        return jnp.concatenate([halo, lax.slice_in_dim(vec, 0, size - 1, axis=axis)], axis=axis)

    def below(vec):
        low_x = lax.ppermute(vec[-1:], "px", fwd_x)
        low_y = lax.ppermute(vec[:, -1:], "py", [(0, 1)])
        return (shifted(vec, 0, False, low_x), shifted(vec, 1, False, low_y),
                shifted(vec, 2, False, jnp.zeros_like(vec[:, :, :1])))

    def above(vec):
        high_x = lax.ppermute(vec[:1], "px", back_x)
        high_y = lax.ppermute(vec[:, :1], "py", [(1, 0)])
        return (shifted(vec, 0, True, high_x), shifted(vec, 1, True, high_y),
                shifted(vec, 2, True, jnp.zeros_like(vec[:, :, :1])))

    minus_x, minus_y, minus_z = below(plus_x)[0], below(plus_y)[1], below(plus_z)[2]
    diag = shift + plus_x + minus_x + plus_y + minus_y + plus_z + minus_z

    def apply_op(vec):
        up_x, up_y, up_z = above(vec)
        down_x, down_y, down_z = below(vec)
        return (diag * vec - plus_x * up_x - minus_x * down_x
                - plus_y * up_y - minus_y * down_y - plus_z * up_z - minus_z * down_z)

    def global_dot(left, right):
        return lax.psum(jnp.sum(left * right), SUM_AXES)

    res = rhs_field - apply_op(x_init)
    rho = global_dot(res, res)
    history = jnp.where(jnp.arange(ITERS + 1) == 0, rho, NIL)

    def step(k, state):
        x, res, p, rho, history = state
        q = apply_op(p)
        alpha = rho / global_dot(p, q)
        x = x + alpha * p
        res = res - alpha * q
        rho_new = global_dot(res, res)
        p = res + (rho_new / rho) * p
        return x, res, p, rho_new, jnp.where(jnp.arange(ITERS + 1) == k + 1, rho_new, history)

    x, _, _, _, history = lax.fori_loop(0, ITERS, step, (jnp.zeros_like(res), res, res, rho, history))
    return x_init + x, jnp.sqrt(history / CELLS)


def solution(mesh):
    field_spec = P("px", "py", None)

    def local_solve(*fields):
        x_rows, history, err = fused_solve(*fields)
        return lax.cond(err < ERR_LIMIT, lambda: (publish(x_rows), history), lambda: classic_solve(*fields))

    return jax.shard_map(local_solve, mesh=mesh, in_specs=(field_spec,) * 6,
                         out_specs=(field_spec, P()), check_vma=False)
```
